32 devices in a mesh: gy: 8 (over z, x), gx: 4 (over y, core).
Axes of the slice: x: 2, y: 2, z: 4, core: 2. Of those that a mesh axis runs over, the one named last changes fastest.
Arguments:
- right_side: float32 [32, 512, 512], P(None, 'gy', 'gx'), may hold values from -32 to 32
- couplings: float32 [3, 512, 512], P(None, 'gy', 'gx'), may hold values from 0.1 to 0.5
- center: float32 [512, 512], P('gy', 'gx'), may hold values from 0.6 to 1.5
- ocean_mask: int32 [512, 512], P('gy', 'gx'), may hold values 0 or 1
Outputs:
- solution: float32 [32, 512, 512], P(None, 'gy', 'gx')
- residual: float32 [32, 512, 512], P(None, 'gy', 'gx')
The draws below stay inside these ranges and needn't reach their ends.
All inputs are finite; a program needn't handle non-finite values. No bound on the sum of `ocean_mask` on one device may be relied on, other than what follows from the above.
Results may differ from the reference program's by a relative error of at most 0.0055.
Values sent between devices are 32-bit elements; how exact they have to be, the bound alone decides.
A program may use at most 64 MiB of HBM per device.

```python
import math
import jax
import jax.numpy as jnp
from jax import lax

MEMBERS = 32
ITERS = 6
NLAT = 512
NLON = 512


def draw_right_side(key, part):
    key_base = jax.random.fold_in(key, 0)
    latitude = jnp.arange(NLAT, dtype=jnp.float32) / max(NLAT - 1, 1)
    rising = (1.0 + 2.0 * latitude)[None, :, None]
    base = jnp.clip(jax.random.normal(key_base, (MEMBERS, NLAT, NLON), jnp.float32), -5.0, 5.0)
    return base * rising


def place_ends(array, stream_key, least, top_value):
    longest = array.shape.index(max(array.shape))
    spots = []
    for shift in (0, 1):
        where = [jax.random.randint(jax.random.fold_in(stream_key, axis), (), 0, length) for axis, length in enumerate(array.shape)]
        where[longest] = (where[longest] + shift) % array.shape[longest]
        spots.append(tuple(where))
    return array.at[spots[0]].set(least).at[spots[1]].set(top_value)


def block_levels(key, extent, cuts, least, top_value):
    level = 1.0
    for dim, parts in cuts:
        steps = jax.random.uniform(jax.random.fold_in(jax.random.fold_in(key, 6), dim), (parts,), jnp.float32, least / len(cuts), top_value / len(cuts))
        level = level * jnp.repeat(jnp.exp(steps), extent[dim] // parts).reshape((-1,) + (1,) * (len(extent) - 1 - dim))
    return level


def setup_inputs(seed: int = 0) -> dict:
    keys = jax.random.split(jax.random.key(seed), 5)
    return {
        "right_side": draw_right_side(jax.random.fold_in(keys[4], 71), 0),
        "couplings": jnp.clip(jnp.exp(math.log(0.5) - 1.609438 * jax.random.uniform(keys[1], (3, NLAT, NLON), jnp.float32) ** block_levels(keys[1], (3, NLAT, NLON), ((1, 8), (2, 4)), -0.2, 0.2)), 0.1, 0.5),
        "center": jnp.clip(jnp.exp(math.log(1.5) - 0.9162907 * jax.random.uniform(keys[2], (NLAT, NLON), jnp.float32) ** block_levels(keys[2], (NLAT, NLON), ((0, 8), (1, 4)), -0.2, 0.2)), 0.6, 1.5),
        "ocean_mask": place_ends((jax.random.randint(keys[3], (NLAT, NLON), 0, 10) < 9).astype(jnp.int32), jax.random.fold_in(keys[3], 1), 0, 1),
    }


def extend_field(field):
    north_row = field[-1, ::-1]
    lat_padded = jnp.concatenate([jnp.zeros((1, field.shape[1]), jnp.float32), field, north_row[None, :]], axis=0)
    return jnp.concatenate([lat_padded[:, -1:], lat_padded, lat_padded[:, :1]], axis=1)


def coupling_terms(couplings):
    north_c = couplings[0]
    east_c = couplings[1]
    corner_c = couplings[2]
    zero_row = jnp.zeros((1, north_c.shape[1]), jnp.float32)
    north_s = jnp.concatenate([zero_row, north_c[:-1]], axis=0)
    east_w = jnp.roll(east_c, 1, axis=1)
    corner_s = jnp.concatenate([zero_row, corner_c[:-1]], axis=0)
    corner_w = jnp.roll(corner_c, 1, axis=1)
    corner_sw = jnp.roll(corner_s, 1, axis=1)
    return (north_c, north_s, east_c, east_w, corner_c, corner_s, corner_w, corner_sw)


def operate(field, terms, diag_total, oceanf):
    padded = extend_field(field)
    beside = terms[0] * padded[2:, 1:-1] + terms[1] * padded[:-2, 1:-1]
    beside = beside + terms[2] * padded[1:-1, 2:] + terms[3] * padded[1:-1, :-2]
    beside = beside + terms[4] * padded[2:, 2:] + terms[5] * padded[:-2, 2:]
    beside = beside + terms[6] * padded[2:, :-2] + terms[7] * padded[:-2, :-2]
    return oceanf * (diag_total * field - beside)


def reference(right_side, couplings, center, ocean_mask):
    oceanf = ocean_mask.astype(jnp.float32)
    terms = coupling_terms(couplings)
    diag_total = center + terms[0] + terms[1] + terms[2] + terms[3] + terms[4] + terms[5] + terms[6] + terms[7]
    inverse = oceanf / diag_total

    def solve_one(member_rhs):
        residual = member_rhs * oceanf
        precond = residual * inverse
        direction = precond
        rz_now = jnp.sum(residual * precond)
        solution = jnp.zeros_like(residual)
        for iteration in range(ITERS):
            image_field = operate(direction, terms, diag_total, oceanf)
            step_size = rz_now / jnp.sum(direction * image_field)
            solution = solution + step_size * direction
            residual = residual - step_size * image_field
            precond = residual * inverse
            rz_new = jnp.sum(residual * precond)
            direction = precond + (rz_new / rz_now) * direction
            rz_now = rz_new
        return solution, residual

    solution, residual = lax.map(solve_one, right_side)
    return (solution, residual)
```

```python
import jax
import jax.numpy as jnp
from jax import lax
from jax.experimental import pallas as pl
from jax.experimental.pallas import tpu as pltpu
from jax.sharding import PartitionSpec as P

ITERS = 6
ROOT = 0.28
PAD = 16
VMEM = 67043328
GRANT = 24 * 1024 * 1024
PAIRS = [(i, j) for i in range(ITERS) for j in range(i, ITERS + 1)]
F32 = jnp.float32


def iota(dim):
    return lax.broadcasted_iota(jnp.int32, (8, 128), dim)


def along(x, idx, axis):
    return jnp.take_along_axis(x, idx, axis=axis, mode="promise_in_bounds")


def prepare(members, rows, top, planes, shifted, inv, links, square):
    groups = 128 // members
    sub_rows = rows // groups
    lanes = iota(1)
    group = lax.shift_right_logical(lanes, members.bit_length() - 1)
    seam = lanes == rows + 8
    folded = jnp.logical_and(top, lanes >= rows + 8)
    tiles = 18
    first = PAD - 8

    @pl.loop(0, tiles)
    def _(t):
        at = pl.ds(pl.multiple_of(first + 8 * t, 8), 8)
        nxt = pl.ds(first + 8 * t + 1, 8)
        for n, p in enumerate((1, 2)):
            shifted[n, at, :] = jnp.where(folded, planes[p, nxt, :], planes[p, at, :])

    def before(v):
        return pltpu.roll(v, 1, 1)

    def after(v):
        return pltpu.roll(v, 127, 1)

    @pl.loop(0, tiles)
    def _(t):
        at = pl.ds(pl.multiple_of(first + 8 * t, 8), 8)
        prv = pl.ds(first + 8 * t - 1, 8)
        cn, ce, cne = planes[0, at, :], shifted[0, at, :], shifted[1, at, :]
        cew, cnw = shifted[0, prv, :], shifted[1, prv, :]
        diag = planes[3, at, :] + cn + ce + cew + cne + cnw + before(cn + cne + cnw)
        ocean = planes[4, at, :] > 0.0
        root = jnp.sqrt(diag)
        recip = jnp.where(ocean, 1.0 / root, 0.0)
        root = jnp.where(ocean, root, 0.0)
        inv[at, :] = jnp.where(seam, after(recip), recip)
        square[at, :] = root

    @pl.loop(0, tiles)
    def _(t):
        at = pl.ds(pl.multiple_of(first + 8 * t, 8), 8)
        nxt = pl.ds(first + 8 * t + 1, 8)
        here, east = inv[at, :], inv[nxt, :]
        up, up_east = after(here), after(east)
        here_up = jnp.where(seam, before(here), here)
        east_up = jnp.where(seam, before(east), east)
        factor = 1.0 / ROOT
        cn, ce, cne = planes[0, at, :] * factor, shifted[0, at, :] * factor, shifted[1, at, :] * factor
        values = (cn * here_up * up, ce * here * east, cne * here_up * up_east, cne * east_up * up)
        step = group * sub_rows
        extra = (group == groups - 1).astype(jnp.int32)
        count = sub_rows + 2 * ITERS
        for r in range(count + 1):
            if r < sub_rows + ITERS:
                idx = step + (r + 8 - ITERS)
            else:
                idx = step + extra + (r + 7 - ITERS)
            for n, v in enumerate(values):
                links[n, r, at, :] = along(v, idx, 1)


def iterate(members, rows, raw, inv, links, basis, gram_ref):
    groups = 128 // members
    sub_rows = rows // groups
    lanes, subs = iota(1), iota(0)
    group = lax.shift_right_logical(lanes, members.bit_length() - 1)
    step = group * sub_rows
    extra = (group == groups - 1).astype(jnp.int32)

    @pl.loop(0, 18)
    def _(t):
        at = pl.ds(pl.multiple_of(PAD - 8 + 8 * t, 8), 8)
        here = inv[at, :]
        for r in range(sub_rows + 2 * ITERS):
            if r < sub_rows + ITERS:
                idx = step + (r + 8 - ITERS)
            else:
                idx = step + extra + (r + 8 - ITERS)
            basis[0][r, at, :] = raw[r, at, :] * along(here, idx, 1)

    for k in range(ITERS):
        depth = ITERS - 1 - k
        here, out = basis[k], basis[k + 1]
        old = basis[k - 1] if k else None

        @pl.loop(0, (128 + 2 * depth + 7) // 8)
        def _(t):
            x0 = PAD - depth + 8 * t
            mid, east, west = pl.ds(x0, 8), pl.ds(x0 + 1, 8), pl.ds(x0 - 1, 8)

            def three(r):
                return here[r, west, :], here[r, mid, :], here[r, east, :]

            start, stop = ITERS - depth, ITERS + sub_rows + depth
            dn, cur = three(start - 1), three(start)
            north = links[0, start - 1, mid, :]
            for r in range(start, stop):
                nxt = three(r + 1)
                c = r + (1 if r >= ITERS + sub_rows else 0)
                if r == ITERS + sub_rows:
                    north = links[0, c - 1, mid, :]
                south, north = north, links[0, c, mid, :]
                total = (north * nxt[1] + south * dn[1]) + (
                    links[1, c, mid, :] * cur[2] + links[1, c, west, :] * cur[0]
                )
                total = total + (links[2, c, mid, :] * nxt[2] + links[2, c - 1, west, :] * dn[0])
                total = total + (links[3, c, west, :] * nxt[0] + links[3, c - 1, mid, :] * dn[2])
                if old is not None:
                    total = total - old[r, mid, :]
                out[r, mid, :] = total
                dn, cur = cur, nxt

    def body(r, sums):
        sums = list(sums)
        for t in range(16):
            at = slice(PAD + 8 * t, PAD + 8 * t + 8)
            vs = [basis[k][r + ITERS, at, :] for k in range(ITERS + 1)]
            for n, (i, j) in enumerate(PAIRS):
                sums[n] = sums[n] + vs[i] * vs[j]
        return tuple(sums)

    zero = jnp.zeros((8, 128), F32)
    sums = lax.fori_loop(0, sub_rows, body, (zero,) * len(PAIRS))
    pack = [zero] * 4
    for n, s in enumerate(sums):
        for step in (1, 2, 4):
            s = s + pltpu.roll(s, step, 0)
        pack[n // 8] = jnp.where(subs == n % 8, s, pack[n // 8])
    total = zero
    for j, v in enumerate(pack):
        width = members
        while width < 128:
            v = v + pltpu.roll(v, width, 1)
            width *= 2
        total = jnp.where(group == j, v, total)
    gram_ref[...] = total


def coefficients(gram):
    def g(i, j):
        return gram[min(i, j)][max(i, j)]

    def applied(p):
        q = []
        for k in range(ITERS + 1):
            terms = []
            if k < len(p):
                terms.append(p[k])
            if 0 < k <= len(p):
                terms.append(-ROOT * p[k - 1])
            if k + 1 < len(p):
                terms.append(-ROOT * p[k + 1])
            if terms:
                q.append(sum(terms[1:], terms[0]))
        return q

    def inner(p, q):
        total = None
        for i, a in enumerate(p):
            row = None
            for j, b in enumerate(q):
                t = g(i, j) * b
                row = t if row is None else row + t
            t = a * row
            total = t if total is None else total + t
        return total

    one = jnp.ones_like(gram[0][0])
    z, p, x = [one], [one], []
    rz = g(0, 0)
    for iteration in range(ITERS):
        q = applied(p)
        step = rz / inner(p, q)
        x = [(x[k] if k < len(x) else 0.0) + step * p[k] for k in range(len(p))]
        z = [(z[k] if k < len(z) else 0.0) - step * q[k] for k in range(len(q))]
        if iteration + 1 < ITERS:
            rz_new = inner(z, z)
            beta = rz_new / rz
            p = [z[k] + (beta * p[k] if k < len(p) else 0.0) for k in range(len(z))]
            rz = rz_new
    return x, z


def combine(members, rows, basis, scale_ref, sums, outs, stage, sems):
    groups = 128 // members
    sub_rows = rows // groups
    tall = stage.shape[2]
    lanes = iota(1)
    tiles = [along(sums, (lanes & (members - 1)) + members * j, 1) for j in range(4)]
    gram = [[None] * (ITERS + 1) for _ in range(ITERS + 1)]
    for n, (i, j) in enumerate(PAIRS):
        gram[i][j] = jnp.broadcast_to(tiles[n // 8][n % 8 : n % 8 + 1, :], (8, 128))
    xs, zs = coefficients(gram)
    flat = stage.reshape(2 * members * tall, 128)
    blocks = members // 8
    half = sub_rows // 2

    def drain(h):
        copies = []
        for o in range(2):
            for g in range(groups):
                at = slice(sub_rows * g + half * h, sub_rows * g + half * (h + 1))
                copies.append(
                    pltpu.make_async_copy(stage.at[o, :, at, :], outs[o].at[:, at, :], sems.at[h, o, g])
                )
        return copies

    started = []
    for h in range(2):

        @pl.loop(half * h, half * (h + 1))
        def _(r):
            found = ([], [])
            for t in range(16):
                at = slice(PAD + 8 * t, PAD + 8 * t + 8)
                vs = [basis[k][r + ITERS, at, :] for k in range(ITERS + 1)]
                found[0].append(sum((xs[k] * vs[k] for k in range(1, ITERS)), xs[0] * vs[0]))
                found[1].append(sum((zs[k] * vs[k] for k in range(1, ITERS + 1)), zs[0] * vs[0]))
            for o in range(2):
                turned = jnp.concatenate(found[o], axis=0).T
                for g in range(groups):
                    row = sub_rows * g + r
                    scale = jnp.broadcast_to(scale_ref[o, pl.ds(row + 8, 1), :], (8, 128))
                    for b in range(blocks):
                        n = 8 * (g * blocks + b)
                        at = pl.ds((o * members + 8 * b) * tall + row, 8, stride=tall)
                        flat[at, :] = turned[n : n + 8, :] * scale

        for c in drain(h):
            c.start()
            started.append(c)
    for c in started:
        c.wait()


def solve_kernel(members, rows, ny, nx, rhs_hbm, coup_hbm, center_hbm, mask_hbm, *refs):
    outs, basis = refs[:2], refs[2 : ITERS + 3]
    (
        scale_ref, stage, drain, field, planes, rhs, coup, center, mask, coef_out, coef_in, rows_out, rows_in, ext,
        shifted, inv, links, square, gram, along_x, along_y, load, send, recv,
    ) = refs[ITERS + 3 :]
    groups = 128 // members
    sub_rows = rows // groups
    tall = rhs.shape[1]
    y, x = lax.axis_index("gy"), lax.axis_index("gx")
    top = (y + 1) // ny
    mirror = nx - 1 - x
    east, west = lax.rem(x + 1, nx), lax.rem(x + nx - 1, nx)
    up = (y + 1 - top, x + top * (mirror - x))
    down = (jnp.maximum(y - 1, 0), x)
    loads = [
        pltpu.make_async_copy(coup_hbm, coup, load.at[0]),
        pltpu.make_async_copy(center_hbm, center, load.at[1]),
        pltpu.make_async_copy(mask_hbm, mask, load.at[2]),
        pltpu.make_async_copy(rhs_hbm, rhs.at[:, 0:rows, :], load.at[3]),
    ]
    for c in loads:
        c.start()
    barrier = pltpu.get_barrier_semaphore()

    def greet(there):
        pl.semaphore_signal(barrier, inc=1, device_id=there, device_id_type=pl.DeviceIdType.MESH)

    for step in range(1, nx):
        greet((y, lax.rem(x + step, nx)))
    for step in range(1, ny):
        greet((lax.rem(y + step, ny), x))

    def copy(src, dst, n, m, there):
        return pltpu.make_async_remote_copy(
            src_ref=src,
            dst_ref=dst,
            send_sem=send.at[n],
            recv_sem=recv.at[m],
            device_id=there,
            device_id_type=pl.DeviceIdType.MESH,
        )

    lanes, subs = iota(1), iota(0)
    flip_lane = jnp.where(top == 1, 127 - lanes, lanes)
    flip_sub = jnp.where(top == 1, 7 - subs, subs)
    for c in loads[:3]:
        c.wait()

    def own(p, at):
        if p < 3:
            return coup[p, at, :]
        return center[at, :] if p == 3 else mask[at, :].astype(F32)

    for p in range(5):
        coef_out[0, p] = along(along(own(p, slice(rows - 8, rows)), flip_lane, 1), flip_sub, 0)
        coef_out[1, p] = own(p, slice(0, 8))
    pl.semaphore_wait(barrier, nx + ny - 2)

    coef_up = copy(coef_out.at[0], coef_in.at[top], 0, top, up)
    coef_down = copy(coef_out.at[1], coef_in.at[1], 1, 1, down)
    rows_up = copy(rows_out.at[0], rows_in.at[top], 2, 2 + top, up)
    rows_down = copy(rows_out.at[1], rows_in.at[1], 3, 3, down)
    coef_up.start()

    @pl.when(y > 0)
    def _():
        coef_down.start()

    flat = rhs.reshape(members * tall, 128)

    def column(row, block):
        return flat[pl.ds(8 * block * tall + row, 8, stride=tall), :]

    blocks = members // 8
    loads[3].wait()
    for q in range(ITERS):
        high = rows - ITERS + q + top * (ITERS - 1 - 2 * q)
        for b in range(blocks):
            at = slice(q * members + 8 * b, q * members + 8 * b + 8)
            rows_out[0, at, :] = along(column(high, b), flip_lane, 1)
            rows_out[1, at, :] = column(q, b)
    rows_up.start()

    @pl.when(y > 0)
    def _():
        rows_down.start()

    @pl.loop(0, sub_rows)
    def _(r):
        stack = [column(sub_rows * g + r, b) for g in range(groups) for b in range(blocks)]
        field[r + ITERS, PAD : PAD + 128, :] = jnp.concatenate(stack, axis=0).T

    coef_north = copy(coef_out.at[1], coef_in.at[1], 1, 1, down)
    coef_south = copy(coef_out.at[0], coef_in.at[0], 0, 0, up)
    coef_north.wait_recv()

    @pl.when(y > 0)
    def _():
        coef_south.wait_recv()

    for p in range(5):
        beyond = coef_in[1, p]
        moved = pltpu.roll(beyond, 1, 0)
        if p in (0, 2):
            last = jnp.broadcast_to(own(p, slice(rows - 1, rows)), (8, 128))
            beyond = jnp.where(top == 1, beyond, jnp.where(subs == 0, last, moved))
        else:
            beyond = jnp.where(subs == 0, beyond, moved)
        ext[0:8, :] = jnp.where(y == 0, 0.0, coef_in[0, p])
        ext[8 : rows + 8, :] = own(p, slice(0, rows))
        ext[rows + 8 : rows + 16, :] = beyond
        ext[rows + 16 : 128, :] = jnp.zeros((112 - rows, 128), F32)
        planes[p, PAD : PAD + 128, :] = ext[...].T

    def sideways(ref, n):
        return [
            copy(ref.at[:, PAD : PAD + 8, :], ref.at[:, PAD + 128 : PAD + 136, :], n, n, (y, west)),
            copy(ref.at[:, PAD + 120 : PAD + 128, :], ref.at[:, PAD - 8 : PAD, :], n + 1, n + 1, (y, east)),
        ]

    sides = sideways(planes, 4)
    for c in sides:
        c.start()
    for c in sides:
        c.wait()
    prepare(members, rows, y == ny - 1, planes, shifted, inv, links, square)
    copy(rows_out.at[1], rows_in.at[1], 3, 3, down).wait_recv()

    @pl.when(y > 0)
    def _():
        copy(rows_out.at[0], rows_in.at[0], 2, 2, up).wait_recv()

    @pl.loop(0, ITERS)
    def _(q):
        def arrived(side, b):
            return rows_in[side, pl.ds(pl.multiple_of(q * members, 8) + 8 * b, 8), :]

        low = [jnp.where(y == 0, 0.0, arrived(0, b)) for b in range(blocks)]
        low += [column(sub_rows * g - ITERS + q, b) for g in range(1, groups) for b in range(blocks)]
        field[q, PAD : PAD + 128, :] = jnp.concatenate(low, axis=0).T
        high = [column(sub_rows * g + q, b) for g in range(1, groups) for b in range(blocks)]
        high += [arrived(1, b) for b in range(blocks)]
        field[q + ITERS + sub_rows, PAD : PAD + 128, :] = jnp.concatenate(high, axis=0).T

    more = sideways(field, 6)
    for c in more:
        c.start()
    coef_up.wait_send()
    rows_up.wait_send()

    @pl.when(y > 0)
    def _():
        coef_down.wait_send()
        rows_down.wait_send()

    for c in more:
        c.wait()
    iterate(members, rows, field, inv, links, basis, gram)

    def sent(source, dst, n, there):
        c = copy(source, dst, n, n, there)
        c.start()
        return c

    across = [sent(gram, along_x.at[s], 7 + s, (y, lax.rem(x + s, nx))) for s in range(1, nx)]
    scale_ref[0] = inv[PAD : PAD + 128, :].T
    scale_ref[1] = square[PAD : PAD + 128, :].T
    for c in across:
        c.wait()
    along_x[0] = sum((along_x[s] for s in range(1, nx)), gram[...])
    across = [
        sent(along_x.at[0], along_y.at[s], 6 + nx + s, (lax.rem(y + s, ny), x)) for s in range(1, ny)
    ]
    for c in across:
        c.wait()
    sums = sum((along_y[s] for s in range(1, ny)), along_x[0])
    combine(members, rows, basis, scale_ref, sums, outs, stage, drain)


def on_device(right_side, couplings, center, ocean_mask):
    members, rows, columns = right_side.shape
    groups = 128 // members
    sub_rows = rows // groups
    assert columns == 128 and members % 8 == 0 and groups * members == 128
    assert rows <= 104 and sub_rows % 16 == 0 and sub_rows >= ITERS
    ny, nx = lax.axis_size("gy"), lax.axis_size("gx")
    vmem = pl.BlockSpec(memory_space=pltpu.VMEM)
    hbm = pl.BlockSpec(memory_space=pltpu.HBM)
    deep, wide = sub_rows + 2 * ITERS, columns + 2 * PAD + 8

    kernel_vmem = 60 * 1024 * 1024

    def first(*refs):
        solve_kernel(members, rows, ny, nx, *refs)

    return pl.pallas_call(
        first,
        out_shape=(jax.ShapeDtypeStruct(right_side.shape, F32),) * 2,
        in_specs=[hbm] * 4,
        out_specs=(hbm, hbm),
        scratch_shapes=[pltpu.VMEM((deep, wide, 128), F32)] * (ITERS + 1)
        + [
            pltpu.VMEM((2, 128, 128), F32),
            pltpu.VMEM((2, members, rows + 8, columns), F32),
            pltpu.SemaphoreType.DMA((2, 2, groups)),
            pltpu.VMEM((deep, wide, 128), F32),
            pltpu.VMEM((5, wide, 128), F32),
            pltpu.VMEM((members, rows + 8, columns), F32),
            pltpu.VMEM((3, rows, columns), F32),
            pltpu.VMEM((rows, columns), F32),
            pltpu.VMEM((rows, columns), jnp.int32),
            pltpu.VMEM((2, 5, 8, columns), F32),
            pltpu.VMEM((2, 5, 8, columns), F32),
            pltpu.VMEM((2, ITERS * members, columns), F32),
            pltpu.VMEM((2, ITERS * members, columns), F32),
            pltpu.VMEM((128, 128), F32),
            pltpu.VMEM((2, wide, 128), F32),
            pltpu.VMEM((wide, 128), F32),
            pltpu.VMEM((4, deep + 1, wide, 128), F32),
            pltpu.VMEM((wide, 128), F32),
            pltpu.VMEM((8, 128), F32),
            pltpu.VMEM((nx, 8, 128), F32),
            pltpu.VMEM((ny, 8, 128), F32),
            pltpu.SemaphoreType.DMA((4,)),
            pltpu.SemaphoreType.DMA((6 + nx + ny,)),
            pltpu.SemaphoreType.DMA((6 + nx + ny,)),
        ],
        compiler_params=pltpu.CompilerParams(
            collective_id=0, has_side_effects=True, vmem_limit_bytes=kernel_vmem
        ),
    )(right_side, couplings, center, ocean_mask)


def solution(mesh):
    in_specs = (P(None, "gy", "gx"), P(None, "gy", "gx"), P("gy", "gx"), P("gy", "gx"))
    out_specs = (P(None, "gy", "gx"), P(None, "gy", "gx"))
    return jax.shard_map(
        on_device, mesh=mesh, in_specs=in_specs, out_specs=out_specs, check_vma=False
    )
```

```python
import jax
import jax.numpy as jnp
from jax import lax
from jax.experimental import pallas as pl
from jax.experimental.pallas import tpu as pltpu
from jax.sharding import PartitionSpec as P

ITERS = 6
ROOT = 0.28
PAD = 16
VMEM = 67043328
GRANT = 24 * 1024 * 1024
PAIRS = [(i, j) for i in range(ITERS) for j in range(i, ITERS + 1)]
F32 = jnp.float32


def iota(dim):
    return lax.broadcasted_iota(jnp.int32, (8, 128), dim)


def along(x, idx, axis):
    return jnp.take_along_axis(x, idx, axis=axis, mode="promise_in_bounds")


def prepare(members, rows, top, planes, shifted, inv, links, square, lhs, pick):
    lanes = iota(1)
    seam = lanes == rows + 8
    folded = jnp.logical_and(top, lanes >= rows + 8)
    tiles = 18
    first = PAD - 8

    @pl.loop(0, tiles)
    def _(t):
        at = pl.ds(pl.multiple_of(first + 8 * t, 8), 8)
        nxt = pl.ds(first + 8 * t + 1, 8)
        for n, p in enumerate((1, 2)):
            shifted[n, at, :] = jnp.where(folded, planes[p, nxt, :], planes[p, at, :])

    def before(v):
        return pltpu.roll(v, 1, 1)

    def after(v):
        return pltpu.roll(v, 127, 1)

    @pl.loop(0, tiles)
    def _(t):
        at = pl.ds(pl.multiple_of(first + 8 * t, 8), 8)
        prv = pl.ds(first + 8 * t - 1, 8)
        cn, ce, cne = planes[0, at, :], shifted[0, at, :], shifted[1, at, :]
        cew, cnw = shifted[0, prv, :], shifted[1, prv, :]
        diag = planes[3, at, :] + cn + ce + cew + cne + cnw + before(cn + cne + cnw)
        ocean = planes[4, at, :] > 0.0
        root = jnp.sqrt(diag)
        recip = jnp.where(ocean, 1.0 / root, 0.0)
        root = jnp.where(ocean, root, 0.0)
        inv[at, :] = jnp.where(seam, after(recip), recip)
        square[at, :] = root

    span = rows + 16
    lanes = lax.broadcasted_iota(jnp.int32, (16, 128), 1)
    seam = lanes == rows + 8

    @pl.loop(0, tiles // 2)
    def _(t):
        at = pl.ds(pl.multiple_of(first + 16 * t, 8), 16)
        nxt = pl.ds(first + 16 * t + 1, 16)
        here, east = inv[at, :], inv[nxt, :]
        up, up_east = after(here), after(east)
        here_up = jnp.where(seam, before(here), here)
        east_up = jnp.where(seam, before(east), east)
        factor = 1.0 / ROOT
        cn, ce, cne = planes[0, at, :] * factor, shifted[0, at, :] * factor, shifted[1, at, :] * factor
        values = (cn * here_up * up, ce * here * east, cne * here_up * up_east, cne * east_up * up, here)
        for n, v in enumerate(values):
            top_part = v.astype(jnp.bfloat16).astype(F32)
            v = v - top_part
            mid_part = v.astype(jnp.bfloat16).astype(F32)
            moved = pltpu.roll(mid_part, span, 1)
            low_part = pltpu.roll(v - mid_part, 2 * span - 128, 1)
            left = jnp.where(lanes < span, top_part, moved)
            right = jnp.where(lanes < 2 * span - 128, moved, low_part)
            right = jnp.where(lanes < 3 * span - 128, right, 0.0)
            to = pl.ds(pl.multiple_of(8 * tiles * n + 16 * t, 16), 16)
            lhs[to, 0:128] = left.astype(jnp.bfloat16)
            lhs[to, 128:256] = right.astype(jnp.bfloat16)

    @pl.loop(0, links.shape[1] // 2)
    def _(p):
        found = jnp.dot(lhs[...], pick[p], preferred_element_type=F32)
        for n in range(5):
            for h in range(2):
                links[n, 2 * p + h, first : first + 8 * tiles, :] = found[
                    8 * tiles * n : 8 * tiles * (n + 1), 128 * h : 128 * h + 128
                ]


def choose(members, rows, pick):
    groups = 128 // members
    sub_rows = rows // groups
    span = rows + 16
    source = lax.broadcasted_iota(jnp.int32, (256, 256), 0)
    lane = lax.broadcasted_iota(jnp.int32, (256, 256), 1)
    source = source - span * ((source >= span).astype(jnp.int32) + (source >= 2 * span).astype(jnp.int32))
    group = lax.shift_right_logical(lane & 127, members.bit_length() - 1)
    half = lax.shift_right_logical(lane, 7)
    last = (group == groups - 1).astype(jnp.int32)
    base = source - sub_rows * group - half - 8 + ITERS

    @pl.loop(0, pick.shape[0])
    def _(p):
        later = (2 * p + half >= sub_rows + ITERS).astype(jnp.int32)
        hit = base == 2 * p + later * (last - 1)
        pick[p] = jnp.where(hit, 1.0, 0.0).astype(jnp.bfloat16)


def iterate(members, rows, raw, inv, links, basis, gram_ref):
    groups = 128 // members
    sub_rows = rows // groups
    lanes, subs = iota(1), iota(0)
    group = lax.shift_right_logical(lanes, members.bit_length() - 1)

    @pl.loop(0, sub_rows + 2 * ITERS)
    def _(r):
        c = r + (r >= sub_rows + ITERS).astype(jnp.int32)
        for t in range(18):
            at = slice(PAD - 8 + 8 * t, PAD + 8 * t)
            basis[0][r, at, :] = raw[r, at, :] * links[4, c, at, :]

    for k in range(ITERS):
        depth = ITERS - 1 - k
        here, out = basis[k], basis[k + 1]
        old = basis[k - 1] if k else None

        @pl.loop(0, (128 + 2 * depth + 7) // 8)
        def _(t):
            x0 = PAD - depth + 8 * t
            mid, east, west = pl.ds(x0, 8), pl.ds(x0 + 1, 8), pl.ds(x0 - 1, 8)

            def three(r):
                return here[r, west, :], here[r, mid, :], here[r, east, :]

            start, stop = ITERS - depth, ITERS + sub_rows + depth
            dn, cur = three(start - 1), three(start)
            north = links[0, start - 1, mid, :]
            for r in range(start, stop):
                nxt = three(r + 1)
                c = r + (1 if r >= ITERS + sub_rows else 0)
                if r == ITERS + sub_rows:
                    north = links[0, c - 1, mid, :]
                south, north = north, links[0, c, mid, :]
                total = (north * nxt[1] + south * dn[1]) + (
                    links[1, c, mid, :] * cur[2] + links[1, c, west, :] * cur[0]
                )
                total = total + (links[2, c, mid, :] * nxt[2] + links[2, c - 1, west, :] * dn[0])
                total = total + (links[3, c, west, :] * nxt[0] + links[3, c - 1, mid, :] * dn[2])
                if old is not None:
                    total = total - old[r, mid, :]
                out[r, mid, :] = total
                dn, cur = cur, nxt

    def body(r, sums):
        sums = list(sums)
        for t in range(16):
            at = slice(PAD + 8 * t, PAD + 8 * t + 8)
            vs = [basis[k][r + ITERS, at, :] for k in range(ITERS + 1)]
            for n, (i, j) in enumerate(PAIRS):
                sums[n] = sums[n] + vs[i] * vs[j]
        return tuple(sums)

    zero = jnp.zeros((8, 128), F32)
    sums = lax.fori_loop(0, sub_rows, body, (zero,) * len(PAIRS))
    pack = [zero] * 4
    for n, s in enumerate(sums):
        for step in (1, 2, 4):
            s = s + pltpu.roll(s, step, 0)
        pack[n // 8] = jnp.where(subs == n % 8, s, pack[n // 8])
    total = zero
    for j, v in enumerate(pack):
        width = members
        while width < 128:
            v = v + pltpu.roll(v, width, 1)
            width *= 2
        total = jnp.where(group == j, v, total)
    gram_ref[...] = total


def solve_kernel(members, rows, ny, nx, rhs_hbm, coup_hbm, center_hbm, mask_hbm, *refs):
    basis, (scale_ref, sum_ref) = refs[: ITERS + 1], refs[ITERS + 1 : ITERS + 3]
    (
        field, planes, rhs, coup, center, mask, coef_out, coef_in, rows_out, rows_in, ext,
        shifted, inv, links, square, lhs, pick, gram, along_x, along_y, load, send, recv,
    ) = refs[ITERS + 3 :]
    groups = 128 // members
    sub_rows = rows // groups
    tall = rhs.shape[1]
    y, x = lax.axis_index("gy"), lax.axis_index("gx")
    top = (y + 1) // ny
    mirror = nx - 1 - x
    east, west = lax.rem(x + 1, nx), lax.rem(x + nx - 1, nx)
    up = (y + 1 - top, x + top * (mirror - x))
    down = (jnp.maximum(y - 1, 0), x)
    loads = [
        pltpu.make_async_copy(coup_hbm, coup, load.at[0]),
        pltpu.make_async_copy(center_hbm, center, load.at[1]),
        pltpu.make_async_copy(mask_hbm, mask, load.at[2]),
        pltpu.make_async_copy(rhs_hbm, rhs.at[:, 0:rows, :], load.at[3]),
    ]
    for c in loads:
        c.start()
    barrier = pltpu.get_barrier_semaphore()

    def greet(there):
        pl.semaphore_signal(barrier, inc=1, device_id=there, device_id_type=pl.DeviceIdType.MESH)

    for step in range(1, nx):
        greet((y, lax.rem(x + step, nx)))
    for step in range(1, ny):
        greet((lax.rem(y + step, ny), x))

    def copy(src, dst, n, m, there):
        return pltpu.make_async_remote_copy(
            src_ref=src,
            dst_ref=dst,
            send_sem=send.at[n],
            recv_sem=recv.at[m],
            device_id=there,
            device_id_type=pl.DeviceIdType.MESH,
        )

    lanes, subs = iota(1), iota(0)
    flip_lane = jnp.where(top == 1, 127 - lanes, lanes)
    flip_sub = jnp.where(top == 1, 7 - subs, subs)
    for c in loads[:3]:
        c.wait()

    def own(p, at):
        if p < 3:
            return coup[p, at, :]
        return center[at, :] if p == 3 else mask[at, :].astype(F32)

    for p in range(5):
        coef_out[0, p] = along(along(own(p, slice(rows - 8, rows)), flip_lane, 1), flip_sub, 0)
        coef_out[1, p] = own(p, slice(0, 8))
    choose(members, rows, pick)
    pl.semaphore_wait(barrier, nx + ny - 2)

    coef_up = copy(coef_out.at[0], coef_in.at[top], 0, top, up)
    coef_down = copy(coef_out.at[1], coef_in.at[1], 1, 1, down)
    rows_up = copy(rows_out.at[0], rows_in.at[top], 2, 2 + top, up)
    rows_down = copy(rows_out.at[1], rows_in.at[1], 3, 3, down)
    coef_up.start()

    @pl.when(y > 0)
    def _():
        coef_down.start()

    flat = rhs.reshape(members * tall, 128)

    def column(row, block):
        return flat[pl.ds(8 * block * tall + row, 8, stride=tall), :]

    blocks = members // 8
    loads[3].wait()
    for q in range(ITERS):
        high = rows - ITERS + q + top * (ITERS - 1 - 2 * q)
        for b in range(blocks):
            at = slice(q * members + 8 * b, q * members + 8 * b + 8)
            rows_out[0, at, :] = along(column(high, b), flip_lane, 1)
            rows_out[1, at, :] = column(q, b)
    rows_up.start()

    @pl.when(y > 0)
    def _():
        rows_down.start()

    @pl.loop(0, sub_rows)
    def _(r):
        stack = [column(sub_rows * g + r, b) for g in range(groups) for b in range(blocks)]
        field[r + ITERS, PAD : PAD + 128, :] = jnp.concatenate(stack, axis=0).T

    coef_north = copy(coef_out.at[1], coef_in.at[1], 1, 1, down)
    coef_south = copy(coef_out.at[0], coef_in.at[0], 0, 0, up)
    coef_north.wait_recv()

    @pl.when(y > 0)
    def _():
        coef_south.wait_recv()

    for p in range(5):
        beyond = coef_in[1, p]
        moved = pltpu.roll(beyond, 1, 0)
        if p in (0, 2):
            last = jnp.broadcast_to(own(p, slice(rows - 1, rows)), (8, 128))
            beyond = jnp.where(top == 1, beyond, jnp.where(subs == 0, last, moved))
        else:
            beyond = jnp.where(subs == 0, beyond, moved)
        ext[0:8, :] = jnp.where(y == 0, 0.0, coef_in[0, p])
        ext[8 : rows + 8, :] = own(p, slice(0, rows))
        ext[rows + 8 : rows + 16, :] = beyond
        ext[rows + 16 : 128, :] = jnp.zeros((112 - rows, 128), F32)
        planes[p, PAD : PAD + 128, :] = ext[...].T

    def sideways(ref, n):
        return [
            copy(ref.at[:, PAD : PAD + 8, :], ref.at[:, PAD + 128 : PAD + 136, :], n, n, (y, west)),
            copy(ref.at[:, PAD + 120 : PAD + 128, :], ref.at[:, PAD - 8 : PAD, :], n + 1, n + 1, (y, east)),
        ]

    sides = sideways(planes, 4)
    for c in sides:
        c.start()
    copy(rows_out.at[1], rows_in.at[1], 3, 3, down).wait_recv()

    @pl.when(y > 0)
    def _():
        copy(rows_out.at[0], rows_in.at[0], 2, 2, up).wait_recv()

    @pl.loop(0, ITERS)
    def _(q):
        def arrived(side, b):
            return rows_in[side, pl.ds(pl.multiple_of(q * members, 8) + 8 * b, 8), :]

        low = [jnp.where(y == 0, 0.0, arrived(0, b)) for b in range(blocks)]
        low += [column(sub_rows * g - ITERS + q, b) for g in range(1, groups) for b in range(blocks)]
        field[q, PAD : PAD + 128, :] = jnp.concatenate(low, axis=0).T
        high = [column(sub_rows * g + q, b) for g in range(1, groups) for b in range(blocks)]
        high += [arrived(1, b) for b in range(blocks)]
        field[q + ITERS + sub_rows, PAD : PAD + 128, :] = jnp.concatenate(high, axis=0).T

    more = sideways(field, 6)
    for c in more:
        c.start()
    coef_up.wait_send()
    rows_up.wait_send()

    @pl.when(y > 0)
    def _():
        coef_down.wait_send()
        rows_down.wait_send()

    for c in sides:
        c.wait()
    prepare(members, rows, y == ny - 1, planes, shifted, inv, links, square, lhs, pick)
    for c in more:
        c.wait()
    iterate(members, rows, field, inv, links, basis, gram)

    def sent(source, dst, n, there):
        c = copy(source, dst, n, n, there)
        c.start()
        return c

    across = [sent(gram, along_x.at[s], 7 + s, (y, lax.rem(x + s, nx))) for s in range(1, nx)]
    scale_ref[0] = inv[PAD : PAD + 128, :].T
    scale_ref[1] = square[PAD : PAD + 128, :].T
    for c in across:
        c.wait()
    along_x[0] = sum((along_x[s] for s in range(1, nx)), gram[...])
    across = [
        sent(along_x.at[0], along_y.at[s], 6 + nx + s, (lax.rem(y + s, ny), x)) for s in range(1, ny)
    ]
    for c in across:
        c.wait()
    sum_ref[...] = sum((along_y[s] for s in range(1, ny)), along_x[0])


def coefficients(gram):
    def g(i, j):
        return gram[min(i, j)][max(i, j)]

    def applied(p):
        q = []
        for k in range(ITERS + 1):
            terms = []
            if k < len(p):
                terms.append(p[k])
            if 0 < k <= len(p):
                terms.append(-ROOT * p[k - 1])
            if k + 1 < len(p):
                terms.append(-ROOT * p[k + 1])
            if terms:
                q.append(sum(terms[1:], terms[0]))
        return q

    def inner(p, q):
        total = None
        for i, a in enumerate(p):
            row = None
            for j, b in enumerate(q):
                t = g(i, j) * b
                row = t if row is None else row + t
            t = a * row
            total = t if total is None else total + t
        return total

    one = jnp.ones_like(gram[0][0])
    z, p, x = [one], [one], []
    rz = g(0, 0)
    for iteration in range(ITERS):
        q = applied(p)
        step = rz / inner(p, q)
        x = [(x[k] if k < len(x) else 0.0) + step * p[k] for k in range(len(p))]
        z = [(z[k] if k < len(z) else 0.0) - step * q[k] for k in range(len(q))]
        if iteration + 1 < ITERS:
            rz_new = inner(z, z)
            beta = rz_new / rz
            p = [z[k] + (beta * p[k] if k < len(p) else 0.0) for k in range(len(z))]
            rz = rz_new
    return x, z


def combine_kernel(members, rows, *refs):
    basis, (scale_ref, sum_ref, x_out, r_out, stage, sems) = refs[: ITERS + 1], refs[ITERS + 1 :]
    groups = 128 // members
    sub_rows = rows // groups
    tall = stage.shape[2]
    lanes = iota(1)
    sums = sum_ref[...]
    tiles = [along(sums, (lanes & (members - 1)) + members * j, 1) for j in range(4)]
    gram = [[None] * (ITERS + 1) for _ in range(ITERS + 1)]
    for n, (i, j) in enumerate(PAIRS):
        gram[i][j] = jnp.broadcast_to(tiles[n // 8][n % 8 : n % 8 + 1, :], (8, 128))
    xs, zs = coefficients(gram)
    flat = stage.reshape(2 * members * tall, 128)
    blocks = members // 8
    half = sub_rows // 2
    outs = (x_out, r_out)

    def drain(h):
        copies = []
        for o in range(2):
            for g in range(groups):
                at = slice(sub_rows * g + half * h, sub_rows * g + half * (h + 1))
                copies.append(
                    pltpu.make_async_copy(stage.at[o, :, at, :], outs[o].at[:, at, :], sems.at[h, o, g])
                )
        return copies

    started = []
    for h in range(2):

        @pl.loop(half * h, half * (h + 1))
        def _(r):
            found = ([], [])
            for t in range(16):
                at = slice(PAD + 8 * t, PAD + 8 * t + 8)
                vs = [basis[k][r + ITERS, at, :] for k in range(ITERS + 1)]
                found[0].append(sum((xs[k] * vs[k] for k in range(1, ITERS)), xs[0] * vs[0]))
                found[1].append(sum((zs[k] * vs[k] for k in range(1, ITERS + 1)), zs[0] * vs[0]))
            for o in range(2):
                turned = jnp.concatenate(found[o], axis=0).T
                for g in range(groups):
                    row = sub_rows * g + r
                    scale = jnp.broadcast_to(scale_ref[o, pl.ds(row + 8, 1), :], (8, 128))
                    for b in range(blocks):
                        n = 8 * (g * blocks + b)
                        at = pl.ds((o * members + 8 * b) * tall + row, 8, stride=tall)
                        flat[at, :] = turned[n : n + 8, :] * scale

        for c in drain(h):
            c.start()
            started.append(c)
    for c in started:
        c.wait()


def on_device(right_side, couplings, center, ocean_mask):
    members, rows, columns = right_side.shape
    groups = 128 // members
    sub_rows = rows // groups
    assert columns == 128 and members % 8 == 0 and groups * members == 128
    assert 3 * (rows + 16) <= 256 < 4 * (rows + 16) and 2 * (rows + 16) >= 128 and sub_rows % 16 == 0 and sub_rows >= ITERS
    ny, nx = lax.axis_size("gy"), lax.axis_size("gx")
    vmem = pl.BlockSpec(memory_space=pltpu.VMEM)
    hbm = pl.BlockSpec(memory_space=pltpu.HBM)
    deep, wide = sub_rows + 2 * ITERS, columns + 2 * PAD + 8

    inputs = [
        pltpu.with_memory_space_constraint(v, pltpu.HBM)
        for v in (right_side, couplings, center, ocean_mask)
    ]

    def first(*refs):
        solve_kernel(members, rows, ny, nx, *refs)

    *basis, scale, sums = pl.pallas_call(
        first,
        out_shape=(pltpu.VMEM((deep, wide, 128), F32),) * (ITERS + 1)
        + (pltpu.VMEM((2, 128, 128), F32), pltpu.VMEM((8, 128), F32)),
        in_specs=[hbm] * 4,
        out_specs=(vmem,) * (ITERS + 3),
        scratch_shapes=[
            pltpu.VMEM((deep, wide, 128), F32),
            pltpu.VMEM((5, wide, 128), F32),
            pltpu.VMEM((members, rows + 8, columns), F32),
            pltpu.VMEM((3, rows, columns), F32),
            pltpu.VMEM((rows, columns), F32),
            pltpu.VMEM((rows, columns), jnp.int32),
            pltpu.VMEM((2, 5, 8, columns), F32),
            pltpu.VMEM((2, 5, 8, columns), F32),
            pltpu.VMEM((2, ITERS * members, columns), F32),
            pltpu.VMEM((2, ITERS * members, columns), F32),
            pltpu.VMEM((128, 128), F32),
            pltpu.VMEM((2, wide, 128), F32),
            pltpu.VMEM((wide, 128), F32),
            pltpu.VMEM((5, deep + 3, wide, 128), F32),
            pltpu.VMEM((wide, 128), F32),
            pltpu.VMEM((5 * 144, 256), jnp.bfloat16),
            pltpu.VMEM(((deep + 2) // 2, 256, 256), jnp.bfloat16),
            pltpu.VMEM((8, 128), F32),
            pltpu.VMEM((nx, 8, 128), F32),
            pltpu.VMEM((ny, 8, 128), F32),
            pltpu.SemaphoreType.DMA((4,)),
            pltpu.SemaphoreType.DMA((6 + nx + ny,)),
            pltpu.SemaphoreType.DMA((6 + nx + ny,)),
        ],
        compiler_params=pltpu.CompilerParams(
            collective_id=0, has_side_effects=True, vmem_limit_bytes=GRANT
        ),
    )(*inputs)

    def second(*refs):
        combine_kernel(members, rows, *refs)

    return pl.pallas_call(
        second,
        out_shape=(jax.ShapeDtypeStruct(right_side.shape, F32),) * 2,
        in_specs=[vmem] * (ITERS + 3),
        out_specs=(hbm, hbm),
        compiler_params=pltpu.CompilerParams(vmem_limit_bytes=GRANT),
        scratch_shapes=[
            pltpu.VMEM((2, members, rows + 8, columns), F32),
            pltpu.SemaphoreType.DMA((2, 2, groups)),
        ],
    )(*basis, scale, sums)


def solution(mesh):
    in_specs = (P(None, "gy", "gx"), P(None, "gy", "gx"), P("gy", "gx"), P("gy", "gx"))
    out_specs = (P(None, "gy", "gx"), P(None, "gy", "gx"))
    return jax.shard_map(
        on_device, mesh=mesh, in_specs=in_specs, out_specs=out_specs, check_vma=False
    )
```

```python
import jax
import jax.numpy as jnp
from jax import lax
from jax.experimental import pallas as pl
from jax.experimental.pallas import tpu as pltpu
from jax.sharding import PartitionSpec as P

ITERS = 6
ROOT = 0.28
PAD = 16
VMEM = 67043328
GRANT = 24 * 1024 * 1024
PAIRS = [(i, j) for i in range(ITERS) for j in range(i, ITERS + 1)]
F32 = jnp.float32


def iota(dim):
    return lax.broadcasted_iota(jnp.int32, (8, 128), dim)


def along(x, idx, axis):
    return jnp.take_along_axis(x, idx, axis=axis, mode="promise_in_bounds")


def prepare(members, rows, top, planes, shifted, inv, links, square, lhs, pick):
    first, chunk, tiles = PAD - 8, 48, 18
    lanes = lax.broadcasted_iota(jnp.int32, (chunk, 128), 1)
    seam = lanes == rows + 8
    folded = jnp.logical_and(top, lanes >= rows + 8)
    span = rows + 16
    factor = 1.0 / ROOT

    def before(v):
        return pltpu.roll(v, 1, 1)

    def after(v):
        return pltpu.roll(v, 127, 1)

    for t in range(0, 8 * tiles, chunk):
        at, nxt = slice(first + t, first + t + chunk), slice(first + t + 1, first + t + 1 + chunk)
        for n, p in enumerate((1, 2)):
            shifted[n, at, :] = jnp.where(folded, planes[p, nxt, :], planes[p, at, :])

    @pl.loop(0, 8 * tiles // chunk)
    def _(t):
        at = pl.ds(pl.multiple_of(first + chunk * t, 8), chunk)
        prv = pl.ds(first + chunk * t - 1, chunk)
        cn, ce, cne = planes[0, at, :], shifted[0, at, :], shifted[1, at, :]
        cew, cnw = shifted[0, prv, :], shifted[1, prv, :]
        diag = planes[3, at, :] + cn + ce + cew + cne + cnw + before(cn + cne + cnw)
        ocean = planes[4, at, :] > 0.0
        root = jnp.sqrt(diag)
        recip = jnp.where(ocean, 1.0 / root, 0.0)
        root = jnp.where(ocean, root, 0.0)
        inv[at, :] = jnp.where(seam, after(recip), recip)
        square[at, :] = root

    @pl.loop(0, 8 * tiles // chunk)
    def _(t):
        at = pl.ds(pl.multiple_of(first + chunk * t, 8), chunk)
        nxt = pl.ds(first + chunk * t + 1, chunk)
        here, east = inv[at, :], inv[nxt, :]
        up, up_east = after(here), after(east)
        here_up = jnp.where(seam, before(here), here)
        east_up = jnp.where(seam, before(east), east)
        cn, ce, cne = planes[0, at, :] * factor, shifted[0, at, :] * factor, shifted[1, at, :] * factor
        values = (cn * here_up * up, ce * here * east, cne * here_up * up_east, cne * east_up * up, here)
        for n, v in enumerate(values):
            top_part = v.astype(jnp.bfloat16).astype(F32)
            v = v - top_part
            mid_part = v.astype(jnp.bfloat16).astype(F32)
            moved = pltpu.roll(mid_part, span, 1)
            low_part = pltpu.roll(v - mid_part, 2 * span - 128, 1)
            left = jnp.where(lanes < span, top_part, moved)
            right = jnp.where(lanes < 2 * span - 128, moved, low_part)
            right = jnp.where(lanes < 3 * span - 128, right, 0.0)
            to = pl.ds(pl.multiple_of(8 * tiles * n + chunk * t, 16), chunk)
            lhs[to, 0:128] = left.astype(jnp.bfloat16)
            lhs[to, 128:256] = right.astype(jnp.bfloat16)

    @pl.loop(0, links.shape[1] // 2)
    def _(p):
        found = jnp.dot(lhs[...], pick[p], preferred_element_type=F32)
        for n in range(5):
            for h in range(2):
                links[n, 2 * p + h, first : first + 8 * tiles, :] = found[
                    8 * tiles * n : 8 * tiles * (n + 1), 128 * h : 128 * h + 128
                ]


def choose(members, rows, pick):
    groups = 128 // members
    sub_rows = rows // groups
    span = rows + 16
    source = lax.broadcasted_iota(jnp.int32, (256, 256), 0)
    lane = lax.broadcasted_iota(jnp.int32, (256, 256), 1)
    source = source - span * ((source >= span).astype(jnp.int32) + (source >= 2 * span).astype(jnp.int32))
    group = lax.shift_right_logical(lane & 127, members.bit_length() - 1)
    half = lax.shift_right_logical(lane, 7)
    last = (group == groups - 1).astype(jnp.int32)
    base = source - sub_rows * group - half - 8 + ITERS

    @pl.loop(0, pick.shape[0])
    def _(p):
        later = (2 * p + half >= sub_rows + ITERS).astype(jnp.int32)
        hit = base == 2 * p + later * (last - 1)
        pick[p] = jnp.where(hit, 1.0, 0.0).astype(jnp.bfloat16)


def iterate(members, rows, raw, inv, links, basis, gram_ref):
    groups = 128 // members
    sub_rows = rows // groups
    lanes, subs = iota(1), iota(0)
    group = lax.shift_right_logical(lanes, members.bit_length() - 1)

    @pl.loop(0, sub_rows + 2 * ITERS)
    def _(r):
        c = r + (r >= sub_rows + ITERS).astype(jnp.int32)
        for t in range(18):
            at = slice(PAD - 8 + 8 * t, PAD + 8 * t)
            basis[0][r, at, :] = raw[r, at, :] * links[4, c, at, :]

    for k in range(ITERS):
        depth = ITERS - 1 - k
        here, out = basis[k], basis[k + 1]
        old = basis[k - 1] if k else None

        @pl.loop(0, (128 + 2 * depth + 7) // 8)
        def _(t):
            x0 = PAD - depth + 8 * t
            mid, east, west = pl.ds(x0, 8), pl.ds(x0 + 1, 8), pl.ds(x0 - 1, 8)

            def three(r):
                return here[r, west, :], here[r, mid, :], here[r, east, :]

            start, stop = ITERS - depth, ITERS + sub_rows + depth
            dn, cur = three(start - 1), three(start)
            north = links[0, start - 1, mid, :]
            for r in range(start, stop):
                nxt = three(r + 1)
                c = r + (1 if r >= ITERS + sub_rows else 0)
                if r == ITERS + sub_rows:
                    north = links[0, c - 1, mid, :]
                south, north = north, links[0, c, mid, :]
                total = (north * nxt[1] + south * dn[1]) + (
                    links[1, c, mid, :] * cur[2] + links[1, c, west, :] * cur[0]
                )
                total = total + (links[2, c, mid, :] * nxt[2] + links[2, c - 1, west, :] * dn[0])
                total = total + (links[3, c, west, :] * nxt[0] + links[3, c - 1, mid, :] * dn[2])
                if old is not None:
                    total = total - old[r, mid, :]
                out[r, mid, :] = total
                dn, cur = cur, nxt

    def body(r, sums):
        sums = list(sums)
        for t in range(16):
            at = slice(PAD + 8 * t, PAD + 8 * t + 8)
            vs = [basis[k][r + ITERS, at, :] for k in range(ITERS + 1)]
            for n, (i, j) in enumerate(PAIRS):
                sums[n] = sums[n] + vs[i] * vs[j]
        return tuple(sums)

    zero = jnp.zeros((8, 128), F32)
    sums = lax.fori_loop(0, sub_rows, body, (zero,) * len(PAIRS))
    pack = [zero] * 4
    for n, s in enumerate(sums):
        for step in (1, 2, 4):
            s = s + pltpu.roll(s, step, 0)
        pack[n // 8] = jnp.where(subs == n % 8, s, pack[n // 8])
    total = zero
    for j, v in enumerate(pack):
        width = members
        while width < 128:
            v = v + pltpu.roll(v, width, 1)
            width *= 2
        total = jnp.where(group == j, v, total)
    gram_ref[...] = total


def solve_kernel(members, rows, ny, nx, rhs_hbm, coup_hbm, center_hbm, mask_hbm, *refs):
    basis, (scale_ref, sum_ref) = refs[: ITERS + 1], refs[ITERS + 1 : ITERS + 3]
    (
        field, links, planes, rhs, coup, center, mask, coef_out, coef_in, rows_out, rows_in, strip_out, corner_out, corner_in, ext,
        shifted, inv, square, lhs, pick, gram, along_x, along_y, load, send, recv,
    ) = refs[ITERS + 3 :]
    groups = 128 // members
    sub_rows = rows // groups
    tall = rhs.shape[1]
    y, x = lax.axis_index("gy"), lax.axis_index("gx")
    top = (y + 1) // ny
    mirror = nx - 1 - x
    east, west = lax.rem(x + 1, nx), lax.rem(x + nx - 1, nx)
    up = (y + 1 - top, x + top * (mirror - x))
    down = (jnp.maximum(y - 1, 0), x)
    loads = [
        pltpu.make_async_copy(coup_hbm, coup, load.at[0]),
        pltpu.make_async_copy(center_hbm, center, load.at[1]),
        pltpu.make_async_copy(mask_hbm, mask, load.at[2]),
        pltpu.make_async_copy(rhs_hbm, rhs.at[:, 0:rows, :], load.at[3]),
    ]
    for c in loads:
        c.start()
    barrier = pltpu.get_barrier_semaphore()

    def greet(there):
        pl.semaphore_signal(barrier, inc=1, device_id=there, device_id_type=pl.DeviceIdType.MESH)

    for step in range(1, nx):
        greet((y, lax.rem(x + step, nx)))
    for step in range(1, ny):
        greet((lax.rem(y + step, ny), x))

    @pl.when(y > 0)
    def _():
        greet((y - 1, east))
        greet((y - 1, west))

    @pl.when(top == 0)
    def _():
        greet((y + 1, east))
        greet((y + 1, west))

    def copy(src, dst, n, m, there):
        return pltpu.make_async_remote_copy(
            src_ref=src,
            dst_ref=dst,
            send_sem=send.at[n],
            recv_sem=recv.at[m],
            device_id=there,
            device_id_type=pl.DeviceIdType.MESH,
        )

    def corner(base, parts):
        found = []
        for e in range(2):
            plain, folded = x + 2 * e - 1, mirror + 1 - 2 * e
            to = lax.rem(plain + top * (folded - plain) + nx, nx)
            k = 1 - e + top * (1 + 2 * e)
            c = copy(
                corner_out.at[e, parts], corner_in.at[k, parts], base + e, base + k, (y + 1 - top, to)
            )
            found.append((jnp.logical_or(top == 0, to != x), c, e, k))
        for e in range(2):
            k = 3 - e
            there = (jnp.maximum(y - 1, 0), east if e else west)
            c = copy(
                corner_out.at[2 + e, parts], corner_in.at[k, parts], base + 2 + e, base + k, there
            )
            found.append((y > 0, c, 2 + e, k))
        return found

    def start_corners(found, parts):
        for n, (remote, c, e, k) in enumerate(found):
            pl.when(remote)(c.start)
            if n < 2:

                @pl.when(jnp.logical_not(remote))
                def _():
                    corner_in[k, parts] = corner_out[e, parts]

    def corner_arrivals(found, base, parts):
        for k in range(4):
            c = copy(corner_out.at[0, parts], corner_in.at[k, parts], base, base + k, (y, east))
            pl.when(y > 0 if k < 2 else found[k - 2][0])(c.wait_recv)

    lanes, subs = iota(1), iota(0)
    flip_lane = jnp.where(top == 1, 127 - lanes, lanes)
    flip_sub = jnp.where(top == 1, 7 - subs, subs)
    tiles = (slice(PAD, PAD + 8), slice(PAD + 120, PAD + 128))
    beyond_tiles = (slice(PAD - 8, PAD), slice(PAD + 128, PAD + 136))
    for c in loads[:3]:
        c.wait()

    def own(p, at):
        if p < 3:
            return coup[p, at, :]
        return center[at, :] if p == 3 else mask[at, :].astype(F32)

    packs = [jnp.zeros((8, 128), F32)] * 4
    plane = lax.shift_right_logical(lanes, 3)
    high_lanes = jnp.where(top == 1, rows + 7 - (lanes & 7), rows + (lanes & 7))
    low_lanes = 8 + (lanes & 7)
    ext[0:8, :] = jnp.zeros((8, 128), F32)
    ext[rows + 8 : 128, :] = jnp.zeros((120 - rows, 128), F32)
    for p in range(5):
        coef_out[0, p] = along(along(own(p, slice(rows - 8, rows)), flip_lane, 1), flip_sub, 0)
        coef_out[1, p] = own(p, slice(0, 8))
        ext[8 : rows + 8, :] = own(p, slice(0, rows))
        turned = ext[...].T
        for e, edge in enumerate((turned[0:8], turned[120:128])):
            strip_out[e, p] = edge
            packs[e] = jnp.where(plane == p, along(edge, high_lanes, 1), packs[e])
            packs[2 + e] = jnp.where(plane == p, along(edge, low_lanes, 1), packs[2 + e])
    for e in range(4):
        corner_out[e, 0] = along(packs[e], flip_sub, 0) if e < 2 else packs[e]
    choose(members, rows, pick)
    pl.semaphore_wait(barrier, nx + ny - 2 + 2 * (1 - top) + 2 * jnp.minimum(y, 1))
    coef_up = copy(coef_out.at[0], coef_in.at[top], 0, top, up)
    coef_down = copy(coef_out.at[1], coef_in.at[1], 1, 1, down)
    rows_up = copy(rows_out.at[0], rows_in.at[top], 2, 2 + top, up)
    rows_down = copy(rows_out.at[1], rows_in.at[1], 3, 3, down)
    first = slice(0, 1)
    later = slice(1, 3)
    coef_corners, rows_corners = corner(8, first), corner(12, later)
    sides = [
        copy(strip_out.at[0], planes.at[:, PAD + 128 : PAD + 136, :], 4, 4, (y, west)),
        copy(strip_out.at[1], planes.at[:, PAD - 8 : PAD, :], 5, 5, (y, east)),
    ]
    start_corners(coef_corners, first)
    coef_up.start()
    pl.when(y > 0)(coef_down.start)
    for c in sides:
        c.start()
    flat = rhs.reshape(members * tall, 128)

    def column(row, block):
        return flat[pl.ds(8 * block * tall + row, 8, stride=tall), :]

    blocks = members // 8
    loads[3].wait()
    for q in range(ITERS):
        high = rows - ITERS + q + top * (ITERS - 1 - 2 * q)
        for b in range(blocks):
            at = slice(q * members + 8 * b, q * members + 8 * b + 8)
            rows_out[0, at, :] = along(column(high, b), flip_lane, 1)
            rows_out[1, at, :] = column(q, b)

    @pl.loop(0, sub_rows)
    def _(r):
        stack = [column(sub_rows * g + r, b) for g in range(groups) for b in range(blocks)]
        field[r + ITERS, PAD : PAD + 128, :] = jnp.concatenate(stack, axis=0).T

    member = lanes & (members - 1)
    group = lax.shift_right_logical(lanes, members.bit_length() - 1)
    for e in range(2):
        packs = [[jnp.zeros((8, 128), F32)] * 2 for _ in range(2)]
        for q in range(ITERS):
            here = group == q % groups
            v = field[sub_rows + q + top * (ITERS - 1 - 2 * q), tiles[e], :]
            v = along(v, member + (128 - members), 1)
            packs[0][q // groups] = jnp.where(here, v, packs[0][q // groups])
            v = along(field[ITERS + q, tiles[e], :], member, 1)
            packs[1][q // groups] = jnp.where(here, v, packs[1][q // groups])
        for n in range(2):
            corner_out[e, 1 + n] = along(packs[0][n], flip_sub, 0)
            corner_out[2 + e, 1 + n] = packs[1][n]
    inner = slice(ITERS, ITERS + sub_rows)
    more = [
        copy(field.at[inner, tiles[0], :], field.at[inner, beyond_tiles[1], :], 6, 6, (y, west)),
        copy(field.at[inner, tiles[1], :], field.at[inner, beyond_tiles[0], :], 7, 7, (y, east)),
    ]
    start_corners(rows_corners, later)
    rows_up.start()
    pl.when(y > 0)(rows_down.start)
    for c in more:
        c.start()
    coef_north = copy(coef_out.at[1], coef_in.at[1], 1, 1, down)
    coef_south = copy(coef_out.at[0], coef_in.at[0], 0, 0, up)
    coef_north.wait_recv()
    pl.when(y > 0)(coef_south.wait_recv)
    for p in range(5):
        beyond = coef_in[1, p]
        moved = pltpu.roll(beyond, 1, 0)
        if p in (0, 2):
            last = jnp.broadcast_to(own(p, slice(rows - 1, rows)), (8, 128))
            beyond = jnp.where(top == 1, beyond, jnp.where(subs == 0, last, moved))
        else:
            beyond = jnp.where(subs == 0, beyond, moved)
        ext[0:8, :] = jnp.where(y == 0, 0.0, coef_in[0, p])
        ext[8 : rows + 8, :] = own(p, slice(0, rows))
        ext[rows + 8 : rows + 16, :] = beyond
        planes[p, PAD : PAD + 128, :] = ext[...].T
    for c in sides:
        c.wait_recv()
    corner_arrivals(coef_corners, 8, first)
    for e in range(2):
        low, high = corner_in[e, 0], corner_in[2 + e, 0]
        for p in range(5):
            strip = planes[p, beyond_tiles[e], :]
            shift = 1 - top if p in (0, 2) else 1
            idx = jnp.clip(lanes - (rows + 8) - shift, 0, 7) + 8 * p
            north = along(high, idx, 1)
            if p in (0, 2):
                joint = jnp.logical_and(lanes == rows + 8, top == 0)
                north = jnp.where(joint, pltpu.roll(strip, 1, 1), north)
            south = jnp.where(y == 0, 0.0, along(low, (lanes & 7) + 8 * p, 1))
            outside = jnp.logical_and(lanes >= rows + 8, lanes < rows + 16)
            strip = jnp.where(lanes < 8, south, jnp.where(outside, north, strip))
            planes[p, beyond_tiles[e], :] = strip
    prepare(members, rows, y == ny - 1, planes, shifted, inv, links, square, lhs, pick)
    copy(rows_out.at[1], rows_in.at[1], 3, 3, down).wait_recv()
    pl.when(y > 0)(copy(rows_out.at[0], rows_in.at[0], 2, 2, up).wait_recv)

    @pl.loop(0, ITERS)
    def _(q):
        def arrived(side, b):
            return rows_in[side, pl.ds(pl.multiple_of(q * members, 8) + 8 * b, 8), :]

        low = [jnp.where(y == 0, 0.0, arrived(0, b)) for b in range(blocks)]
        low += [column(sub_rows * g - ITERS + q, b) for g in range(1, groups) for b in range(blocks)]
        field[q, PAD : PAD + 128, :] = jnp.concatenate(low, axis=0).T
        high = [column(sub_rows * g + q, b) for g in range(1, groups) for b in range(blocks)]
        high += [arrived(1, b) for b in range(blocks)]
        field[q + ITERS + sub_rows, PAD : PAD + 128, :] = jnp.concatenate(high, axis=0).T

    for c in more:
        c.wait_recv()
    corner_arrivals(rows_corners, 12, later)
    for e in range(2):
        for q in range(ITERS):
            idx = member + members * (q % groups)
            south = along(corner_in[e, 1 + q // groups], idx, 1)
            south = jnp.where(y == 0, 0.0, south)
            v = pltpu.roll(field[sub_rows + q, beyond_tiles[e], :], members, 1)
            field[q, beyond_tiles[e], :] = jnp.where(group == 0, south, v)
            north = along(corner_in[2 + e, 1 + q // groups], idx, 1)
            v = pltpu.roll(field[ITERS + q, beyond_tiles[e], :], 128 - members, 1)
            field[ITERS + sub_rows + q, beyond_tiles[e], :] = jnp.where(group == groups - 1, north, v)
    coef_up.wait_send()
    rows_up.wait_send()

    @pl.when(y > 0)
    def _():
        coef_down.wait_send()
        rows_down.wait_send()

    for c in sides + more:
        c.wait_send()
    for remote, c, _, _ in coef_corners + rows_corners:
        pl.when(remote)(c.wait_send)
    iterate(members, rows, field, inv, links, basis, gram)

    def sent(source, dst, n, there):
        c = copy(source, dst, n, n, there)
        c.start()
        return c

    across = [sent(gram, along_x.at[s], 15 + s, (y, lax.rem(x + s, nx))) for s in range(1, nx)]
    scale_ref[0] = inv[PAD : PAD + 128, :].T
    scale_ref[1] = square[PAD : PAD + 128, :].T
    for c in across:
        c.wait()
    along_x[0] = sum((along_x[s] for s in range(1, nx)), gram[...])
    across = [
        sent(along_x.at[0], along_y.at[s], 14 + nx + s, (lax.rem(y + s, ny), x)) for s in range(1, ny)
    ]
    for c in across:
        c.wait()
    sum_ref[...] = sum((along_y[s] for s in range(1, ny)), along_x[0])


def coefficients(gram):
    def g(i, j):
        return gram[min(i, j)][max(i, j)]

    def applied(p):
        q = []
        for k in range(ITERS + 1):
            terms = []
            if k < len(p):
                terms.append(p[k])
            if 0 < k <= len(p):
                terms.append(-ROOT * p[k - 1])
            if k + 1 < len(p):
                terms.append(-ROOT * p[k + 1])
            if terms:
                q.append(sum(terms[1:], terms[0]))
        return q

    def inner(p, q):
        total = None
        for i, a in enumerate(p):
            row = None
            for j, b in enumerate(q):
                t = g(i, j) * b
                row = t if row is None else row + t
            t = a * row
            total = t if total is None else total + t
        return total

    one = jnp.ones_like(gram[0][0])
    z, p, x = [one], [one], []
    rz = g(0, 0)
    for iteration in range(ITERS):
        q = applied(p)
        step = rz / inner(p, q)
        x = [(x[k] if k < len(x) else 0.0) + step * p[k] for k in range(len(p))]
        z = [(z[k] if k < len(z) else 0.0) - step * q[k] for k in range(len(q))]
        if iteration + 1 < ITERS:
            rz_new = inner(z, z)
            beta = rz_new / rz
            p = [z[k] + (beta * p[k] if k < len(p) else 0.0) for k in range(len(z))]
            rz = rz_new
    return x, z


def combine_kernel(members, rows, *refs):
    basis, (scale_ref, sum_ref, x_out, r_out, stage, sems) = refs[: ITERS + 1], refs[ITERS + 1 :]
    groups = 128 // members
    sub_rows = rows // groups
    tall = stage.shape[2]
    lanes = iota(1)
    sums = sum_ref[...]
    tiles = [along(sums, (lanes & (members - 1)) + members * j, 1) for j in range(4)]
    gram = [[None] * (ITERS + 1) for _ in range(ITERS + 1)]
    for n, (i, j) in enumerate(PAIRS):
        gram[i][j] = jnp.broadcast_to(tiles[n // 8][n % 8 : n % 8 + 1, :], (8, 128))
    xs, zs = coefficients(gram)
    flat = stage.reshape(2 * members * tall, 128)
    blocks = members // 8
    half = sub_rows // 2
    outs = (x_out, r_out)

    def drain(h):
        copies = []
        for o in range(2):
            for g in range(groups):
                at = slice(sub_rows * g + half * h, sub_rows * g + half * (h + 1))
                copies.append(
                    pltpu.make_async_copy(stage.at[o, :, at, :], outs[o].at[:, at, :], sems.at[h, o, g])
                )
        return copies

    started = []
    for h in range(2):

        @pl.loop(half * h, half * (h + 1))
        def _(r):
            found = ([], [])
            for t in range(16):
                at = slice(PAD + 8 * t, PAD + 8 * t + 8)
                vs = [basis[k][r + ITERS, at, :] for k in range(ITERS + 1)]
                found[0].append(sum((xs[k] * vs[k] for k in range(1, ITERS)), xs[0] * vs[0]))
                found[1].append(sum((zs[k] * vs[k] for k in range(1, ITERS + 1)), zs[0] * vs[0]))
            for o in range(2):
                turned = jnp.concatenate(found[o], axis=0).T
                for g in range(groups):
                    row = sub_rows * g + r
                    scale = jnp.broadcast_to(scale_ref[o, pl.ds(row + 8, 1), :], (8, 128))
                    for b in range(blocks):
                        n = 8 * (g * blocks + b)
                        at = pl.ds((o * members + 8 * b) * tall + row, 8, stride=tall)
                        flat[at, :] = turned[n : n + 8, :] * scale

        for c in drain(h):
            c.start()
            started.append(c)
    for c in started:
        c.wait()


def on_device(right_side, couplings, center, ocean_mask):
    members, rows, columns = right_side.shape
    groups = 128 // members
    sub_rows = rows // groups
    assert lax.axis_size("gx") > 2 and ITERS <= 2 * groups
    assert columns == 128 and members % 8 == 0 and groups * members == 128
    assert 3 * (rows + 16) <= 256 < 4 * (rows + 16) and 2 * (rows + 16) >= 128 and sub_rows % 16 == 0 and sub_rows >= ITERS
    ny, nx = lax.axis_size("gy"), lax.axis_size("gx")
    vmem = pl.BlockSpec(memory_space=pltpu.VMEM)
    hbm = pl.BlockSpec(memory_space=pltpu.HBM)
    deep, wide = sub_rows + 2 * ITERS, columns + 2 * PAD + 8

    inputs = [
        pltpu.with_memory_space_constraint(v, pltpu.HBM)
        for v in (right_side, couplings, center, ocean_mask)
    ]

    def first(*refs):
        solve_kernel(members, rows, ny, nx, *refs)

    *basis, scale, sums = pl.pallas_call(
        first,
        out_shape=(pltpu.VMEM((deep, wide, 128), F32),) * (ITERS + 1)
        + (pltpu.VMEM((2, 128, 128), F32), pltpu.VMEM((8, 128), F32)),
        in_specs=[hbm] * 4,
        out_specs=(vmem,) * (ITERS + 3),
        scratch_shapes=[
            pltpu.VMEM((deep, wide, 128), F32),
            pltpu.VMEM((5, deep + 3, wide, 128), F32),
            pltpu.VMEM((5, wide, 128), F32),
            pltpu.VMEM((members, rows + 8, columns), F32),
            pltpu.VMEM((3, rows, columns), F32),
            pltpu.VMEM((rows, columns), F32),
            pltpu.VMEM((rows, columns), jnp.int32),
            pltpu.VMEM((2, 5, 8, columns), F32),
            pltpu.VMEM((2, 5, 8, columns), F32),
            pltpu.VMEM((2, ITERS * members, columns), F32),
            pltpu.VMEM((2, ITERS * members, columns), F32),
            pltpu.VMEM((2, 5, 8, 128), F32),
            pltpu.VMEM((4, 3, 8, 128), F32),
            pltpu.VMEM((4, 3, 8, 128), F32),
            pltpu.VMEM((128, 128), F32),
            pltpu.VMEM((2, wide, 128), F32),
            pltpu.VMEM((wide, 128), F32),
            pltpu.VMEM((wide, 128), F32),
            pltpu.VMEM((5 * 144, 256), jnp.bfloat16),
            pltpu.VMEM(((deep + 2) // 2, 256, 256), jnp.bfloat16),
            pltpu.VMEM((8, 128), F32),
            pltpu.VMEM((nx, 8, 128), F32),
            pltpu.VMEM((ny, 8, 128), F32),
            pltpu.SemaphoreType.DMA((4,)),
            pltpu.SemaphoreType.DMA((14 + nx + ny,)),
            pltpu.SemaphoreType.DMA((14 + nx + ny,)),
        ],
        compiler_params=pltpu.CompilerParams(
            collective_id=0, has_side_effects=True, vmem_limit_bytes=GRANT
        ),
    )(*inputs)

    def second(*refs):
        combine_kernel(members, rows, *refs)

    return pl.pallas_call(
        second,
        out_shape=(jax.ShapeDtypeStruct(right_side.shape, F32),) * 2,
        in_specs=[vmem] * (ITERS + 3),
        out_specs=(hbm, hbm),
        compiler_params=pltpu.CompilerParams(vmem_limit_bytes=GRANT),
        scratch_shapes=[
            pltpu.VMEM((2, members, rows + 8, columns), F32),
            pltpu.SemaphoreType.DMA((2, 2, groups)),
        ],
    )(*basis, scale, sums)


def solution(mesh):
    in_specs = (P(None, "gy", "gx"), P(None, "gy", "gx"), P("gy", "gx"), P("gy", "gx"))
    out_specs = (P(None, "gy", "gx"), P(None, "gy", "gx"))
    return jax.shard_map(
        on_device, mesh=mesh, in_specs=in_specs, out_specs=out_specs, check_vma=False
    )
```

```python
import jax
import jax.numpy as jnp
from jax import lax
from jax.experimental import pallas as pl
from jax.experimental.pallas import tpu as pltpu
from jax.sharding import PartitionSpec as P

ITERS = 6
ROOT = 0.28
PAD = 16
VMEM = 67043328
GRANT = 24 * 1024 * 1024
PAIRS = [(i, j) for i in range(ITERS) for j in range(i, ITERS + 1)]
F32 = jnp.float32


def iota(dim):
    return lax.broadcasted_iota(jnp.int32, (8, 128), dim)


def along(x, idx, axis):
    return jnp.take_along_axis(x, idx, axis=axis, mode="promise_in_bounds")


def prepare(members, rows, top, planes, shifted, inv, links, square, lhs, pick):
    first, chunk, tiles = PAD - 8, 48, 18
    lanes = lax.broadcasted_iota(jnp.int32, (chunk, 128), 1)
    seam = lanes == rows + 8
    folded = jnp.logical_and(top, lanes >= rows + 8)
    span = rows + 16
    factor = 1.0 / ROOT

    def before(v):
        return pltpu.roll(v, 1, 1)

    def after(v):
        return pltpu.roll(v, 127, 1)

    for t in range(0, 8 * tiles, chunk):
        at, nxt = slice(first + t, first + t + chunk), slice(first + t + 1, first + t + 1 + chunk)
        for n, p in enumerate((1, 2)):
            shifted[n, at, :] = jnp.where(folded, planes[p, nxt, :], planes[p, at, :])

    @pl.loop(0, 8 * tiles // chunk)
    def _(t):
        at = pl.ds(pl.multiple_of(first + chunk * t, 8), chunk)
        prv = pl.ds(first + chunk * t - 1, chunk)
        cn, ce, cne = planes[0, at, :], shifted[0, at, :], shifted[1, at, :]
        cew, cnw = shifted[0, prv, :], shifted[1, prv, :]
        diag = planes[3, at, :] + cn + ce + cew + cne + cnw + before(cn + cne + cnw)
        ocean = planes[4, at, :] > 0.0
        root = jnp.sqrt(diag)
        recip = jnp.where(ocean, 1.0 / root, 0.0)
        root = jnp.where(ocean, root, 0.0)
        inv[at, :] = jnp.where(seam, after(recip), recip)
        square[at, :] = root

    @pl.loop(0, 8 * tiles // chunk)
    def _(t):
        at = pl.ds(pl.multiple_of(first + chunk * t, 8), chunk)
        nxt = pl.ds(first + chunk * t + 1, chunk)
        here, east = inv[at, :], inv[nxt, :]
        up, up_east = after(here), after(east)
        here_up = jnp.where(seam, before(here), here)
        east_up = jnp.where(seam, before(east), east)
        cn, ce, cne = planes[0, at, :] * factor, shifted[0, at, :] * factor, shifted[1, at, :] * factor
        values = (cn * here_up * up, ce * here * east, cne * here_up * up_east, cne * east_up * up, here)
        for n, v in enumerate(values):
            top_part = v.astype(jnp.bfloat16).astype(F32)
            v = v - top_part
            mid_part = v.astype(jnp.bfloat16).astype(F32)
            moved = pltpu.roll(mid_part, span, 1)
            low_part = pltpu.roll(v - mid_part, 2 * span - 128, 1)
            left = jnp.where(lanes < span, top_part, moved)
            right = jnp.where(lanes < 2 * span - 128, moved, low_part)
            right = jnp.where(lanes < 3 * span - 128, right, 0.0)
            to = pl.ds(pl.multiple_of(8 * tiles * n + chunk * t, 16), chunk)
            lhs[to, 0:128] = left.astype(jnp.bfloat16)
            lhs[to, 128:256] = right.astype(jnp.bfloat16)

    def spread(p, planes_from, halves):
        found = jnp.dot(lhs[8 * tiles * planes_from :, :], pick[p], preferred_element_type=F32)
        for n in range(planes_from, 5):
            for h in range(halves):
                at = 8 * tiles * (n - planes_from)
                links[n, 2 * p + h, first : first + 8 * tiles, :] = found[
                    at : at + 8 * tiles, 128 * h : 128 * h + 128
                ]

    pairs = pick.shape[0] - 1
    together = 2 - pairs % 2

    @pl.loop(0, pairs // together)
    def _(part):
        for within in range(together):
            spread(together * part + within, 0, 2)

    spread(pairs, 4, 1)


def choose(members, rows, pick):
    groups = 128 // members
    sub_rows = rows // groups
    span = rows + 16
    source = lax.broadcasted_iota(jnp.int32, (256, 256), 0)
    lane = lax.broadcasted_iota(jnp.int32, (256, 256), 1)
    source = source - span * ((source >= span).astype(jnp.int32) + (source >= 2 * span).astype(jnp.int32))
    group = lax.shift_right_logical(lane & 127, members.bit_length() - 1)
    half = lax.shift_right_logical(lane, 7)
    last = (group == groups - 1).astype(jnp.int32)
    base = source - sub_rows * group - half - 8 + ITERS

    @pl.loop(0, pick.shape[0])
    def _(p):
        later = (2 * p + half >= sub_rows + ITERS).astype(jnp.int32)
        hit = base == 2 * p + later * (last - 1)
        pick[p] = jnp.where(hit, 1.0, 0.0).astype(jnp.bfloat16)


def iterate(members, rows, raw, inv, links, basis, gram_ref):
    groups = 128 // members
    sub_rows = rows // groups
    lanes, subs = iota(1), iota(0)
    group = lax.shift_right_logical(lanes, members.bit_length() - 1)

    @pl.loop(0, sub_rows + 2 * ITERS)
    def _(r):
        c = r + (r >= sub_rows + ITERS).astype(jnp.int32)
        for t in range(18):
            at = slice(PAD - 8 + 8 * t, PAD + 8 * t)
            basis[0][r, at, :] = raw[r, at, :] * links[4, c, at, :]

    for k in range(ITERS):
        depth = ITERS - 1 - k
        here, out = basis[k], basis[k + 1]
        old = basis[k - 1] if k else None

        @pl.loop(0, (128 + 2 * depth + 7) // 8)
        def _(t):
            x0 = PAD - depth + 8 * t
            mid, east, west = pl.ds(x0, 8), pl.ds(x0 + 1, 8), pl.ds(x0 - 1, 8)

            def three(r):
                return here[r, west, :], here[r, mid, :], here[r, east, :]

            start, stop = ITERS - depth, ITERS + sub_rows + depth
            dn, cur = three(start - 1), three(start)
            north = links[0, start - 1, mid, :]
            for r in range(start, stop):
                nxt = three(r + 1)
                c = r + (1 if r >= ITERS + sub_rows else 0)
                if r == ITERS + sub_rows:
                    north = links[0, c - 1, mid, :]
                south, north = north, links[0, c, mid, :]
                total = (north * nxt[1] + south * dn[1]) + (
                    links[1, c, mid, :] * cur[2] + links[1, c, west, :] * cur[0]
                )
                total = total + (links[2, c, mid, :] * nxt[2] + links[2, c - 1, west, :] * dn[0])
                total = total + (links[3, c, west, :] * nxt[0] + links[3, c - 1, mid, :] * dn[2])
                if old is not None:
                    total = total - old[r, mid, :]
                out[r, mid, :] = total
                dn, cur = cur, nxt

    def body(r, sums):
        sums = list(sums)
        for t in range(16):
            at = slice(PAD + 8 * t, PAD + 8 * t + 8)
            vs = [basis[k][r + ITERS, at, :] for k in range(ITERS + 1)]
            for n, (i, j) in enumerate(PAIRS):
                sums[n] = sums[n] + vs[i] * vs[j]
        return tuple(sums)

    zero = jnp.zeros((8, 128), F32)
    sums = lax.fori_loop(0, sub_rows, body, (zero,) * len(PAIRS))
    pack = [zero] * 4
    for n, s in enumerate(sums):
        for step in (1, 2, 4):
            s = s + pltpu.roll(s, step, 0)
        pack[n // 8] = jnp.where(subs == n % 8, s, pack[n // 8])
    total = zero
    for j, v in enumerate(pack):
        width = members
        while width < 128:
            v = v + pltpu.roll(v, width, 1)
            width *= 2
        total = jnp.where(group == j, v, total)
    gram_ref[...] = total


def solve_kernel(members, rows, ny, nx, rhs_hbm, coup_hbm, center_hbm, mask_hbm, *refs):
    basis, (scale_ref, sum_ref) = refs[: ITERS + 1], refs[ITERS + 1 : ITERS + 3]
    (
        field, links, planes, rhs, coup, center, mask, coef_out, coef_in, rows_out, rows_in, strip_out, corner_out, corner_in, ext,
        shifted, inv, square, lhs, pick, gram, along_x, along_y, load, send, recv,
    ) = refs[ITERS + 3 :]
    groups = 128 // members
    sub_rows = rows // groups
    tall = rhs.shape[1]
    y, x = lax.axis_index("gy"), lax.axis_index("gx")
    top = (y + 1) // ny
    mirror = nx - 1 - x
    east, west = lax.rem(x + 1, nx), lax.rem(x + nx - 1, nx)
    up = (y + 1 - top, x + top * (mirror - x))
    down = (jnp.maximum(y - 1, 0), x)
    loads = [
        pltpu.make_async_copy(coup_hbm, coup, load.at[0]),
        pltpu.make_async_copy(center_hbm, center, load.at[1]),
        pltpu.make_async_copy(mask_hbm, mask, load.at[2]),
        pltpu.make_async_copy(rhs_hbm, rhs.at[:, 0:rows, :], load.at[3]),
    ]
    for c in loads:
        c.start()
    barrier = pltpu.get_barrier_semaphore()

    def greet(there):
        pl.semaphore_signal(barrier, inc=1, device_id=there, device_id_type=pl.DeviceIdType.MESH)

    for step in range(1, nx):
        greet((y, lax.rem(x + step, nx)))
    for step in range(1, ny):
        greet((lax.rem(y + step, ny), x))

    @pl.when(y > 0)
    def _():
        greet((y - 1, east))
        greet((y - 1, west))

    @pl.when(top == 0)
    def _():
        greet((y + 1, east))
        greet((y + 1, west))

    def copy(src, dst, n, m, there):
        return pltpu.make_async_remote_copy(
            src_ref=src,
            dst_ref=dst,
            send_sem=send.at[n],
            recv_sem=recv.at[m],
            device_id=there,
            device_id_type=pl.DeviceIdType.MESH,
        )

    def corner(base, parts):
        found = []
        for e in range(2):
            plain, folded = x + 2 * e - 1, mirror + 1 - 2 * e
            to = lax.rem(plain + top * (folded - plain) + nx, nx)
            k = 1 - e + top * (1 + 2 * e)
            c = copy(
                corner_out.at[e, parts], corner_in.at[k, parts], base + e, base + k, (y + 1 - top, to)
            )
            found.append((jnp.logical_or(top == 0, to != x), c, e, k))
        for e in range(2):
            k = 3 - e
            there = (jnp.maximum(y - 1, 0), east if e else west)
            c = copy(
                corner_out.at[2 + e, parts], corner_in.at[k, parts], base + 2 + e, base + k, there
            )
            found.append((y > 0, c, 2 + e, k))
        return found

    def start_corners(found, parts):
        for n, (remote, c, e, k) in enumerate(found):
            pl.when(remote)(c.start)
            if n < 2:

                @pl.when(jnp.logical_not(remote))
                def _():
                    corner_in[k, parts] = corner_out[e, parts]

    def corner_arrivals(found, base, parts):
        for k in range(4):
            c = copy(corner_out.at[0, parts], corner_in.at[k, parts], base, base + k, (y, east))
            pl.when(y > 0 if k < 2 else found[k - 2][0])(c.wait_recv)

    lanes, subs = iota(1), iota(0)
    flip_lane = jnp.where(top == 1, 127 - lanes, lanes)
    flip_sub = jnp.where(top == 1, 7 - subs, subs)
    tiles = (slice(PAD, PAD + 8), slice(PAD + 120, PAD + 128))
    beyond_tiles = (slice(PAD - 8, PAD), slice(PAD + 128, PAD + 136))
    for c in loads[:3]:
        c.wait()

    def own(p, at):
        if p < 3:
            return coup[p, at, :]
        return center[at, :] if p == 3 else mask[at, :].astype(F32)

    packs = [jnp.zeros((8, 128), F32)] * 4
    plane = lax.shift_right_logical(lanes, 3)
    high_lanes = jnp.where(top == 1, rows + 7 - (lanes & 7), rows + (lanes & 7))
    low_lanes = 8 + (lanes & 7)
    ext[0:8, :] = jnp.zeros((8, 128), F32)
    ext[rows + 8 : 128, :] = jnp.zeros((120 - rows, 128), F32)
    for p in range(5):
        coef_out[0, p] = along(along(own(p, slice(rows - 8, rows)), flip_lane, 1), flip_sub, 0)
        coef_out[1, p] = own(p, slice(0, 8))
        ext[8 : rows + 8, :] = own(p, slice(0, rows))
        turned = ext[...].T
        for e, edge in enumerate((turned[0:8], turned[120:128])):
            strip_out[e, p] = edge
            packs[e] = jnp.where(plane == p, along(edge, high_lanes, 1), packs[e])
            packs[2 + e] = jnp.where(plane == p, along(edge, low_lanes, 1), packs[2 + e])
    for e in range(4):
        corner_out[e, 0] = along(packs[e], flip_sub, 0) if e < 2 else packs[e]
    pl.semaphore_wait(barrier, nx + ny - 2 + 2 * (1 - top) + 2 * jnp.minimum(y, 1))
    coef_up = copy(coef_out.at[0], coef_in.at[top], 0, top, up)
    coef_down = copy(coef_out.at[1], coef_in.at[1], 1, 1, down)
    rows_up = copy(rows_out.at[0], rows_in.at[top], 2, 2 + top, up)
    rows_down = copy(rows_out.at[1], rows_in.at[1], 3, 3, down)
    first = slice(0, 1)
    later = slice(1, 3)
    coef_corners, rows_corners = corner(8, first), corner(12, later)
    sides = [
        copy(strip_out.at[0], planes.at[:, PAD + 128 : PAD + 136, :], 4, 4, (y, west)),
        copy(strip_out.at[1], planes.at[:, PAD - 8 : PAD, :], 5, 5, (y, east)),
    ]
    start_corners(coef_corners, first)
    coef_up.start()
    pl.when(y > 0)(coef_down.start)
    for c in sides:
        c.start()
    flat = rhs.reshape(members * tall, 128)

    def column(row, block):
        return flat[pl.ds(8 * block * tall + row, 8, stride=tall), :]

    blocks = members // 8
    loads[3].wait()
    for q in range(ITERS):
        high = rows - ITERS + q + top * (ITERS - 1 - 2 * q)
        for b in range(blocks):
            at = slice(q * members + 8 * b, q * members + 8 * b + 8)
            rows_out[0, at, :] = along(column(high, b), flip_lane, 1)
            rows_out[1, at, :] = column(q, b)

    @pl.loop(0, sub_rows // 4)
    def _(part):
        for within in range(4):
            r = 4 * part + within
            stack = [column(sub_rows * g + r, b) for g in range(groups) for b in range(blocks)]
            field[r + ITERS, PAD : PAD + 128, :] = jnp.concatenate(stack, axis=0).T

    member = lanes & (members - 1)
    group = lax.shift_right_logical(lanes, members.bit_length() - 1)
    for e in range(2):
        packs = [[jnp.zeros((8, 128), F32)] * 2 for _ in range(2)]
        for q in range(ITERS):
            here = group == q % groups
            v = field[sub_rows + q + top * (ITERS - 1 - 2 * q), tiles[e], :]
            v = along(v, member + (128 - members), 1)
            packs[0][q // groups] = jnp.where(here, v, packs[0][q // groups])
            v = along(field[ITERS + q, tiles[e], :], member, 1)
            packs[1][q // groups] = jnp.where(here, v, packs[1][q // groups])
        for n in range(2):
            corner_out[e, 1 + n] = along(packs[0][n], flip_sub, 0)
            corner_out[2 + e, 1 + n] = packs[1][n]
    inner = slice(ITERS, ITERS + sub_rows)
    more = [
        copy(field.at[inner, tiles[0], :], field.at[inner, beyond_tiles[1], :], 6, 6, (y, west)),
        copy(field.at[inner, tiles[1], :], field.at[inner, beyond_tiles[0], :], 7, 7, (y, east)),
    ]
    start_corners(rows_corners, later)
    for c in more:
        c.start()
    choose(members, rows, pick)
    coef_north = copy(coef_out.at[1], coef_in.at[1], 1, 1, down)
    coef_south = copy(coef_out.at[0], coef_in.at[0], 0, 0, up)
    coef_north.wait_recv()
    pl.when(y > 0)(coef_south.wait_recv)
    rows_up.start()
    pl.when(y > 0)(rows_down.start)
    for p in range(5):
        beyond = coef_in[1, p]
        moved = pltpu.roll(beyond, 1, 0)
        if p in (0, 2):
            last = jnp.broadcast_to(own(p, slice(rows - 1, rows)), (8, 128))
            beyond = jnp.where(top == 1, beyond, jnp.where(subs == 0, last, moved))
        else:
            beyond = jnp.where(subs == 0, beyond, moved)
        ext[0:8, :] = jnp.where(y == 0, 0.0, coef_in[0, p])
        ext[8 : rows + 8, :] = own(p, slice(0, rows))
        ext[rows + 8 : rows + 16, :] = beyond
        planes[p, PAD : PAD + 128, :] = ext[...].T
    for c in sides:
        c.wait_recv()
    corner_arrivals(coef_corners, 8, first)
    for e in range(2):
        low, high = corner_in[e, 0], corner_in[2 + e, 0]
        for p in range(5):
            strip = planes[p, beyond_tiles[e], :]
            shift = 1 - top if p in (0, 2) else 1
            idx = jnp.clip(lanes - (rows + 8) - shift, 0, 7) + 8 * p
            north = along(high, idx, 1)
            if p in (0, 2):
                joint = jnp.logical_and(lanes == rows + 8, top == 0)
                north = jnp.where(joint, pltpu.roll(strip, 1, 1), north)
            south = jnp.where(y == 0, 0.0, along(low, (lanes & 7) + 8 * p, 1))
            outside = jnp.logical_and(lanes >= rows + 8, lanes < rows + 16)
            strip = jnp.where(lanes < 8, south, jnp.where(outside, north, strip))
            planes[p, beyond_tiles[e], :] = strip
    prepare(members, rows, y == ny - 1, planes, shifted, inv, links, square, lhs, pick)
    copy(rows_out.at[1], rows_in.at[1], 3, 3, down).wait_recv()
    pl.when(y > 0)(copy(rows_out.at[0], rows_in.at[0], 2, 2, up).wait_recv)

    def arrived(side, q, b):
        return rows_in[side, pl.ds(pl.multiple_of(q * members, 8) + 8 * b, 8), :]

    @pl.loop(0, ITERS // 2)
    def _(part):
        for within in range(2):
            q = 2 * part + within
            low = [jnp.where(y == 0, 0.0, arrived(0, q, b)) for b in range(blocks)]
            low += [column(sub_rows * g - ITERS + q, b) for g in range(1, groups) for b in range(blocks)]
            field[q, PAD : PAD + 128, :] = jnp.concatenate(low, axis=0).T
            high = [column(sub_rows * g + q, b) for g in range(1, groups) for b in range(blocks)]
            high += [arrived(1, q, b) for b in range(blocks)]
            field[q + ITERS + sub_rows, PAD : PAD + 128, :] = jnp.concatenate(high, axis=0).T

    for c in more:
        c.wait_recv()
    corner_arrivals(rows_corners, 12, later)
    for e in range(2):
        for q in range(ITERS):
            idx = member + members * (q % groups)
            south = along(corner_in[e, 1 + q // groups], idx, 1)
            south = jnp.where(y == 0, 0.0, south)
            v = pltpu.roll(field[sub_rows + q, beyond_tiles[e], :], members, 1)
            field[q, beyond_tiles[e], :] = jnp.where(group == 0, south, v)
            north = along(corner_in[2 + e, 1 + q // groups], idx, 1)
            v = pltpu.roll(field[ITERS + q, beyond_tiles[e], :], 128 - members, 1)
            field[ITERS + sub_rows + q, beyond_tiles[e], :] = jnp.where(group == groups - 1, north, v)
    coef_up.wait_send()
    rows_up.wait_send()

    @pl.when(y > 0)
    def _():
        coef_down.wait_send()
        rows_down.wait_send()

    for c in sides + more:
        c.wait_send()
    for remote, c, _, _ in coef_corners + rows_corners:
        pl.when(remote)(c.wait_send)
    iterate(members, rows, field, inv, links, basis, gram)

    def sent(source, dst, n, there):
        c = copy(source, dst, n, n, there)
        c.start()
        return c

    across = [sent(gram, along_x.at[s], 15 + s, (y, lax.rem(x + s, nx))) for s in range(1, nx)]
    scale_ref[0] = inv[PAD : PAD + 128, :].T
    scale_ref[1] = square[PAD : PAD + 128, :].T
    for c in across:
        c.wait()
    along_x[0] = sum((along_x[s] for s in range(1, nx)), gram[...])
    across = [
        sent(along_x.at[0], along_y.at[s], 14 + nx + s, (lax.rem(y + s, ny), x)) for s in range(1, ny)
    ]
    for c in across:
        c.wait()
    sum_ref[...] = sum((along_y[s] for s in range(1, ny)), along_x[0])


def coefficients(gram):
    def g(i, j):
        return gram[min(i, j)][max(i, j)]

    def applied(p):
        q = []
        for k in range(ITERS + 1):
            terms = []
            if k < len(p):
                terms.append(p[k])
            if 0 < k <= len(p):
                terms.append(-ROOT * p[k - 1])
            if k + 1 < len(p):
                terms.append(-ROOT * p[k + 1])
            if terms:
                q.append(sum(terms[1:], terms[0]))
        return q

    def inner(p, q):
        total = None
        for i, a in enumerate(p):
            row = None
            for j, b in enumerate(q):
                t = g(i, j) * b
                row = t if row is None else row + t
            t = a * row
            total = t if total is None else total + t
        return total

    one = jnp.ones_like(gram[0][0])
    z, p, x = [one], [one], []
    rz = g(0, 0)
    for iteration in range(ITERS):
        q = applied(p)
        step = rz / inner(p, q)
        x = [(x[k] if k < len(x) else 0.0) + step * p[k] for k in range(len(p))]
        z = [(z[k] if k < len(z) else 0.0) - step * q[k] for k in range(len(q))]
        if iteration + 1 < ITERS:
            rz_new = inner(z, z)
            beta = rz_new / rz
            p = [z[k] + (beta * p[k] if k < len(p) else 0.0) for k in range(len(z))]
            rz = rz_new
    return x, z


def combine_kernel(members, rows, *refs):
    basis, (scale_ref, sum_ref, x_out, r_out, stage, sems) = refs[: ITERS + 1], refs[ITERS + 1 :]
    groups = 128 // members
    sub_rows = rows // groups
    tall = stage.shape[2]
    lanes = iota(1)
    sums = sum_ref[...]
    tiles = [along(sums, (lanes & (members - 1)) + members * j, 1) for j in range(4)]
    gram = [[None] * (ITERS + 1) for _ in range(ITERS + 1)]
    for n, (i, j) in enumerate(PAIRS):
        gram[i][j] = jnp.broadcast_to(tiles[n // 8][n % 8 : n % 8 + 1, :], (8, 128))
    xs, zs = coefficients(gram)
    flat = stage.reshape(2 * members * tall, 128)
    blocks = members // 8
    half = sub_rows // 2
    outs = (x_out, r_out)

    def drain(h):
        copies = []
        for o in range(2):
            for g in range(groups):
                at = slice(sub_rows * g + half * h, sub_rows * g + half * (h + 1))
                copies.append(
                    pltpu.make_async_copy(stage.at[o, :, at, :], outs[o].at[:, at, :], sems.at[h, o, g])
                )
        return copies

    started = []
    for h in range(2):

        def row(r):
            found = ([], [])
            for t in range(16):
                at = slice(PAD + 8 * t, PAD + 8 * t + 8)
                vs = [basis[k][r + ITERS, at, :] for k in range(ITERS + 1)]
                found[0].append(sum((xs[k] * vs[k] for k in range(1, ITERS)), xs[0] * vs[0]))
                found[1].append(sum((zs[k] * vs[k] for k in range(1, ITERS + 1)), zs[0] * vs[0]))
            for o in range(2):
                turned = jnp.concatenate(found[o], axis=0).T
                for g in range(groups):
                    row = sub_rows * g + r
                    scale = jnp.broadcast_to(scale_ref[o, pl.ds(row + 8, 1), :], (8, 128))
                    for b in range(blocks):
                        n = 8 * (g * blocks + b)
                        at = pl.ds((o * members + 8 * b) * tall + row, 8, stride=tall)
                        flat[at, :] = turned[n : n + 8, :] * scale

        @pl.loop(0, half // 4)
        def _(part):
            for within in range(4):
                row(half * h + 4 * part + within)

        for c in drain(h):
            c.start()
            started.append(c)
    for c in started:
        c.wait()


def on_device(right_side, couplings, center, ocean_mask):
    members, rows, columns = right_side.shape
    groups = 128 // members
    sub_rows = rows // groups
    assert lax.axis_size("gx") > 2 and ITERS <= 2 * groups
    assert columns == 128 and members % 8 == 0 and groups * members == 128
    assert 3 * (rows + 16) <= 256 < 4 * (rows + 16) and 2 * (rows + 16) >= 128 and sub_rows % 16 == 0 and sub_rows >= ITERS
    ny, nx = lax.axis_size("gy"), lax.axis_size("gx")
    vmem = pl.BlockSpec(memory_space=pltpu.VMEM)
    hbm = pl.BlockSpec(memory_space=pltpu.HBM)
    deep, wide = sub_rows + 2 * ITERS, columns + 2 * PAD + 8

    inputs = [
        pltpu.with_memory_space_constraint(v, pltpu.HBM)
        for v in (right_side, couplings, center, ocean_mask)
    ]

    def first(*refs):
        solve_kernel(members, rows, ny, nx, *refs)

    *basis, scale, sums = pl.pallas_call(
        first,
        out_shape=(pltpu.VMEM((deep, wide, 128), F32),) * (ITERS + 1)
        + (pltpu.VMEM((2, 128, 128), F32), pltpu.VMEM((8, 128), F32)),
        in_specs=[hbm] * 4,
        out_specs=(vmem,) * (ITERS + 3),
        scratch_shapes=[
            pltpu.VMEM((deep, wide, 128), F32),
            pltpu.VMEM((5, deep + 3, wide, 128), F32),
            pltpu.VMEM((5, wide, 128), F32),
            pltpu.VMEM((members, rows + 8, columns), F32),
            pltpu.VMEM((3, rows, columns), F32),
            pltpu.VMEM((rows, columns), F32),
            pltpu.VMEM((rows, columns), jnp.int32),
            pltpu.VMEM((2, 5, 8, columns), F32),
            pltpu.VMEM((2, 5, 8, columns), F32),
            pltpu.VMEM((2, ITERS * members, columns), F32),
            pltpu.VMEM((2, ITERS * members, columns), F32),
            pltpu.VMEM((2, 5, 8, 128), F32),
            pltpu.VMEM((4, 3, 8, 128), F32),
            pltpu.VMEM((4, 3, 8, 128), F32),
            pltpu.VMEM((128, 128), F32),
            pltpu.VMEM((2, wide, 128), F32),
            pltpu.VMEM((wide, 128), F32),
            pltpu.VMEM((wide, 128), F32),
            pltpu.VMEM((5 * 144, 256), jnp.bfloat16),
            pltpu.VMEM(((deep + 2) // 2, 256, 256), jnp.bfloat16),
            pltpu.VMEM((8, 128), F32),
            pltpu.VMEM((nx, 8, 128), F32),
            pltpu.VMEM((ny, 8, 128), F32),
            pltpu.SemaphoreType.DMA((4,)),
            pltpu.SemaphoreType.DMA((14 + nx + ny,)),
            pltpu.SemaphoreType.DMA((14 + nx + ny,)),
        ],
        compiler_params=pltpu.CompilerParams(
            collective_id=0, has_side_effects=True, vmem_limit_bytes=GRANT
        ),
    )(*inputs)

    def second(*refs):
        combine_kernel(members, rows, *refs)

    return pl.pallas_call(
        second,
        out_shape=(jax.ShapeDtypeStruct(right_side.shape, F32),) * 2,
        in_specs=[vmem] * (ITERS + 3),
        out_specs=(hbm, hbm),
        compiler_params=pltpu.CompilerParams(vmem_limit_bytes=GRANT),
        scratch_shapes=[
            pltpu.VMEM((2, members, rows + 8, columns), F32),
            pltpu.SemaphoreType.DMA((2, 2, groups)),
        ],
    )(*basis, scale, sums)


def solution(mesh):
    in_specs = (P(None, "gy", "gx"), P(None, "gy", "gx"), P("gy", "gx"), P("gy", "gx"))
    out_specs = (P(None, "gy", "gx"), P(None, "gy", "gx"))
    return jax.shard_map(
        on_device, mesh=mesh, in_specs=in_specs, out_specs=out_specs, check_vma=False
    )
```

```python
import jax
import jax.numpy as jnp
from jax import lax
from jax.experimental import pallas as pl
from jax.experimental.pallas import tpu as pltpu
from jax.sharding import PartitionSpec as P

ITERS = 6
ROOT = 0.28
PAD = 16
VMEM = 67043328
GRANT = 24 * 1024 * 1024
SKEW = [(i, j) for i in range(ITERS) for j in range(i + 1, ITERS)]
SEAM = 16 + ITERS
F32 = jnp.float32


def iota(dim):
    return lax.broadcasted_iota(jnp.int32, (8, 128), dim)


def along(x, idx, axis):
    return jnp.take_along_axis(x, idx, axis=axis, mode="promise_in_bounds")


def prepare(members, rows, top, planes, shifted, inv, links, square, lhs, pick):
    first, chunk, tiles = PAD - 8, 48, 18
    lanes = lax.broadcasted_iota(jnp.int32, (chunk, 128), 1)
    seam = lanes == rows + 8
    folded = jnp.logical_and(top, lanes >= rows + 8)
    span = rows + 16
    factor = 1.0 / ROOT

    def before(v):
        return pltpu.roll(v, 1, 1)

    def after(v):
        return pltpu.roll(v, 127, 1)

    for t in range(0, 8 * tiles, chunk):
        at, nxt = slice(first + t, first + t + chunk), slice(first + t + 1, first + t + 1 + chunk)
        for n, p in enumerate((1, 2)):
            shifted[n, at, :] = jnp.where(folded, planes[p, nxt, :], planes[p, at, :])

    for t in range(0, 8 * tiles, chunk):
        at = slice(first + t, first + t + chunk)
        prv = slice(first + t - 1, first + t - 1 + chunk)
        cn, ce, cne = planes[0, at, :], shifted[0, at, :], shifted[1, at, :]
        cew, cnw = shifted[0, prv, :], shifted[1, prv, :]
        diag = planes[3, at, :] + cn + ce + cew + cne + cnw + before(cn + cne + cnw)
        ocean = planes[4, at, :] > 0.0
        root = jnp.sqrt(diag)
        recip = jnp.where(ocean, 1.0 / root, 0.0)
        root = jnp.where(ocean, root, 0.0)
        inv[at, :] = jnp.where(seam, after(recip), recip)
        square[at, :] = root

    for t in range(0, 8 * tiles, chunk):
        at = slice(first + t, first + t + chunk)
        nxt = slice(first + t + 1, first + t + 1 + chunk)
        here, east = inv[at, :], inv[nxt, :]
        up, up_east = after(here), after(east)
        here_up = jnp.where(seam, before(here), here)
        east_up = jnp.where(seam, before(east), east)
        cn, ce, cne = planes[0, at, :] * factor, shifted[0, at, :] * factor, shifted[1, at, :] * factor
        values = (cn * here_up * up, ce * here * east, cne * here_up * up_east, cne * east_up * up, here)
        for n, v in enumerate(values):
            top_part = v.astype(jnp.bfloat16).astype(F32)
            v = v - top_part
            mid_part = v.astype(jnp.bfloat16).astype(F32)
            moved = pltpu.roll(mid_part, span, 1)
            low_part = pltpu.roll(v - mid_part, 2 * span - 128, 1)
            left = jnp.where(lanes < span, top_part, moved)
            right = jnp.where(lanes < 2 * span - 128, moved, low_part)
            right = jnp.where(lanes < 3 * span - 128, right, 0.0)
            to = slice(8 * tiles * n + t, 8 * tiles * n + t + chunk)
            lhs[to, 0:128] = left.astype(jnp.bfloat16)
            lhs[to, 128:256] = right.astype(jnp.bfloat16)

    def spread(p, planes_from, halves):
        found = jnp.dot(lhs[8 * tiles * planes_from :, :], pick[p], preferred_element_type=F32)
        for n in range(planes_from, 5):
            for h in range(halves):
                at = 8 * tiles * (n - planes_from)
                links[n, 2 * p + h, first : first + 8 * tiles, :] = found[
                    at : at + 8 * tiles, 128 * h : 128 * h + 128
                ]

    pairs = pick.shape[0] - 1
    together = 2 - pairs % 2

    @pl.loop(0, pairs // together)
    def _(part):
        for within in range(together):
            spread(together * part + within, 0, 2)

    spread(pairs, 4, 1)


def choose(members, rows, pick):
    groups = 128 // members
    sub_rows = rows // groups
    span = rows + 16
    source = lax.broadcasted_iota(jnp.int32, (256, 256), 0)
    lane = lax.broadcasted_iota(jnp.int32, (256, 256), 1)
    source = source - span * ((source >= span).astype(jnp.int32) + (source >= 2 * span).astype(jnp.int32))
    group = lax.shift_right_logical(lane & 127, members.bit_length() - 1)
    half = lax.shift_right_logical(lane, 7)
    last = (group == groups - 1).astype(jnp.int32)
    base = source - sub_rows * group - half - 8 + ITERS

    @pl.loop(0, pick.shape[0])
    def _(p):
        later = (2 * p + half >= sub_rows + ITERS).astype(jnp.int32)
        hit = base == 2 * p + later * (last - 1)
        pick[p] = jnp.where(hit, 1.0, 0.0).astype(jnp.bfloat16)


def apply(k, links, basis, start, stop, tiles, tile):
    depth = ITERS - 1 - k
    here, out = basis[k], basis[k + 1]
    old = basis[k - 1] if k else None

    @pl.loop(0, tiles)
    def _(t):
        x0 = PAD - depth + 8 * tile(t)
        mid, east, west = pl.ds(x0, 8), pl.ds(x0 + 1, 8), pl.ds(x0 - 1, 8)

        def three(r):
            return here[r, west, :], here[r, mid, :], here[r, east, :]

        dn, cur = three(start - 1), three(start)
        north = links[0, start - 1 + (1 if start > SEAM else 0), mid, :]
        for r in range(start, stop):
            nxt = three(r + 1)
            c = r + (1 if r >= SEAM else 0)
            if r == SEAM:
                north = links[0, c - 1, mid, :]
            south, north = north, links[0, c, mid, :]
            total = (north * nxt[1] + south * dn[1]) + (
                links[1, c, mid, :] * cur[2] + links[1, c, west, :] * cur[0]
            )
            total = total + (links[2, c, mid, :] * nxt[2] + links[2, c - 1, west, :] * dn[0])
            total = total + (links[3, c, west, :] * nxt[0] + links[3, c - 1, mid, :] * dn[2])
            if old is not None:
                total = total - old[r, mid, :]
            out[r, mid, :] = total
            dn, cur = cur, nxt


def begin(raw, links, basis):
    @pl.loop(ITERS, SEAM)
    def _(r):
        for t in range(16):
            at = slice(PAD + 8 * t, PAD + 8 * t + 8)
            basis[0][r, at, :] = raw[r, at, :] * links[4, r, at, :]

    apply(0, links, basis, ITERS + 1, SEAM - 1, 15, lambda t: t + 1)
    apply(1, links, basis, ITERS + 2, SEAM - 2, 14, lambda t: t + 1)


def iterate(members, rows, top, raw, links, basis, gram_ref):
    subs = iota(0)
    group = lax.shift_right_logical(iota(1), members.bit_length() - 1)
    for r in range(ITERS, SEAM):
        for t in (0, 17):
            at = slice(PAD - 8 + 8 * t, PAD + 8 * t)
            basis[0][r, at, :] = raw[r, at, :] * links[4, r, at, :]

    apply(0, links, basis, 1, ITERS + 1, 18, lambda t: t)
    apply(0, links, basis, SEAM - 1, SEAM + ITERS - 1, 18, lambda t: t)
    apply(0, links, basis, ITERS + 1, SEAM - 1, 3, lambda t: t + 15 * jnp.minimum(t, 1))
    apply(1, links, basis, 2, ITERS + 2, 17, lambda t: t)
    apply(1, links, basis, SEAM - 2, SEAM + ITERS - 2, 17, lambda t: t)
    apply(1, links, basis, ITERS + 2, SEAM - 2, 3, lambda t: t + 14 * jnp.minimum(t, 1))
    for k in range(2, ITERS):
        depth = ITERS - 1 - k
        count = (128 + 2 * depth + 7) // 8
        apply(k, links, basis, ITERS - depth, SEAM + depth, count, lambda t: t)

    def body(r, sums):
        sums = list(sums)
        for t in range(16):
            at = slice(PAD + 8 * t, PAD + 8 * t + 8)
            vs = [basis[k][r + ITERS, at, :] for k in range(ITERS + 1)]
            for i in range(ITERS):
                sums[2 * i] = sums[2 * i] + vs[i] * vs[i]
                sums[2 * i + 1] = sums[2 * i + 1] + vs[i] * vs[i + 1]
        return tuple(sums)

    zero = jnp.zeros((8, 128), F32)
    sums = lax.fori_loop(0, SEAM - ITERS, body, (zero,) * (2 * ITERS))
    fold = jnp.logical_and(group == 128 // members - 1, top)

    def across(t, sums):
        sums = list(sums)
        for u in range(4):
            x0 = PAD + 32 * t + 8 * u
            mid, east, west = pl.ds(x0, 8), pl.ds(x0 + 1, 8), pl.ds(x0 - 1, 8)
            north, right, left = links[0, SEAM - 1, mid, :], links[2, SEAM - 1, mid, :], links[3, SEAM - 1, west, :]
            here, over = [], []
            for k in range(ITERS):
                w = basis[k]
                v = north * w[SEAM, mid, :] + right * w[SEAM, east, :] + left * w[SEAM, west, :]
                over.append(jnp.where(fold, v, 0.0))
                here.append(w[SEAM - 1, mid, :])
            for n, (i, j) in enumerate(SKEW):
                sums[n] = sums[n] + (here[i] * over[j] - here[j] * over[i])
        return tuple(sums)

    sums = sums + lax.fori_loop(0, 4, across, (zero,) * len(SKEW))
    pack = [zero] * 4
    for n, s in enumerate(sums):
        for step in (1, 2, 4):
            s = s + pltpu.roll(s, step, 0)
        pack[n // 8] = jnp.where(subs == n % 8, s, pack[n // 8])
    total = zero
    for j, v in enumerate(pack):
        width = members
        while width < 128:
            v = v + pltpu.roll(v, width, 1)
            width *= 2
        total = jnp.where(group == j, v, total)
    gram_ref[...] = total


def solve_kernel(members, rows, ny, nx, rhs_hbm, coup_hbm, center_hbm, mask_hbm, *refs):
    basis, (scale_ref, sum_ref) = refs[: ITERS + 1], refs[ITERS + 1 : ITERS + 3]
    (
        field, links, planes, rhs, coup, center, mask, coef_out, coef_in, rows_out, rows_in, strip_out, corner_out, corner_in, ext,
        shifted, inv, square, lhs, pick, gram, along_x, along_y, load, send, recv,
    ) = refs[ITERS + 3 :]
    groups = 128 // members
    sub_rows = rows // groups
    tall = rhs.shape[1]
    y, x = lax.axis_index("gy"), lax.axis_index("gx")
    top = (y + 1) // ny
    mirror = nx - 1 - x
    east, west = lax.rem(x + 1, nx), lax.rem(x + nx - 1, nx)
    up = (y + 1 - top, x + top * (mirror - x))
    down = (jnp.maximum(y - 1, 0), x)
    loads = [
        pltpu.make_async_copy(coup_hbm, coup, load.at[0]),
        pltpu.make_async_copy(center_hbm, center, load.at[1]),
        pltpu.make_async_copy(mask_hbm, mask, load.at[2]),
        pltpu.make_async_copy(rhs_hbm, rhs.at[:, 0:rows, :], load.at[3]),
    ]
    for c in loads:
        c.start()
    barrier = pltpu.get_barrier_semaphore()

    def greet(there):
        pl.semaphore_signal(barrier, inc=1, device_id=there, device_id_type=pl.DeviceIdType.MESH)

    for step in range(1, nx):
        greet((y, lax.rem(x + step, nx)))
    for step in range(1, ny):
        greet((lax.rem(y + step, ny), x))

    @pl.when(y > 0)
    def _():
        greet((y - 1, east))
        greet((y - 1, west))

    @pl.when(top == 0)
    def _():
        greet((y + 1, east))
        greet((y + 1, west))

    def copy(src, dst, n, m, there):
        return pltpu.make_async_remote_copy(
            src_ref=src,
            dst_ref=dst,
            send_sem=send.at[n],
            recv_sem=recv.at[m],
            device_id=there,
            device_id_type=pl.DeviceIdType.MESH,
        )

    def corner(base, parts):
        found = []
        for e in range(2):
            plain, folded = x + 2 * e - 1, mirror + 1 - 2 * e
            to = lax.rem(plain + top * (folded - plain) + nx, nx)
            k = 1 - e + top * (1 + 2 * e)
            c = copy(
                corner_out.at[e, parts], corner_in.at[k, parts], base + e, base + k, (y + 1 - top, to)
            )
            found.append((jnp.logical_or(top == 0, to != x), c, e, k))
        for e in range(2):
            k = 3 - e
            there = (jnp.maximum(y - 1, 0), east if e else west)
            c = copy(
                corner_out.at[2 + e, parts], corner_in.at[k, parts], base + 2 + e, base + k, there
            )
            found.append((y > 0, c, 2 + e, k))
        return found

    def start_corners(found, parts):
        for n, (remote, c, e, k) in enumerate(found):
            pl.when(remote)(c.start)
            if n < 2:

                @pl.when(jnp.logical_not(remote))
                def _():
                    corner_in[k, parts] = corner_out[e, parts]

    def corner_arrivals(found, base, parts):
        for k in range(4):
            c = copy(corner_out.at[0, parts], corner_in.at[k, parts], base, base + k, (y, east))
            pl.when(y > 0 if k < 2 else found[k - 2][0])(c.wait_recv)

    lanes, subs = iota(1), iota(0)
    flip_lane = jnp.where(top == 1, 127 - lanes, lanes)
    flip_sub = jnp.where(top == 1, 7 - subs, subs)
    tiles = (slice(PAD, PAD + 8), slice(PAD + 120, PAD + 128))
    beyond_tiles = (slice(PAD - 8, PAD), slice(PAD + 128, PAD + 136))
    for c in loads[:3]:
        c.wait()

    def own(p, at):
        if p < 3:
            return coup[p, at, :]
        return center[at, :] if p == 3 else mask[at, :].astype(F32)

    packs = [jnp.zeros((8, 128), F32)] * 4
    plane = lax.shift_right_logical(lanes, 3)
    high_lanes = jnp.where(top == 1, rows + 7 - (lanes & 7), rows + (lanes & 7))
    low_lanes = 8 + (lanes & 7)
    ext[0:8, :] = jnp.zeros((8, 128), F32)
    ext[rows + 8 : 128, :] = jnp.zeros((120 - rows, 128), F32)
    for p in range(5):
        coef_out[0, p] = along(along(own(p, slice(rows - 8, rows)), flip_lane, 1), flip_sub, 0)
        coef_out[1, p] = own(p, slice(0, 8))
        ext[8 : rows + 8, :] = own(p, slice(0, rows))
        turned = ext[...].T
        for e, edge in enumerate((turned[0:8], turned[120:128])):
            strip_out[e, p] = edge
            packs[e] = jnp.where(plane == p, along(edge, high_lanes, 1), packs[e])
            packs[2 + e] = jnp.where(plane == p, along(edge, low_lanes, 1), packs[2 + e])
    for e in range(4):
        corner_out[e, 0] = along(packs[e], flip_sub, 0) if e < 2 else packs[e]
    pl.semaphore_wait(barrier, nx + ny - 2 + 2 * (1 - top) + 2 * jnp.minimum(y, 1))
    coef_up = copy(coef_out.at[0], coef_in.at[top], 0, top, up)
    coef_down = copy(coef_out.at[1], coef_in.at[1], 1, 1, down)
    rows_up = copy(rows_out.at[0], rows_in.at[top], 2, 2 + top, up)
    rows_down = copy(rows_out.at[1], rows_in.at[1], 3, 3, down)
    first = slice(0, 1)
    later = slice(1, 3)
    coef_corners, rows_corners = corner(8, first), corner(12, later)
    sides = [
        copy(strip_out.at[0], planes.at[:, PAD + 128 : PAD + 136, :], 4, 4, (y, west)),
        copy(strip_out.at[1], planes.at[:, PAD - 8 : PAD, :], 5, 5, (y, east)),
    ]
    start_corners(coef_corners, first)
    coef_up.start()
    pl.when(y > 0)(coef_down.start)
    for c in sides:
        c.start()
    flat = rhs.reshape(members * tall, 128)

    def column(row, block):
        return flat[pl.ds(8 * block * tall + row, 8, stride=tall), :]

    blocks = members // 8
    loads[3].wait()
    for q in range(ITERS):
        high = rows - ITERS + q + top * (ITERS - 1 - 2 * q)
        for b in range(blocks):
            at = slice(q * members + 8 * b, q * members + 8 * b + 8)
            rows_out[0, at, :] = along(column(high, b), flip_lane, 1)
            rows_out[1, at, :] = column(q, b)

    @pl.loop(0, sub_rows // 4)
    def _(part):
        for within in range(4):
            r = 4 * part + within
            stack = [column(sub_rows * g + r, b) for g in range(groups) for b in range(blocks)]
            field[r + ITERS, PAD : PAD + 128, :] = jnp.concatenate(stack, axis=0).T

    member = lanes & (members - 1)
    group = lax.shift_right_logical(lanes, members.bit_length() - 1)
    for e in range(2):
        packs = [[jnp.zeros((8, 128), F32)] * 2 for _ in range(2)]
        for q in range(ITERS):
            here = group == q % groups
            v = field[sub_rows + q + top * (ITERS - 1 - 2 * q), tiles[e], :]
            v = along(v, member + (128 - members), 1)
            packs[0][q // groups] = jnp.where(here, v, packs[0][q // groups])
            v = along(field[ITERS + q, tiles[e], :], member, 1)
            packs[1][q // groups] = jnp.where(here, v, packs[1][q // groups])
        for n in range(2):
            corner_out[e, 1 + n] = along(packs[0][n], flip_sub, 0)
            corner_out[2 + e, 1 + n] = packs[1][n]
    inner = slice(ITERS, ITERS + sub_rows)
    more = [
        copy(field.at[inner, tiles[0], :], field.at[inner, beyond_tiles[1], :], 6, 6, (y, west)),
        copy(field.at[inner, tiles[1], :], field.at[inner, beyond_tiles[0], :], 7, 7, (y, east)),
    ]
    start_corners(rows_corners, later)
    for c in more:
        c.start()
    choose(members, rows, pick)
    coef_north = copy(coef_out.at[1], coef_in.at[1], 1, 1, down)
    coef_south = copy(coef_out.at[0], coef_in.at[0], 0, 0, up)
    coef_north.wait_recv()
    pl.when(y > 0)(coef_south.wait_recv)
    rows_up.start()
    pl.when(y > 0)(rows_down.start)
    for p in range(5):
        beyond = coef_in[1, p]
        moved = pltpu.roll(beyond, 1, 0)
        if p in (0, 2):
            last = jnp.broadcast_to(own(p, slice(rows - 1, rows)), (8, 128))
            beyond = jnp.where(top == 1, beyond, jnp.where(subs == 0, last, moved))
        else:
            beyond = jnp.where(subs == 0, beyond, moved)
        ext[0:8, :] = jnp.where(y == 0, 0.0, coef_in[0, p])
        ext[8 : rows + 8, :] = own(p, slice(0, rows))
        ext[rows + 8 : rows + 16, :] = beyond
        planes[p, PAD : PAD + 128, :] = ext[...].T
    for c in sides:
        c.wait_recv()
    corner_arrivals(coef_corners, 8, first)
    for e in range(2):
        low, high = corner_in[e, 0], corner_in[2 + e, 0]
        for p in range(5):
            strip = planes[p, beyond_tiles[e], :]
            shift = 1 - top if p in (0, 2) else 1
            idx = jnp.clip(lanes - (rows + 8) - shift, 0, 7) + 8 * p
            north = along(high, idx, 1)
            if p in (0, 2):
                joint = jnp.logical_and(lanes == rows + 8, top == 0)
                north = jnp.where(joint, pltpu.roll(strip, 1, 1), north)
            south = jnp.where(y == 0, 0.0, along(low, (lanes & 7) + 8 * p, 1))
            outside = jnp.logical_and(lanes >= rows + 8, lanes < rows + 16)
            strip = jnp.where(lanes < 8, south, jnp.where(outside, north, strip))
            planes[p, beyond_tiles[e], :] = strip
    prepare(members, rows, y == ny - 1, planes, shifted, inv, links, square, lhs, pick)
    begin(field, links, basis)
    copy(rows_out.at[1], rows_in.at[1], 3, 3, down).wait_recv()
    pl.when(y > 0)(copy(rows_out.at[0], rows_in.at[0], 2, 2, up).wait_recv)

    def arrived(side, q, b):
        return rows_in[side, pl.ds(pl.multiple_of(q * members, 8) + 8 * b, 8), :]

    @pl.loop(0, ITERS // 2)
    def _(part):
        for within in range(2):
            q = 2 * part + within
            low = [jnp.where(y == 0, 0.0, arrived(0, q, b)) for b in range(blocks)]
            low += [column(sub_rows * g - ITERS + q, b) for g in range(1, groups) for b in range(blocks)]
            basis[0][q, PAD : PAD + 128, :] = (
                jnp.concatenate(low, axis=0).T * links[4, q, PAD : PAD + 128, :]
            )
            high = [column(sub_rows * g + q, b) for g in range(1, groups) for b in range(blocks)]
            high += [arrived(1, q, b) for b in range(blocks)]
            r = q + ITERS + sub_rows
            basis[0][r, PAD : PAD + 128, :] = (
                jnp.concatenate(high, axis=0).T * links[4, r + 1, PAD : PAD + 128, :]
            )

    for c in more:
        c.wait_recv()
    corner_arrivals(rows_corners, 12, later)
    for e in range(2):
        for q in range(ITERS):
            idx = member + members * (q % groups)
            south = along(corner_in[e, 1 + q // groups], idx, 1)
            south = jnp.where(y == 0, 0.0, south)
            v = pltpu.roll(field[sub_rows + q, beyond_tiles[e], :], members, 1)
            v = jnp.where(group == 0, south, v)
            basis[0][q, beyond_tiles[e], :] = v * links[4, q, beyond_tiles[e], :]
            north = along(corner_in[2 + e, 1 + q // groups], idx, 1)
            v = pltpu.roll(field[ITERS + q, beyond_tiles[e], :], 128 - members, 1)
            v, r = jnp.where(group == groups - 1, north, v), ITERS + sub_rows + q
            basis[0][r, beyond_tiles[e], :] = v * links[4, r + 1, beyond_tiles[e], :]
    coef_up.wait_send()
    rows_up.wait_send()

    @pl.when(y > 0)
    def _():
        coef_down.wait_send()
        rows_down.wait_send()

    for c in sides + more:
        c.wait_send()
    for remote, c, _, _ in coef_corners + rows_corners:
        pl.when(remote)(c.wait_send)
    iterate(members, rows, y == ny - 1, field, links, basis, gram)

    def sent(source, dst, n, there):
        c = copy(source, dst, n, n, there)
        c.start()
        return c

    across = [sent(gram, along_x.at[s], 15 + s, (y, lax.rem(x + s, nx))) for s in range(1, nx)]
    scale_ref[0] = inv[PAD : PAD + 128, :].T
    scale_ref[1] = square[PAD : PAD + 128, :].T
    for c in across:
        c.wait()
    along_x[0] = sum((along_x[s] for s in range(1, nx)), gram[...])
    across = [
        sent(along_x.at[0], along_y.at[s], 14 + nx + s, (lax.rem(y + s, ny), x)) for s in range(1, ny)
    ]
    for c in across:
        c.wait()
    sum_ref[...] = sum((along_y[s] for s in range(1, ny)), along_x[0])


def coefficients(gram):
    def g(i, j):
        return gram[min(i, j)][max(i, j)]

    def applied(p):
        q = []
        for k in range(ITERS + 1):
            terms = []
            if k < len(p):
                terms.append(p[k])
            if 0 < k <= len(p):
                terms.append(-ROOT * p[k - 1])
            if k + 1 < len(p):
                terms.append(-ROOT * p[k + 1])
            if terms:
                q.append(sum(terms[1:], terms[0]))
        return q

    def inner(p, q):
        total = None
        for i, a in enumerate(p):
            row = None
            for j, b in enumerate(q):
                t = g(i, j) * b
                row = t if row is None else row + t
            t = a * row
            total = t if total is None else total + t
        return total

    one = jnp.ones_like(gram[0][0])
    z, p, x = [one], [one], []
    rz = g(0, 0)
    for iteration in range(ITERS):
        q = applied(p)
        step = rz / inner(p, q)
        x = [(x[k] if k < len(x) else 0.0) + step * p[k] for k in range(len(p))]
        z = [(z[k] if k < len(z) else 0.0) - step * q[k] for k in range(len(q))]
        if iteration + 1 < ITERS:
            rz_new = inner(z, z)
            beta = rz_new / rz
            p = [z[k] + (beta * p[k] if k < len(p) else 0.0) for k in range(len(z))]
            rz = rz_new
    return x, z


def combine_kernel(members, rows, *refs):
    basis, (scale_ref, sum_ref, x_out, r_out, stage, sems) = refs[: ITERS + 1], refs[ITERS + 1 :]
    groups = 128 // members
    sub_rows = rows // groups
    tall = stage.shape[2]
    lanes = iota(1)
    sums = sum_ref[...]
    tiles = [along(sums, (lanes & (members - 1)) + members * j, 1) for j in range(4)]
    found = [
        jnp.broadcast_to(tiles[n // 8][n % 8 : n % 8 + 1, :], (8, 128))
        for n in range(2 * ITERS + len(SKEW))
    ]
    gram = [[None] * (ITERS + 1) for _ in range(ITERS + 1)]
    for i in range(ITERS):
        gram[i][i], gram[i][i + 1] = found[2 * i], found[2 * i + 1]
    skew = dict(zip(SKEW, found[2 * ITERS :]))
    for gap in range(2, ITERS + 1):
        for i in range(ITERS + 1 - gap):
            j = i + gap - 1
            v = gram[i + 1][j] - gram[i][j - 1] + skew[i, j]
            gram[i][j + 1] = v + gram[i - 1][j] if i else v
    xs, zs = coefficients(gram)
    flat = stage.reshape(2 * members * tall, 128)
    blocks = members // 8
    half = sub_rows // 2
    outs = (x_out, r_out)

    def drain(h):
        copies = []
        for o in range(2):
            for g in range(groups):
                at = slice(sub_rows * g + half * h, sub_rows * g + half * (h + 1))
                copies.append(
                    pltpu.make_async_copy(stage.at[o, :, at, :], outs[o].at[:, at, :], sems.at[h, o, g])
                )
        return copies

    started = []
    for h in range(2):

        def row(r):
            found = ([], [])
            for t in range(16):
                at = slice(PAD + 8 * t, PAD + 8 * t + 8)
                vs = [basis[k][r + ITERS, at, :] for k in range(ITERS + 1)]
                found[0].append(sum((xs[k] * vs[k] for k in range(1, ITERS)), xs[0] * vs[0]))
                found[1].append(sum((zs[k] * vs[k] for k in range(1, ITERS + 1)), zs[0] * vs[0]))
            for o in range(2):
                turned = jnp.concatenate(found[o], axis=0).T
                for g in range(groups):
                    row = sub_rows * g + r
                    scale = jnp.broadcast_to(scale_ref[o, pl.ds(row + 8, 1), :], (8, 128))
                    for b in range(blocks):
                        n = 8 * (g * blocks + b)
                        at = pl.ds((o * members + 8 * b) * tall + row, 8, stride=tall)
                        flat[at, :] = turned[n : n + 8, :] * scale

        @pl.loop(0, half // 4)
        def _(part):
            for within in range(4):
                row(half * h + 4 * part + within)

        for c in drain(h):
            c.start()
            started.append(c)
    for c in started:
        c.wait()


def on_device(right_side, couplings, center, ocean_mask):
    members, rows, columns = right_side.shape
    groups = 128 // members
    sub_rows = rows // groups
    assert lax.axis_size("gx") > 2 and ITERS <= 2 * groups
    assert columns == 128 and members % 8 == 0 and groups * members == 128
    assert 3 * (rows + 16) <= 256 < 4 * (rows + 16) and 2 * (rows + 16) >= 128 and sub_rows == SEAM - ITERS
    ny, nx = lax.axis_size("gy"), lax.axis_size("gx")
    vmem = pl.BlockSpec(memory_space=pltpu.VMEM)
    hbm = pl.BlockSpec(memory_space=pltpu.HBM)
    deep, wide = sub_rows + 2 * ITERS, columns + 2 * PAD + 8

    inputs = [
        pltpu.with_memory_space_constraint(v, pltpu.HBM)
        for v in (right_side, couplings, center, ocean_mask)
    ]

    def first(*refs):
        solve_kernel(members, rows, ny, nx, *refs)

    *basis, scale, sums = pl.pallas_call(
        first,
        out_shape=(pltpu.VMEM((deep, wide, 128), F32),) * (ITERS + 1)
        + (pltpu.VMEM((2, 128, 128), F32), pltpu.VMEM((8, 128), F32)),
        in_specs=[hbm] * 4,
        out_specs=(vmem,) * (ITERS + 3),
        scratch_shapes=[
            pltpu.VMEM((deep, wide, 128), F32),
            pltpu.VMEM((5, deep + 3, wide, 128), F32),
            pltpu.VMEM((5, wide, 128), F32),
            pltpu.VMEM((members, rows + 8, columns), F32),
            pltpu.VMEM((3, rows, columns), F32),
            pltpu.VMEM((rows, columns), F32),
            pltpu.VMEM((rows, columns), jnp.int32),
            pltpu.VMEM((2, 5, 8, columns), F32),
            pltpu.VMEM((2, 5, 8, columns), F32),
            pltpu.VMEM((2, ITERS * members, columns), F32),
            pltpu.VMEM((2, ITERS * members, columns), F32),
            pltpu.VMEM((2, 5, 8, 128), F32),
            pltpu.VMEM((4, 3, 8, 128), F32),
            pltpu.VMEM((4, 3, 8, 128), F32),
            pltpu.VMEM((128, 128), F32),
            pltpu.VMEM((2, wide, 128), F32),
            pltpu.VMEM((wide, 128), F32),
            pltpu.VMEM((wide, 128), F32),
            pltpu.VMEM((5 * 144, 256), jnp.bfloat16),
            pltpu.VMEM(((deep + 2) // 2, 256, 256), jnp.bfloat16),
            pltpu.VMEM((8, 128), F32),
            pltpu.VMEM((nx, 8, 128), F32),
            pltpu.VMEM((ny, 8, 128), F32),
            pltpu.SemaphoreType.DMA((4,)),
            pltpu.SemaphoreType.DMA((14 + nx + ny,)),
            pltpu.SemaphoreType.DMA((14 + nx + ny,)),
        ],
        compiler_params=pltpu.CompilerParams(
            collective_id=0, has_side_effects=True, vmem_limit_bytes=GRANT
        ),
    )(*inputs)

    def second(*refs):
        combine_kernel(members, rows, *refs)

    return pl.pallas_call(
        second,
        out_shape=(jax.ShapeDtypeStruct(right_side.shape, F32),) * 2,
        in_specs=[vmem] * (ITERS + 3),
        out_specs=(hbm, hbm),
        compiler_params=pltpu.CompilerParams(vmem_limit_bytes=GRANT),
        scratch_shapes=[
            pltpu.VMEM((2, members, rows + 8, columns), F32),
            pltpu.SemaphoreType.DMA((2, 2, groups)),
        ],
    )(*basis, scale, sums)


def solution(mesh):
    in_specs = (P(None, "gy", "gx"), P(None, "gy", "gx"), P("gy", "gx"), P("gy", "gx"))
    out_specs = (P(None, "gy", "gx"), P(None, "gy", "gx"))
    return jax.shard_map(
        on_device, mesh=mesh, in_specs=in_specs, out_specs=out_specs, check_vma=False
    )
```

```python
import jax
import jax.numpy as jnp
from jax import lax
from jax.experimental import pallas as pl
from jax.experimental.pallas import tpu as pltpu
from jax.sharding import PartitionSpec as P

ITERS = 6
ROOT = 0.18
PAD = 16
VMEM = 67043328
GRANT = 24 * 1024 * 1024
SKEW = [(i, j) for i in range(ITERS) for j in range(i + 1, ITERS)]
SEAM = 16 + ITERS
F32 = jnp.float32


def iota(dim):
    return lax.broadcasted_iota(jnp.int32, (8, 128), dim)


def along(x, idx, axis):
    return jnp.take_along_axis(x, idx, axis=axis, mode="promise_in_bounds")


def prepare(members, rows, top, planes, shifted, inv, links, square, lhs, pick):
    first, chunk, tiles = PAD - 8, 48, 18
    lanes = lax.broadcasted_iota(jnp.int32, (chunk, 128), 1)
    seam = lanes == rows + 8
    folded = jnp.logical_and(top, lanes >= rows + 8)
    span = rows + 16
    factor = 1.0 / ROOT

    def before(v):
        return pltpu.roll(v, 1, 1)

    def after(v):
        return pltpu.roll(v, 127, 1)

    for t in range(0, 8 * tiles, chunk):
        at, nxt = slice(first + t, first + t + chunk), slice(first + t + 1, first + t + 1 + chunk)
        for n, p in enumerate((1, 2)):
            shifted[n, at, :] = jnp.where(folded, planes[p, nxt, :], planes[p, at, :])

    for t in range(0, 8 * tiles, chunk):
        at = slice(first + t, first + t + chunk)
        prv = slice(first + t - 1, first + t - 1 + chunk)
        cn, ce, cne = planes[0, at, :], shifted[0, at, :], shifted[1, at, :]
        cew, cnw = shifted[0, prv, :], shifted[1, prv, :]
        diag = planes[3, at, :] + cn + ce + cew + cne + cnw + before(cn + cne + cnw)
        ocean = planes[4, at, :] > 0.0
        root = jnp.sqrt(diag)
        recip = jnp.where(ocean, 1.0 / root, 0.0)
        root = jnp.where(ocean, root, 0.0)
        inv[at, :] = jnp.where(seam, after(recip), recip)
        square[at, :] = root

    for t in range(0, 8 * tiles, chunk):
        at = slice(first + t, first + t + chunk)
        nxt = slice(first + t + 1, first + t + 1 + chunk)
        here, east = inv[at, :], inv[nxt, :]
        up, up_east = after(here), after(east)
        here_up = jnp.where(seam, before(here), here)
        east_up = jnp.where(seam, before(east), east)
        cn, ce, cne = planes[0, at, :] * factor, shifted[0, at, :] * factor, shifted[1, at, :] * factor
        values = (cn * here_up * up, ce * here * east, cne * here_up * up_east, cne * east_up * up, here)
        for n, v in enumerate(values):
            top_part = v.astype(jnp.bfloat16).astype(F32)
            v = v - top_part
            mid_part = v.astype(jnp.bfloat16).astype(F32)
            moved = pltpu.roll(mid_part, span, 1)
            low_part = pltpu.roll(v - mid_part, 2 * span - 128, 1)
            left = jnp.where(lanes < span, top_part, moved)
            right = jnp.where(lanes < 2 * span - 128, moved, low_part)
            right = jnp.where(lanes < 3 * span - 128, right, 0.0)
            to = slice(8 * tiles * n + t, 8 * tiles * n + t + chunk)
            lhs[to, 0:128] = left.astype(jnp.bfloat16)
            lhs[to, 128:256] = right.astype(jnp.bfloat16)

    def spread(p, planes_from, halves):
        found = jnp.dot(lhs[8 * tiles * planes_from :, :], pick[p], preferred_element_type=F32)
        for n in range(planes_from, 5):
            for h in range(halves):
                at = 8 * tiles * (n - planes_from)
                links[n, 2 * p + h, first : first + 8 * tiles, :] = found[
                    at : at + 8 * tiles, 128 * h : 128 * h + 128
                ]

    pairs = pick.shape[0] - 1
    together = 2 - pairs % 2

    @pl.loop(0, pairs // together)
    def _(part):
        for within in range(together):
            spread(together * part + within, 0, 2)

    spread(pairs, 4, 1)


def choose(members, rows, pick):
    groups = 128 // members
    sub_rows = rows // groups
    span = rows + 16
    source = lax.broadcasted_iota(jnp.int32, (256, 256), 0)
    lane = lax.broadcasted_iota(jnp.int32, (256, 256), 1)
    source = source - span * ((source >= span).astype(jnp.int32) + (source >= 2 * span).astype(jnp.int32))
    group = lax.shift_right_logical(lane & 127, members.bit_length() - 1)
    half = lax.shift_right_logical(lane, 7)
    last = (group == groups - 1).astype(jnp.int32)
    base = source - sub_rows * group - half - 8 + ITERS

    @pl.loop(0, pick.shape[0])
    def _(p):
        later = (2 * p + half >= sub_rows + ITERS).astype(jnp.int32)
        hit = base == 2 * p + later * (last - 1)
        pick[p] = jnp.where(hit, 1.0, 0.0).astype(jnp.bfloat16)


def apply(k, links, basis, parts, tiles, tile):
    depth = ITERS - 1 - k
    here, out = basis[k], basis[k + 1]
    old = basis[k - 1] if k else None

    @pl.loop(0, tiles)
    def _(t):
        x0 = PAD - depth + 8 * tile(t)
        mid, east, west = pl.ds(x0, 8), pl.ds(x0 + 1, 8), pl.ds(x0 - 1, 8)

        def three(r):
            return here[r, west, :], here[r, mid, :], here[r, east, :]

        for start, stop in parts:
            dn, cur = three(start - 1), three(start)
            north = links[0, start - 1 + (1 if start > SEAM else 0), mid, :]
            for r in range(start, stop):
                nxt = three(r + 1)
                c = r + (1 if r >= SEAM else 0)
                if r == SEAM:
                    north = links[0, c - 1, mid, :]
                south, north = north, links[0, c, mid, :]
                total = (north * nxt[1] + south * dn[1]) + (
                    links[1, c, mid, :] * cur[2] + links[1, c, west, :] * cur[0]
                )
                total = total + (links[2, c, mid, :] * nxt[2] + links[2, c - 1, west, :] * dn[0])
                total = total + (links[3, c, west, :] * nxt[0] + links[3, c - 1, mid, :] * dn[2])
                total = total - (cur[1] if old is None else cur[1] + old[r, mid, :])
                out[r, mid, :] = total
                dn, cur = cur, nxt


def begin(raw, links, basis):
    @pl.loop(ITERS, SEAM)
    def _(r):
        for t in range(16):
            at = slice(PAD + 8 * t, PAD + 8 * t + 8)
            basis[0][r, at, :] = raw[r, at, :] * links[4, r, at, :]

    apply(0, links, basis, [(ITERS + 1, SEAM - 1)], 15, lambda t: t + 1)
    apply(1, links, basis, [(ITERS + 2, SEAM - 2)], 14, lambda t: t + 1)


def iterate(members, rows, top, raw, links, basis, gram_ref):
    subs = iota(0)
    group = lax.shift_right_logical(iota(1), members.bit_length() - 1)
    for r in range(ITERS, SEAM):
        for t in (0, 17):
            at = slice(PAD - 8 + 8 * t, PAD + 8 * t)
            basis[0][r, at, :] = raw[r, at, :] * links[4, r, at, :]

    apply(0, links, basis, [(1, ITERS + 1), (SEAM - 1, SEAM + ITERS - 1)], 18, lambda t: t)
    apply(0, links, basis, [(ITERS + 1, SEAM - 1)], 3, lambda t: t + 15 * jnp.minimum(t, 1))
    apply(1, links, basis, [(2, ITERS + 2), (SEAM - 2, SEAM + ITERS - 2)], 17, lambda t: t)
    apply(1, links, basis, [(ITERS + 2, SEAM - 2)], 3, lambda t: t + 14 * jnp.minimum(t, 1))
    for k in range(2, ITERS):
        depth = ITERS - 1 - k
        count = (128 + 2 * depth + 7) // 8
        apply(k, links, basis, [(ITERS - depth, SEAM + depth)], count, lambda t: t)

    def body(r, sums):
        sums = list(sums)
        for t in range(16):
            at = slice(PAD + 8 * t, PAD + 8 * t + 8)
            vs = [basis[k][r + ITERS, at, :] for k in range(ITERS + 1)]
            for i in range(ITERS):
                sums[2 * i] = sums[2 * i] + vs[i] * vs[i]
                sums[2 * i + 1] = sums[2 * i + 1] + vs[i] * vs[i + 1]
        return tuple(sums)

    zero = jnp.zeros((8, 128), F32)
    sums = lax.fori_loop(0, SEAM - ITERS, body, (zero,) * (2 * ITERS))
    fold = jnp.logical_and(group == 128 // members - 1, top)

    def across(t, sums):
        sums = list(sums)
        for u in range(4):
            x0 = PAD + 32 * t + 8 * u
            mid, east, west = pl.ds(x0, 8), pl.ds(x0 + 1, 8), pl.ds(x0 - 1, 8)
            north, right, left = links[0, SEAM - 1, mid, :], links[2, SEAM - 1, mid, :], links[3, SEAM - 1, west, :]
            here, over = [], []
            for k in range(ITERS):
                w = basis[k]
                v = north * w[SEAM, mid, :] + right * w[SEAM, east, :] + left * w[SEAM, west, :]
                over.append(jnp.where(fold, v, 0.0))
                here.append(w[SEAM - 1, mid, :])
            for n, (i, j) in enumerate(SKEW):
                sums[n] = sums[n] + (here[i] * over[j] - here[j] * over[i])
        return tuple(sums)

    sums = sums + lax.fori_loop(0, 4, across, (zero,) * len(SKEW))
    pack = [zero] * 4
    for n, s in enumerate(sums):
        for step in (1, 2, 4):
            s = s + pltpu.roll(s, step, 0)
        pack[n // 8] = jnp.where(subs == n % 8, s, pack[n // 8])
    total = zero
    for j, v in enumerate(pack):
        width = members
        while width < 128:
            v = v + pltpu.roll(v, width, 1)
            width *= 2
        total = jnp.where(group == j, v, total)
    gram_ref[...] = total


def solve_kernel(members, rows, ny, nx, rhs_hbm, coup_hbm, center_hbm, mask_hbm, *refs):
    basis, (scale_ref, sum_ref) = refs[: ITERS + 1], refs[ITERS + 1 : ITERS + 3]
    (
        field, links, planes, rhs, coup, center, mask, coef_out, coef_in, rows_out, rows_in, strip_out, corner_out, corner_in, ext,
        shifted, inv, square, lhs, pick, gram, along_x, along_y, load, send, recv,
    ) = refs[ITERS + 3 :]
    groups = 128 // members
    sub_rows = rows // groups
    tall = rhs.shape[1]
    y, x = lax.axis_index("gy"), lax.axis_index("gx")
    top = (y + 1) // ny
    mirror = nx - 1 - x
    east, west = lax.rem(x + 1, nx), lax.rem(x + nx - 1, nx)
    up = (y + 1 - top, x + top * (mirror - x))
    down = (jnp.maximum(y - 1, 0), x)
    loads = [
        pltpu.make_async_copy(coup_hbm, coup, load.at[0]),
        pltpu.make_async_copy(center_hbm, center, load.at[1]),
        pltpu.make_async_copy(mask_hbm, mask, load.at[2]),
        pltpu.make_async_copy(rhs_hbm, rhs.at[:, 0:rows, :], load.at[3]),
    ]
    for c in loads:
        c.start()
    barrier = pltpu.get_barrier_semaphore()

    def greet(there):
        pl.semaphore_signal(barrier, inc=1, device_id=there, device_id_type=pl.DeviceIdType.MESH)

    for step in range(1, nx):
        greet((y, lax.rem(x + step, nx)))
    for step in range(1, ny):
        greet((lax.rem(y + step, ny), x))

    @pl.when(y > 0)
    def _():
        greet((y - 1, east))
        greet((y - 1, west))

    @pl.when(top == 0)
    def _():
        greet((y + 1, east))
        greet((y + 1, west))

    def copy(src, dst, n, m, there):
        return pltpu.make_async_remote_copy(
            src_ref=src,
            dst_ref=dst,
            send_sem=send.at[n],
            recv_sem=recv.at[m],
            device_id=there,
            device_id_type=pl.DeviceIdType.MESH,
        )

    def corner(base, parts):
        found = []
        for e in range(2):
            plain, folded = x + 2 * e - 1, mirror + 1 - 2 * e
            to = lax.rem(plain + top * (folded - plain) + nx, nx)
            k = 1 - e + top * (1 + 2 * e)
            c = copy(
                corner_out.at[e, parts], corner_in.at[k, parts], base + e, base + k, (y + 1 - top, to)
            )
            found.append((jnp.logical_or(top == 0, to != x), c, e, k))
        for e in range(2):
            k = 3 - e
            there = (jnp.maximum(y - 1, 0), east if e else west)
            c = copy(
                corner_out.at[2 + e, parts], corner_in.at[k, parts], base + 2 + e, base + k, there
            )
            found.append((y > 0, c, 2 + e, k))
        return found

    def start_corners(found, parts):
        for n, (remote, c, e, k) in enumerate(found):
            pl.when(remote)(c.start)
            if n < 2:

                @pl.when(jnp.logical_not(remote))
                def _():
                    corner_in[k, parts] = corner_out[e, parts]

    def corner_arrivals(found, base, parts):
        for k in range(4):
            c = copy(corner_out.at[0, parts], corner_in.at[k, parts], base, base + k, (y, east))
            pl.when(y > 0 if k < 2 else found[k - 2][0])(c.wait_recv)

    lanes, subs = iota(1), iota(0)
    flip_lane = jnp.where(top == 1, 127 - lanes, lanes)
    flip_sub = jnp.where(top == 1, 7 - subs, subs)
    tiles = (slice(PAD, PAD + 8), slice(PAD + 120, PAD + 128))
    beyond_tiles = (slice(PAD - 8, PAD), slice(PAD + 128, PAD + 136))
    for c in loads[:3]:
        c.wait()

    def own(p, at):
        if p < 3:
            return coup[p, at, :]
        return center[at, :] if p == 3 else mask[at, :].astype(F32)

    packs = [jnp.zeros((8, 128), F32)] * 4
    plane = lax.shift_right_logical(lanes, 3)
    high_lanes = jnp.where(top == 1, rows + 7 - (lanes & 7), rows + (lanes & 7))
    low_lanes = 8 + (lanes & 7)
    ext[0:8, :] = jnp.zeros((8, 128), F32)
    ext[rows + 8 : 128, :] = jnp.zeros((120 - rows, 128), F32)
    for p in range(5):
        coef_out[0, p] = along(along(own(p, slice(rows - 8, rows)), flip_lane, 1), flip_sub, 0)
        coef_out[1, p] = own(p, slice(0, 8))
        ext[8 : rows + 8, :] = own(p, slice(0, rows))
        turned = ext[...].T
        for e, edge in enumerate((turned[0:8], turned[120:128])):
            strip_out[e, p] = edge
            packs[e] = jnp.where(plane == p, along(edge, high_lanes, 1), packs[e])
            packs[2 + e] = jnp.where(plane == p, along(edge, low_lanes, 1), packs[2 + e])
    for e in range(4):
        corner_out[e, 0] = along(packs[e], flip_sub, 0) if e < 2 else packs[e]
    pl.semaphore_wait(barrier, nx + ny - 2 + 2 * (1 - top) + 2 * jnp.minimum(y, 1))
    coef_up = copy(coef_out.at[0], coef_in.at[top], 0, top, up)
    coef_down = copy(coef_out.at[1], coef_in.at[1], 1, 1, down)
    rows_up = copy(rows_out.at[0], rows_in.at[top], 2, 2 + top, up)
    rows_down = copy(rows_out.at[1], rows_in.at[1], 3, 3, down)
    first = slice(0, 1)
    later = slice(1, 3)
    coef_corners, rows_corners = corner(8, first), corner(12, later)
    sides = [
        copy(strip_out.at[0], planes.at[:, PAD + 128 : PAD + 136, :], 4, 4, (y, west)),
        copy(strip_out.at[1], planes.at[:, PAD - 8 : PAD, :], 5, 5, (y, east)),
    ]
    start_corners(coef_corners, first)
    coef_up.start()
    pl.when(y > 0)(coef_down.start)
    for c in sides:
        c.start()
    flat = rhs.reshape(members * tall, 128)

    def column(row, block):
        return flat[pl.ds(8 * block * tall + row, 8, stride=tall), :]

    blocks = members // 8
    loads[3].wait()
    for q in range(ITERS):
        high = rows - ITERS + q + top * (ITERS - 1 - 2 * q)
        for b in range(blocks):
            at = slice(q * members + 8 * b, q * members + 8 * b + 8)
            rows_out[0, at, :] = along(column(high, b), flip_lane, 1)
            rows_out[1, at, :] = column(q, b)

    @pl.loop(0, sub_rows // 4)
    def _(part):
        for within in range(4):
            r = 4 * part + within
            stack = [column(sub_rows * g + r, b) for g in range(groups) for b in range(blocks)]
            field[r + ITERS, PAD : PAD + 128, :] = jnp.concatenate(stack, axis=0).T

    member = lanes & (members - 1)
    group = lax.shift_right_logical(lanes, members.bit_length() - 1)
    for e in range(2):
        packs = [[jnp.zeros((8, 128), F32)] * 2 for _ in range(2)]
        for q in range(ITERS):
            here = group == q % groups
            v = field[sub_rows + q + top * (ITERS - 1 - 2 * q), tiles[e], :]
            v = along(v, member + (128 - members), 1)
            packs[0][q // groups] = jnp.where(here, v, packs[0][q // groups])
            v = along(field[ITERS + q, tiles[e], :], member, 1)
            packs[1][q // groups] = jnp.where(here, v, packs[1][q // groups])
        for n in range(2):
            corner_out[e, 1 + n] = along(packs[0][n], flip_sub, 0)
            corner_out[2 + e, 1 + n] = packs[1][n]
    inner = slice(ITERS, ITERS + sub_rows)
    more = [
        copy(field.at[inner, tiles[0], :], field.at[inner, beyond_tiles[1], :], 6, 6, (y, west)),
        copy(field.at[inner, tiles[1], :], field.at[inner, beyond_tiles[0], :], 7, 7, (y, east)),
    ]
    start_corners(rows_corners, later)
    for c in more:
        c.start()
    choose(members, rows, pick)
    coef_north = copy(coef_out.at[1], coef_in.at[1], 1, 1, down)
    coef_south = copy(coef_out.at[0], coef_in.at[0], 0, 0, up)
    coef_north.wait_recv()
    pl.when(y > 0)(coef_south.wait_recv)
    rows_up.start()
    pl.when(y > 0)(rows_down.start)
    for p in range(5):
        beyond = coef_in[1, p]
        moved = pltpu.roll(beyond, 1, 0)
        if p in (0, 2):
            last = jnp.broadcast_to(own(p, slice(rows - 1, rows)), (8, 128))
            beyond = jnp.where(top == 1, beyond, jnp.where(subs == 0, last, moved))
        else:
            beyond = jnp.where(subs == 0, beyond, moved)
        ext[0:8, :] = jnp.where(y == 0, 0.0, coef_in[0, p])
        ext[8 : rows + 8, :] = own(p, slice(0, rows))
        ext[rows + 8 : rows + 16, :] = beyond
        planes[p, PAD : PAD + 128, :] = ext[...].T
    for c in sides:
        c.wait_recv()
    corner_arrivals(coef_corners, 8, first)
    for e in range(2):
        low, high = corner_in[e, 0], corner_in[2 + e, 0]
        for p in range(5):
            strip = planes[p, beyond_tiles[e], :]
            shift = 1 - top if p in (0, 2) else 1
            idx = jnp.clip(lanes - (rows + 8) - shift, 0, 7) + 8 * p
            north = along(high, idx, 1)
            if p in (0, 2):
                joint = jnp.logical_and(lanes == rows + 8, top == 0)
                north = jnp.where(joint, pltpu.roll(strip, 1, 1), north)
            south = jnp.where(y == 0, 0.0, along(low, (lanes & 7) + 8 * p, 1))
            outside = jnp.logical_and(lanes >= rows + 8, lanes < rows + 16)
            strip = jnp.where(lanes < 8, south, jnp.where(outside, north, strip))
            planes[p, beyond_tiles[e], :] = strip
    prepare(members, rows, y == ny - 1, planes, shifted, inv, links, square, lhs, pick)
    begin(field, links, basis)
    copy(rows_out.at[1], rows_in.at[1], 3, 3, down).wait_recv()
    pl.when(y > 0)(copy(rows_out.at[0], rows_in.at[0], 2, 2, up).wait_recv)

    def arrived(side, q, b):
        return rows_in[side, pl.ds(pl.multiple_of(q * members, 8) + 8 * b, 8), :]

    @pl.loop(0, ITERS // 2)
    def _(part):
        for within in range(2):
            q = 2 * part + within
            low = [jnp.where(y == 0, 0.0, arrived(0, q, b)) for b in range(blocks)]
            low += [column(sub_rows * g - ITERS + q, b) for g in range(1, groups) for b in range(blocks)]
            basis[0][q, PAD : PAD + 128, :] = (
                jnp.concatenate(low, axis=0).T * links[4, q, PAD : PAD + 128, :]
            )
            high = [column(sub_rows * g + q, b) for g in range(1, groups) for b in range(blocks)]
            high += [arrived(1, q, b) for b in range(blocks)]
            r = q + ITERS + sub_rows
            basis[0][r, PAD : PAD + 128, :] = (
                jnp.concatenate(high, axis=0).T * links[4, r + 1, PAD : PAD + 128, :]
            )

    for c in more:
        c.wait_recv()
    corner_arrivals(rows_corners, 12, later)
    for e in range(2):
        for q in range(ITERS):
            idx = member + members * (q % groups)
            south = along(corner_in[e, 1 + q // groups], idx, 1)
            south = jnp.where(y == 0, 0.0, south)
            v = pltpu.roll(field[sub_rows + q, beyond_tiles[e], :], members, 1)
            v = jnp.where(group == 0, south, v)
            basis[0][q, beyond_tiles[e], :] = v * links[4, q, beyond_tiles[e], :]
            north = along(corner_in[2 + e, 1 + q // groups], idx, 1)
            v = pltpu.roll(field[ITERS + q, beyond_tiles[e], :], 128 - members, 1)
            v, r = jnp.where(group == groups - 1, north, v), ITERS + sub_rows + q
            basis[0][r, beyond_tiles[e], :] = v * links[4, r + 1, beyond_tiles[e], :]
    coef_up.wait_send()
    rows_up.wait_send()

    @pl.when(y > 0)
    def _():
        coef_down.wait_send()
        rows_down.wait_send()

    for c in sides + more:
        c.wait_send()
    for remote, c, _, _ in coef_corners + rows_corners:
        pl.when(remote)(c.wait_send)
    iterate(members, rows, y == ny - 1, field, links, basis, gram)

    def sent(source, dst, n, there):
        c = copy(source, dst, n, n, there)
        c.start()
        return c

    across = [sent(gram, along_x.at[s], 15 + s, (y, lax.rem(x + s, nx))) for s in range(1, nx)]
    scale_ref[0] = inv[PAD : PAD + 128, :].T
    scale_ref[1] = square[PAD : PAD + 128, :].T
    for c in across:
        c.wait()
    along_x[0] = sum((along_x[s] for s in range(1, nx)), gram[...])
    across = [
        sent(along_x.at[0], along_y.at[s], 14 + nx + s, (lax.rem(y + s, ny), x)) for s in range(1, ny)
    ]
    for c in across:
        c.wait()
    sum_ref[...] = sum((along_y[s] for s in range(1, ny)), along_x[0])


def coefficients(gram):
    def g(i, j):
        return gram[min(i, j)][max(i, j)]

    def applied(p):
        q = []
        for k in range(ITERS + 1):
            terms = []
            if k < len(p):
                terms.append((1.0 - ROOT) * p[k])
            if 0 < k <= len(p):
                terms.append(-ROOT * p[k - 1])
            if k + 1 < len(p):
                terms.append(-ROOT * p[k + 1])
            if terms:
                q.append(sum(terms[1:], terms[0]))
        return q

    def inner(p, q):
        total = None
        for i, a in enumerate(p):
            row = None
            for j, b in enumerate(q):
                t = g(i, j) * b
                row = t if row is None else row + t
            t = a * row
            total = t if total is None else total + t
        return total

    one = jnp.ones_like(gram[0][0])
    z, p, x = [one], [one], []
    rz = g(0, 0)
    for iteration in range(ITERS):
        q = applied(p)
        step = rz / inner(p, q)
        x = [(x[k] if k < len(x) else 0.0) + step * p[k] for k in range(len(p))]
        z = [(z[k] if k < len(z) else 0.0) - step * q[k] for k in range(len(q))]
        if iteration + 1 < ITERS:
            rz_new = inner(z, z)
            beta = rz_new / rz
            p = [z[k] + (beta * p[k] if k < len(p) else 0.0) for k in range(len(z))]
            rz = rz_new
    return x, z


def combine_kernel(members, rows, *refs):
    basis, (scale_ref, sum_ref, x_out, r_out, stage, sems) = refs[: ITERS + 1], refs[ITERS + 1 :]
    groups = 128 // members
    sub_rows = rows // groups
    tall = stage.shape[2]
    lanes = iota(1)
    sums = sum_ref[...]
    tiles = [along(sums, (lanes & (members - 1)) + members * j, 1) for j in range(4)]
    found = [
        jnp.broadcast_to(tiles[n // 8][n % 8 : n % 8 + 1, :], (8, 128))
        for n in range(2 * ITERS + len(SKEW))
    ]
    gram = [[None] * (ITERS + 1) for _ in range(ITERS + 1)]
    for i in range(ITERS):
        gram[i][i], gram[i][i + 1] = found[2 * i], found[2 * i + 1]
    skew = dict(zip(SKEW, found[2 * ITERS :]))
    for gap in range(2, ITERS + 1):
        for i in range(ITERS + 1 - gap):
            j = i + gap - 1
            v = gram[i + 1][j] - gram[i][j - 1] + skew[i, j]
            gram[i][j + 1] = v + gram[i - 1][j] if i else v
    xs, zs = coefficients(gram)
    flat = stage.reshape(2 * members * tall, 128)
    blocks = members // 8
    half = sub_rows // 2
    outs = (x_out, r_out)

    def drain(h):
        copies = []
        for o in range(2):
            for g in range(groups):
                at = slice(sub_rows * g + half * h, sub_rows * g + half * (h + 1))
                copies.append(
                    pltpu.make_async_copy(stage.at[o, :, at, :], outs[o].at[:, at, :], sems.at[h, o, g])
                )
        return copies

    started = []
    for h in range(2):

        def row(r):
            found = ([], [])
            for t in range(16):
                at = slice(PAD + 8 * t, PAD + 8 * t + 8)
                vs = [basis[k][r + ITERS, at, :] for k in range(ITERS + 1)]
                found[0].append(sum((xs[k] * vs[k] for k in range(1, ITERS)), xs[0] * vs[0]))
                found[1].append(sum((zs[k] * vs[k] for k in range(1, ITERS + 1)), zs[0] * vs[0]))
            for o in range(2):
                turned = jnp.concatenate(found[o], axis=0).T
                for g in range(groups):
                    row = sub_rows * g + r
                    scale = jnp.broadcast_to(scale_ref[o, pl.ds(row + 8, 1), :], (8, 128))
                    for b in range(blocks):
                        n = 8 * (g * blocks + b)
                        at = pl.ds((o * members + 8 * b) * tall + row, 8, stride=tall)
                        flat[at, :] = turned[n : n + 8, :] * scale

        @pl.loop(0, half // 4)
        def _(part):
            for within in range(4):
                row(half * h + 4 * part + within)

        for c in drain(h):
            c.start()
            started.append(c)
    for c in started:
        c.wait()


def on_device(right_side, couplings, center, ocean_mask):
    members, rows, columns = right_side.shape
    groups = 128 // members
    sub_rows = rows // groups
    assert lax.axis_size("gx") > 2 and ITERS <= 2 * groups
    assert columns == 128 and members % 8 == 0 and groups * members == 128
    assert 3 * (rows + 16) <= 256 < 4 * (rows + 16) and 2 * (rows + 16) >= 128 and sub_rows == SEAM - ITERS
    ny, nx = lax.axis_size("gy"), lax.axis_size("gx")
    vmem = pl.BlockSpec(memory_space=pltpu.VMEM)
    hbm = pl.BlockSpec(memory_space=pltpu.HBM)
    deep, wide = sub_rows + 2 * ITERS, columns + 2 * PAD + 8

    inputs = [
        pltpu.with_memory_space_constraint(v, pltpu.HBM)
        for v in (right_side, couplings, center, ocean_mask)
    ]

    def first(*refs):
        solve_kernel(members, rows, ny, nx, *refs)

    *basis, scale, sums = pl.pallas_call(
        first,
        out_shape=(pltpu.VMEM((deep, wide, 128), F32),) * (ITERS + 1)
        + (pltpu.VMEM((2, 128, 128), F32), pltpu.VMEM((8, 128), F32)),
        in_specs=[hbm] * 4,
        out_specs=(vmem,) * (ITERS + 3),
        scratch_shapes=[
            pltpu.VMEM((deep, wide, 128), F32),
            pltpu.VMEM((5, deep + 3, wide, 128), F32),
            pltpu.VMEM((5, wide, 128), F32),
            pltpu.VMEM((members, rows + 8, columns), F32),
            pltpu.VMEM((3, rows, columns), F32),
            pltpu.VMEM((rows, columns), F32),
            pltpu.VMEM((rows, columns), jnp.int32),
            pltpu.VMEM((2, 5, 8, columns), F32),
            pltpu.VMEM((2, 5, 8, columns), F32),
            pltpu.VMEM((2, ITERS * members, columns), F32),
            pltpu.VMEM((2, ITERS * members, columns), F32),
            pltpu.VMEM((2, 5, 8, 128), F32),
            pltpu.VMEM((4, 3, 8, 128), F32),
            pltpu.VMEM((4, 3, 8, 128), F32),
            pltpu.VMEM((128, 128), F32),
            pltpu.VMEM((2, wide, 128), F32),
            pltpu.VMEM((wide, 128), F32),
            pltpu.VMEM((wide, 128), F32),
            pltpu.VMEM((5 * 144, 256), jnp.bfloat16),
            pltpu.VMEM(((deep + 2) // 2, 256, 256), jnp.bfloat16),
            pltpu.VMEM((8, 128), F32),
            pltpu.VMEM((nx, 8, 128), F32),
            pltpu.VMEM((ny, 8, 128), F32),
            pltpu.SemaphoreType.DMA((4,)),
            pltpu.SemaphoreType.DMA((14 + nx + ny,)),
            pltpu.SemaphoreType.DMA((14 + nx + ny,)),
        ],
        compiler_params=pltpu.CompilerParams(
            collective_id=0, has_side_effects=True, vmem_limit_bytes=GRANT
        ),
    )(*inputs)

    def second(*refs):
        combine_kernel(members, rows, *refs)

    return pl.pallas_call(
        second,
        out_shape=(jax.ShapeDtypeStruct(right_side.shape, F32),) * 2,
        in_specs=[vmem] * (ITERS + 3),
        out_specs=(hbm, hbm),
        compiler_params=pltpu.CompilerParams(vmem_limit_bytes=GRANT),
        scratch_shapes=[
            pltpu.VMEM((2, members, rows + 8, columns), F32),
            pltpu.SemaphoreType.DMA((2, 2, groups)),
        ],
    )(*basis, scale, sums)


def solution(mesh):
    in_specs = (P(None, "gy", "gx"), P(None, "gy", "gx"), P("gy", "gx"), P("gy", "gx"))
    out_specs = (P(None, "gy", "gx"), P(None, "gy", "gx"))
    return jax.shard_map(
        on_device, mesh=mesh, in_specs=in_specs, out_specs=out_specs, check_vma=False
    )
```

```python
import jax
import jax.numpy as jnp
from jax import lax
from jax.experimental import pallas as pl
from jax.experimental.pallas import tpu as pltpu
from jax.sharding import PartitionSpec as P

ITERS = 6
ROOT = 0.18
PAD = 16
VMEM = 67043328
GRANT = 24 * 1024 * 1024
SKEW = [(i, j) for i in range(ITERS) for j in range(i + 1, ITERS)]
SEAM = 16 + ITERS
F32 = jnp.float32


def iota(dim):
    return lax.broadcasted_iota(jnp.int32, (8, 128), dim)


def along(x, idx, axis):
    return jnp.take_along_axis(x, idx, axis=axis, mode="promise_in_bounds")


def prepare(members, rows, top, planes, shifted, inv, links, square, lhs, pick):
    first, chunk, tiles = PAD - 8, 48, 18
    lanes = lax.broadcasted_iota(jnp.int32, (chunk, 128), 1)
    seam = lanes == rows + 8
    folded = jnp.logical_and(top, lanes >= rows + 8)
    span = rows + 16
    factor = 1.0 / ROOT

    def before(v):
        return pltpu.roll(v, 1, 1)

    def after(v):
        return pltpu.roll(v, 127, 1)

    for t in range(0, 8 * tiles, chunk):
        at, nxt = slice(first + t, first + t + chunk), slice(first + t + 1, first + t + 1 + chunk)
        for n, p in enumerate((1, 2)):
            shifted[n, at, :] = jnp.where(folded, planes[p, nxt, :], planes[p, at, :])

    for t in range(0, 8 * tiles, chunk):
        at = slice(first + t, first + t + chunk)
        prv = slice(first + t - 1, first + t - 1 + chunk)
        cn, ce, cne = planes[0, at, :], shifted[0, at, :], shifted[1, at, :]
        cew, cnw = shifted[0, prv, :], shifted[1, prv, :]
        diag = planes[3, at, :] + cn + ce + cew + cne + cnw + before(cn + cne + cnw)
        ocean = planes[4, at, :] > 0.0
        root = jnp.sqrt(diag)
        recip = jnp.where(ocean, 1.0 / root, 0.0)
        root = jnp.where(ocean, root, 0.0)
        inv[at, :] = jnp.where(seam, after(recip), recip)
        square[at, :] = root

    for t in range(0, 8 * tiles, chunk):
        at = slice(first + t, first + t + chunk)
        nxt = slice(first + t + 1, first + t + 1 + chunk)
        here, east = inv[at, :], inv[nxt, :]
        up, up_east = after(here), after(east)
        here_up = jnp.where(seam, before(here), here)
        east_up = jnp.where(seam, before(east), east)
        cn, ce, cne = planes[0, at, :] * factor, shifted[0, at, :] * factor, shifted[1, at, :] * factor
        values = (cn * here_up * up, ce * here * east, cne * here_up * up_east, cne * east_up * up, here)
        for n, v in enumerate(values):
            top_part = v.astype(jnp.bfloat16).astype(F32)
            v = v - top_part
            mid_part = v.astype(jnp.bfloat16).astype(F32)
            moved = pltpu.roll(mid_part, span, 1)
            low_part = pltpu.roll(v - mid_part, 2 * span - 128, 1)
            left = jnp.where(lanes < span, top_part, moved)
            right = jnp.where(lanes < 2 * span - 128, moved, low_part)
            right = jnp.where(lanes < 3 * span - 128, right, 0.0)
            to = slice(8 * tiles * n + t, 8 * tiles * n + t + chunk)
            lhs[to, 0:128] = left.astype(jnp.bfloat16)
            lhs[to, 128:256] = right.astype(jnp.bfloat16)

    def spread(p, planes_from, halves):
        found = jnp.dot(lhs[8 * tiles * planes_from :, :], pick[p], preferred_element_type=F32)
        for n in range(planes_from, 5):
            for h in range(halves):
                at = 8 * tiles * (n - planes_from)
                links[n, 2 * p + h, first : first + 8 * tiles, :] = found[
                    at : at + 8 * tiles, 128 * h : 128 * h + 128
                ]

    pairs = pick.shape[0] - 1
    together = 2 - pairs % 2

    @pl.loop(0, pairs // together)
    def _(part):
        for within in range(together):
            spread(together * part + within, 0, 2)

    spread(pairs, 4, 1)


def choose(members, rows, pick):
    groups = 128 // members
    sub_rows = rows // groups
    span = rows + 16
    source = lax.broadcasted_iota(jnp.int32, (256, 256), 0)
    lane = lax.broadcasted_iota(jnp.int32, (256, 256), 1)
    source = source - span * ((source >= span).astype(jnp.int32) + (source >= 2 * span).astype(jnp.int32))
    group = lax.shift_right_logical(lane & 127, members.bit_length() - 1)
    half = lax.shift_right_logical(lane, 7)
    last = (group == groups - 1).astype(jnp.int32)
    base = source - sub_rows * group - half - 8 + ITERS

    @pl.loop(0, pick.shape[0])
    def _(p):
        later = (2 * p + half >= sub_rows + ITERS).astype(jnp.int32)
        hit = base == 2 * p + later * (last - 1)
        pick[p] = jnp.where(hit, 1.0, 0.0).astype(jnp.bfloat16)


def apply(k, links, basis, parts, tiles, tile):
    depth = ITERS - 1 - k
    here, out = basis[k], basis[k + 1]
    old = basis[k - 1] if k else None

    @pl.loop(0, tiles)
    def _(t):
        x0 = PAD - depth + 8 * tile(t)
        mid, east, west = pl.ds(x0, 8), pl.ds(x0 + 1, 8), pl.ds(x0 - 1, 8)

        def three(r):
            return here[r, west, :], here[r, mid, :], here[r, east, :]

        for start, stop in parts:
            dn, cur = three(start - 1), three(start)
            north = links[0, start - 1 + (1 if start > SEAM else 0), mid, :]
            for r in range(start, stop):
                nxt = three(r + 1)
                c = r + (1 if r >= SEAM else 0)
                if r == SEAM:
                    north = links[0, c - 1, mid, :]
                south, north = north, links[0, c, mid, :]
                total = (north * nxt[1] + south * dn[1]) + (
                    links[1, c, mid, :] * cur[2] + links[1, c, west, :] * cur[0]
                )
                total = total + (links[2, c, mid, :] * nxt[2] + links[2, c - 1, west, :] * dn[0])
                total = total + (links[3, c, west, :] * nxt[0] + links[3, c - 1, mid, :] * dn[2])
                total = total - (cur[1] if old is None else cur[1] + old[r, mid, :])
                out[r, mid, :] = total
                dn, cur = cur, nxt


def begin(raw, links, basis):
    @pl.loop(ITERS, SEAM)
    def _(r):
        for t in range(16):
            at = slice(PAD + 8 * t, PAD + 8 * t + 8)
            basis[0][r, at, :] = raw[r, at, :] * links[4, r, at, :]

    apply(0, links, basis, [(ITERS + 1, SEAM - 1)], 15, lambda t: t + 1)
    apply(1, links, basis, [(ITERS + 2, SEAM - 2)], 14, lambda t: t + 1)


def iterate(members, rows, top, raw, links, basis, gram_ref):
    subs = iota(0)
    group = lax.shift_right_logical(iota(1), members.bit_length() - 1)
    for r in range(ITERS, SEAM):
        for t in (0, 17):
            at = slice(PAD - 8 + 8 * t, PAD + 8 * t)
            basis[0][r, at, :] = raw[r, at, :] * links[4, r, at, :]

    apply(0, links, basis, [(1, ITERS + 1), (SEAM - 1, SEAM + ITERS - 1)], 18, lambda t: t)
    apply(0, links, basis, [(ITERS + 1, SEAM - 1)], 3, lambda t: t + 15 * jnp.minimum(t, 1))
    apply(1, links, basis, [(2, ITERS + 2), (SEAM - 2, SEAM + ITERS - 2)], 17, lambda t: t)
    apply(1, links, basis, [(ITERS + 2, SEAM - 2)], 3, lambda t: t + 14 * jnp.minimum(t, 1))
    for k in range(2, ITERS - 1):
        depth = ITERS - 1 - k
        count = (128 + 2 * depth + 7) // 8
        apply(k, links, basis, [(ITERS - depth, SEAM + depth)], count, lambda t: t)

    zero = jnp.zeros((8, 128), F32)
    fold = jnp.logical_and(group == 128 // members - 1, top)
    newest = basis[ITERS - 1]

    def body(r, sums):
        sums = list(sums)
        r = r + ITERS
        share = jnp.where(jnp.logical_and(fold, r == SEAM - 1), 0.5, 1.0)
        for t in range(16):
            at = slice(PAD + 8 * t, PAD + 8 * t + 8)
            east, west = (slice(PAD + 8 * t + d, PAD + 8 * t + d + 8) for d in (1, -1))
            vs = [basis[k][r, at, :] for k in range(ITERS)]
            for i in range(ITERS):
                sums[2 * i] = sums[2 * i] + vs[i] * vs[i]
                if i + 1 < ITERS:
                    sums[2 * i + 1] = sums[2 * i + 1] + vs[i] * vs[i + 1]
            ahead = links[0, r, at, :] * newest[r + 1, at, :]
            ahead = ahead + links[2, r, at, :] * newest[r + 1, east, :]
            ahead = ahead + links[3, r, west, :] * newest[r + 1, west, :]
            ahead = ahead * share + links[1, r, at, :] * newest[r, east, :]
            sums[-1] = sums[-1] + vs[-1] * ahead
        return tuple(sums)

    sums = lax.fori_loop(0, SEAM - ITERS, body, (zero,) * (2 * ITERS))
    sums = sums[:-1] + (sums[-1] + sums[-1],)

    def across(t, sums):
        sums = list(sums)
        for u in range(4):
            x0 = PAD + 32 * t + 8 * u
            mid, east, west = pl.ds(x0, 8), pl.ds(x0 + 1, 8), pl.ds(x0 - 1, 8)
            north, right, left = links[0, SEAM - 1, mid, :], links[2, SEAM - 1, mid, :], links[3, SEAM - 1, west, :]
            here, over = [], []
            for k in range(ITERS):
                w = basis[k]
                v = north * w[SEAM, mid, :] + right * w[SEAM, east, :] + left * w[SEAM, west, :]
                over.append(jnp.where(fold, v, 0.0))
                here.append(w[SEAM - 1, mid, :])
            for n, (i, j) in enumerate(SKEW):
                sums[n] = sums[n] + (here[i] * over[j] - here[j] * over[i])
        return tuple(sums)

    sums = sums + lax.fori_loop(0, 4, across, (zero,) * len(SKEW))
    pack = [zero] * 4
    for n, s in enumerate(sums):
        for step in (1, 2, 4):
            s = s + pltpu.roll(s, step, 0)
        pack[n // 8] = jnp.where(subs == n % 8, s, pack[n // 8])
    total = zero
    for j, v in enumerate(pack):
        width = members
        while width < 128:
            v = v + pltpu.roll(v, width, 1)
            width *= 2
        total = jnp.where(group == j, v, total)
    gram_ref[...] = total


def solve_kernel(members, rows, ny, nx, rhs_hbm, coup_hbm, center_hbm, mask_hbm, *refs):
    basis, (scale_ref, sum_ref) = refs[: ITERS + 1], refs[ITERS + 1 : ITERS + 3]
    (
        field, links, planes, rhs, coup, center, mask, coef_out, coef_in, rows_out, rows_in, strip_out, corner_out, corner_in, ext,
        shifted, inv, square, lhs, pick, gram, along_x, along_y, load, send, recv,
    ) = refs[ITERS + 3 :]
    groups = 128 // members
    sub_rows = rows // groups
    tall = rhs.shape[1]
    y, x = lax.axis_index("gy"), lax.axis_index("gx")
    top = (y + 1) // ny
    mirror = nx - 1 - x
    east, west = lax.rem(x + 1, nx), lax.rem(x + nx - 1, nx)
    up = (y + 1 - top, x + top * (mirror - x))
    down = (jnp.maximum(y - 1, 0), x)
    loads = [
        pltpu.make_async_copy(coup_hbm, coup, load.at[0]),
        pltpu.make_async_copy(center_hbm, center, load.at[1]),
        pltpu.make_async_copy(mask_hbm, mask, load.at[2]),
        pltpu.make_async_copy(rhs_hbm, rhs.at[:, 0:rows, :], load.at[3]),
    ]
    for c in loads:
        c.start()
    barrier = pltpu.get_barrier_semaphore()

    def greet(there):
        pl.semaphore_signal(barrier, inc=1, device_id=there, device_id_type=pl.DeviceIdType.MESH)

    for step in range(1, nx):
        greet((y, lax.rem(x + step, nx)))
    for step in range(1, ny):
        greet((lax.rem(y + step, ny), x))

    @pl.when(y > 0)
    def _():
        greet((y - 1, east))
        greet((y - 1, west))

    @pl.when(top == 0)
    def _():
        greet((y + 1, east))
        greet((y + 1, west))

    def copy(src, dst, n, m, there):
        return pltpu.make_async_remote_copy(
            src_ref=src,
            dst_ref=dst,
            send_sem=send.at[n],
            recv_sem=recv.at[m],
            device_id=there,
            device_id_type=pl.DeviceIdType.MESH,
        )

    def corner(base, parts):
        found = []
        for e in range(2):
            plain, folded = x + 2 * e - 1, mirror + 1 - 2 * e
            to = lax.rem(plain + top * (folded - plain) + nx, nx)
            k = 1 - e + top * (1 + 2 * e)
            c = copy(
                corner_out.at[e, parts], corner_in.at[k, parts], base + e, base + k, (y + 1 - top, to)
            )
            found.append((jnp.logical_or(top == 0, to != x), c, e, k))
        for e in range(2):
            k = 3 - e
            there = (jnp.maximum(y - 1, 0), east if e else west)
            c = copy(
                corner_out.at[2 + e, parts], corner_in.at[k, parts], base + 2 + e, base + k, there
            )
            found.append((y > 0, c, 2 + e, k))
        return found

    def start_corners(found, parts):
        for n, (remote, c, e, k) in enumerate(found):
            pl.when(remote)(c.start)
            if n < 2:

                @pl.when(jnp.logical_not(remote))
                def _():
                    corner_in[k, parts] = corner_out[e, parts]

    def corner_arrivals(found, base, parts):
        for k in range(4):
            c = copy(corner_out.at[0, parts], corner_in.at[k, parts], base, base + k, (y, east))
            pl.when(y > 0 if k < 2 else found[k - 2][0])(c.wait_recv)

    lanes, subs = iota(1), iota(0)
    flip_lane = jnp.where(top == 1, 127 - lanes, lanes)
    flip_sub = jnp.where(top == 1, 7 - subs, subs)
    tiles = (slice(PAD, PAD + 8), slice(PAD + 120, PAD + 128))
    beyond_tiles = (slice(PAD - 8, PAD), slice(PAD + 128, PAD + 136))
    for c in loads[:3]:
        c.wait()

    def own(p, at):
        if p < 3:
            return coup[p, at, :]
        return center[at, :] if p == 3 else mask[at, :].astype(F32)

    packs = [jnp.zeros((8, 128), F32)] * 4
    plane = lax.shift_right_logical(lanes, 3)
    high_lanes = jnp.where(top == 1, rows + 7 - (lanes & 7), rows + (lanes & 7))
    low_lanes = 8 + (lanes & 7)
    ext[0:8, :] = jnp.zeros((8, 128), F32)
    ext[rows + 8 : 128, :] = jnp.zeros((120 - rows, 128), F32)
    for p in range(5):
        coef_out[0, p] = along(along(own(p, slice(rows - 8, rows)), flip_lane, 1), flip_sub, 0)
        coef_out[1, p] = own(p, slice(0, 8))
        ext[8 : rows + 8, :] = own(p, slice(0, rows))
        turned = ext[...].T
        for e, edge in enumerate((turned[0:8], turned[120:128])):
            strip_out[e, p] = edge
            packs[e] = jnp.where(plane == p, along(edge, high_lanes, 1), packs[e])
            packs[2 + e] = jnp.where(plane == p, along(edge, low_lanes, 1), packs[2 + e])
    for e in range(4):
        corner_out[e, 0] = along(packs[e], flip_sub, 0) if e < 2 else packs[e]
    pl.semaphore_wait(barrier, nx + ny - 2 + 2 * (1 - top) + 2 * jnp.minimum(y, 1))
    coef_up = copy(coef_out.at[0], coef_in.at[top], 0, top, up)
    coef_down = copy(coef_out.at[1], coef_in.at[1], 1, 1, down)
    rows_up = copy(rows_out.at[0], rows_in.at[top], 2, 2 + top, up)
    rows_down = copy(rows_out.at[1], rows_in.at[1], 3, 3, down)
    first = slice(0, 1)
    later = slice(1, 3)
    coef_corners, rows_corners = corner(8, first), corner(12, later)
    sides = [
        copy(strip_out.at[0], planes.at[:, PAD + 128 : PAD + 136, :], 4, 4, (y, west)),
        copy(strip_out.at[1], planes.at[:, PAD - 8 : PAD, :], 5, 5, (y, east)),
    ]
    start_corners(coef_corners, first)
    coef_up.start()
    pl.when(y > 0)(coef_down.start)
    for c in sides:
        c.start()
    flat = rhs.reshape(members * tall, 128)

    def column(row, block):
        return flat[pl.ds(8 * block * tall + row, 8, stride=tall), :]

    blocks = members // 8
    loads[3].wait()
    for q in range(ITERS):
        high = rows - ITERS + q + top * (ITERS - 1 - 2 * q)
        for b in range(blocks):
            at = slice(q * members + 8 * b, q * members + 8 * b + 8)
            rows_out[0, at, :] = along(column(high, b), flip_lane, 1)
            rows_out[1, at, :] = column(q, b)

    @pl.loop(0, sub_rows // 4)
    def _(part):
        for within in range(4):
            r = 4 * part + within
            stack = [column(sub_rows * g + r, b) for g in range(groups) for b in range(blocks)]
            field[r + ITERS, PAD : PAD + 128, :] = jnp.concatenate(stack, axis=0).T

    member = lanes & (members - 1)
    group = lax.shift_right_logical(lanes, members.bit_length() - 1)
    for e in range(2):
        packs = [[jnp.zeros((8, 128), F32)] * 2 for _ in range(2)]
        for q in range(ITERS):
            here = group == q % groups
            v = field[sub_rows + q + top * (ITERS - 1 - 2 * q), tiles[e], :]
            v = along(v, member + (128 - members), 1)
            packs[0][q // groups] = jnp.where(here, v, packs[0][q // groups])
            v = along(field[ITERS + q, tiles[e], :], member, 1)
            packs[1][q // groups] = jnp.where(here, v, packs[1][q // groups])
        for n in range(2):
            corner_out[e, 1 + n] = along(packs[0][n], flip_sub, 0)
            corner_out[2 + e, 1 + n] = packs[1][n]
    inner = slice(ITERS, ITERS + sub_rows)
    more = [
        copy(field.at[inner, tiles[0], :], field.at[inner, beyond_tiles[1], :], 6, 6, (y, west)),
        copy(field.at[inner, tiles[1], :], field.at[inner, beyond_tiles[0], :], 7, 7, (y, east)),
    ]
    start_corners(rows_corners, later)
    for c in more:
        c.start()
    choose(members, rows, pick)
    coef_north = copy(coef_out.at[1], coef_in.at[1], 1, 1, down)
    coef_south = copy(coef_out.at[0], coef_in.at[0], 0, 0, up)
    coef_north.wait_recv()
    pl.when(y > 0)(coef_south.wait_recv)
    rows_up.start()
    pl.when(y > 0)(rows_down.start)
    for p in range(5):
        beyond = coef_in[1, p]
        moved = pltpu.roll(beyond, 1, 0)
        if p in (0, 2):
            last = jnp.broadcast_to(own(p, slice(rows - 1, rows)), (8, 128))
            beyond = jnp.where(top == 1, beyond, jnp.where(subs == 0, last, moved))
        else:
            beyond = jnp.where(subs == 0, beyond, moved)
        ext[0:8, :] = jnp.where(y == 0, 0.0, coef_in[0, p])
        ext[8 : rows + 8, :] = own(p, slice(0, rows))
        ext[rows + 8 : rows + 16, :] = beyond
        planes[p, PAD : PAD + 128, :] = ext[...].T
    for c in sides:
        c.wait_recv()
    corner_arrivals(coef_corners, 8, first)
    for e in range(2):
        low, high = corner_in[e, 0], corner_in[2 + e, 0]
        for p in range(5):
            strip = planes[p, beyond_tiles[e], :]
            shift = 1 - top if p in (0, 2) else 1
            idx = jnp.clip(lanes - (rows + 8) - shift, 0, 7) + 8 * p
            north = along(high, idx, 1)
            if p in (0, 2):
                joint = jnp.logical_and(lanes == rows + 8, top == 0)
                north = jnp.where(joint, pltpu.roll(strip, 1, 1), north)
            south = jnp.where(y == 0, 0.0, along(low, (lanes & 7) + 8 * p, 1))
            outside = jnp.logical_and(lanes >= rows + 8, lanes < rows + 16)
            strip = jnp.where(lanes < 8, south, jnp.where(outside, north, strip))
            planes[p, beyond_tiles[e], :] = strip
    prepare(members, rows, y == ny - 1, planes, shifted, inv, links, square, lhs, pick)
    begin(field, links, basis)
    copy(rows_out.at[1], rows_in.at[1], 3, 3, down).wait_recv()
    pl.when(y > 0)(copy(rows_out.at[0], rows_in.at[0], 2, 2, up).wait_recv)

    def arrived(side, q, b):
        return rows_in[side, q * members + 8 * b : q * members + 8 * b + 8, :]

    for _ in range(1):
        for q in range(ITERS):
            low = [jnp.where(y == 0, 0.0, arrived(0, q, b)) for b in range(blocks)]
            low += [column(sub_rows * g - ITERS + q, b) for g in range(1, groups) for b in range(blocks)]
            basis[0][q, PAD : PAD + 128, :] = (
                jnp.concatenate(low, axis=0).T * links[4, q, PAD : PAD + 128, :]
            )
            high = [column(sub_rows * g + q, b) for g in range(1, groups) for b in range(blocks)]
            high += [arrived(1, q, b) for b in range(blocks)]
            r = q + ITERS + sub_rows
            basis[0][r, PAD : PAD + 128, :] = (
                jnp.concatenate(high, axis=0).T * links[4, r + 1, PAD : PAD + 128, :]
            )

    for c in more:
        c.wait_recv()
    corner_arrivals(rows_corners, 12, later)
    for e in range(2):
        for q in range(ITERS):
            idx = member + members * (q % groups)
            south = along(corner_in[e, 1 + q // groups], idx, 1)
            south = jnp.where(y == 0, 0.0, south)
            v = pltpu.roll(field[sub_rows + q, beyond_tiles[e], :], members, 1)
            v = jnp.where(group == 0, south, v)
            basis[0][q, beyond_tiles[e], :] = v * links[4, q, beyond_tiles[e], :]
            north = along(corner_in[2 + e, 1 + q // groups], idx, 1)
            v = pltpu.roll(field[ITERS + q, beyond_tiles[e], :], 128 - members, 1)
            v, r = jnp.where(group == groups - 1, north, v), ITERS + sub_rows + q
            basis[0][r, beyond_tiles[e], :] = v * links[4, r + 1, beyond_tiles[e], :]
    coef_up.wait_send()
    rows_up.wait_send()

    @pl.when(y > 0)
    def _():
        coef_down.wait_send()
        rows_down.wait_send()

    for c in sides + more:
        c.wait_send()
    for remote, c, _, _ in coef_corners + rows_corners:
        pl.when(remote)(c.wait_send)
    iterate(members, rows, y == ny - 1, field, links, basis, gram)

    def sent(source, dst, n, there):
        c = copy(source, dst, n, n, there)
        c.start()
        return c

    across = [sent(gram, along_x.at[s], 15 + s, (y, lax.rem(x + s, nx))) for s in range(1, nx)]
    apply(ITERS - 1, links, basis, [(ITERS, SEAM)], 16, lambda t: t)
    scale_ref[0] = inv[PAD : PAD + 128, :].T
    scale_ref[1] = square[PAD : PAD + 128, :].T
    for c in across:
        c.wait()
    along_x[0] = sum((along_x[s] for s in range(1, nx)), gram[...])
    across = [
        sent(along_x.at[0], along_y.at[s], 14 + nx + s, (lax.rem(y + s, ny), x)) for s in range(1, ny)
    ]
    for c in across:
        c.wait()
    sum_ref[...] = sum((along_y[s] for s in range(1, ny)), along_x[0])


def coefficients(gram):
    def g(i, j):
        return gram[min(i, j)][max(i, j)]

    def applied(p):
        q = []
        for k in range(ITERS + 1):
            terms = []
            if k < len(p):
                terms.append((1.0 - ROOT) * p[k])
            if 0 < k <= len(p):
                terms.append(-ROOT * p[k - 1])
            if k + 1 < len(p):
                terms.append(-ROOT * p[k + 1])
            if terms:
                q.append(sum(terms[1:], terms[0]))
        return q

    def inner(p, q):
        total = None
        for i, a in enumerate(p):
            row = None
            for j, b in enumerate(q):
                t = g(i, j) * b
                row = t if row is None else row + t
            t = a * row
            total = t if total is None else total + t
        return total

    one = jnp.ones_like(gram[0][0])
    z, p, x = [one], [one], []
    rz = g(0, 0)
    for iteration in range(ITERS):
        q = applied(p)
        step = rz / inner(p, q)
        x = [(x[k] if k < len(x) else 0.0) + step * p[k] for k in range(len(p))]
        z = [(z[k] if k < len(z) else 0.0) - step * q[k] for k in range(len(q))]
        if iteration + 1 < ITERS:
            rz_new = inner(z, z)
            beta = rz_new / rz
            p = [z[k] + (beta * p[k] if k < len(p) else 0.0) for k in range(len(z))]
            rz = rz_new
    return x, z


def combine_kernel(members, rows, *refs):
    basis, (scale_ref, sum_ref, x_out, r_out, stage, sems) = refs[: ITERS + 1], refs[ITERS + 1 :]
    groups = 128 // members
    sub_rows = rows // groups
    tall = stage.shape[2]
    lanes = iota(1)
    sums = sum_ref[...]
    tiles = [along(sums, (lanes & (members - 1)) + members * j, 1) for j in range(4)]
    found = [
        jnp.broadcast_to(tiles[n // 8][n % 8 : n % 8 + 1, :], (8, 128))
        for n in range(2 * ITERS + len(SKEW))
    ]
    gram = [[None] * (ITERS + 1) for _ in range(ITERS + 1)]
    for i in range(ITERS):
        gram[i][i], gram[i][i + 1] = found[2 * i], found[2 * i + 1]
    last = ITERS - 1
    gram[last][ITERS] = gram[last][ITERS] - gram[last][last] - gram[last - 1][last]
    skew = dict(zip(SKEW, found[2 * ITERS :]))
    for gap in range(2, ITERS + 1):
        for i in range(ITERS + 1 - gap):
            j = i + gap - 1
            v = gram[i + 1][j] - gram[i][j - 1] + skew[i, j]
            gram[i][j + 1] = v + gram[i - 1][j] if i else v
    xs, zs = coefficients(gram)
    flat = stage.reshape(2 * members * tall, 128)
    blocks = members // 8
    half = sub_rows // 2
    outs = (x_out, r_out)

    def drain(h):
        copies = []
        for o in range(2):
            for g in range(groups):
                at = slice(sub_rows * g + half * h, sub_rows * g + half * (h + 1))
                copies.append(
                    pltpu.make_async_copy(stage.at[o, :, at, :], outs[o].at[:, at, :], sems.at[h, o, g])
                )
        return copies

    started = []
    for h in range(2):

        def row(r):
            found = ([], [])
            for t in range(16):
                at = slice(PAD + 8 * t, PAD + 8 * t + 8)
                vs = [basis[k][r + ITERS, at, :] for k in range(ITERS + 1)]
                found[0].append(sum((xs[k] * vs[k] for k in range(1, ITERS)), xs[0] * vs[0]))
                found[1].append(sum((zs[k] * vs[k] for k in range(1, ITERS + 1)), zs[0] * vs[0]))
            for o in range(2):
                turned = jnp.concatenate(found[o], axis=0).T
                for g in range(groups):
                    row = sub_rows * g + r
                    scale = jnp.broadcast_to(scale_ref[o, pl.ds(row + 8, 1), :], (8, 128))
                    for b in range(blocks):
                        n = 8 * (g * blocks + b)
                        at = pl.ds((o * members + 8 * b) * tall + row, 8, stride=tall)
                        flat[at, :] = turned[n : n + 8, :] * scale

        @pl.loop(0, half // 4)
        def _(part):
            for within in range(4):
                row(half * h + 4 * part + within)

        for c in drain(h):
            c.start()
            started.append(c)
    for c in started:
        c.wait()


def on_device(right_side, couplings, center, ocean_mask):
    members, rows, columns = right_side.shape
    groups = 128 // members
    sub_rows = rows // groups
    assert lax.axis_size("gx") > 2 and ITERS <= 2 * groups
    assert columns == 128 and members % 8 == 0 and groups * members == 128
    assert 3 * (rows + 16) <= 256 < 4 * (rows + 16) and 2 * (rows + 16) >= 128 and sub_rows == SEAM - ITERS
    ny, nx = lax.axis_size("gy"), lax.axis_size("gx")
    vmem = pl.BlockSpec(memory_space=pltpu.VMEM)
    hbm = pl.BlockSpec(memory_space=pltpu.HBM)
    deep, wide = sub_rows + 2 * ITERS, columns + 2 * PAD + 8

    inputs = [
        pltpu.with_memory_space_constraint(v, pltpu.HBM)
        for v in (right_side, couplings, center, ocean_mask)
    ]

    def first(*refs):
        solve_kernel(members, rows, ny, nx, *refs)

    *basis, scale, sums = pl.pallas_call(
        first,
        out_shape=(pltpu.VMEM((deep, wide, 128), F32),) * (ITERS + 1)
        + (pltpu.VMEM((2, 128, 128), F32), pltpu.VMEM((8, 128), F32)),
        in_specs=[hbm] * 4,
        out_specs=(vmem,) * (ITERS + 3),
        scratch_shapes=[
            pltpu.VMEM((deep, wide, 128), F32),
            pltpu.VMEM((5, deep + 3, wide, 128), F32),
            pltpu.VMEM((5, wide, 128), F32),
            pltpu.VMEM((members, rows + 8, columns), F32),
            pltpu.VMEM((3, rows, columns), F32),
            pltpu.VMEM((rows, columns), F32),
            pltpu.VMEM((rows, columns), jnp.int32),
            pltpu.VMEM((2, 5, 8, columns), F32),
            pltpu.VMEM((2, 5, 8, columns), F32),
            pltpu.VMEM((2, ITERS * members, columns), F32),
            pltpu.VMEM((2, ITERS * members, columns), F32),
            pltpu.VMEM((2, 5, 8, 128), F32),
            pltpu.VMEM((4, 3, 8, 128), F32),
            pltpu.VMEM((4, 3, 8, 128), F32),
            pltpu.VMEM((128, 128), F32),
            pltpu.VMEM((2, wide, 128), F32),
            pltpu.VMEM((wide, 128), F32),
            pltpu.VMEM((wide, 128), F32),
            pltpu.VMEM((5 * 144, 256), jnp.bfloat16),
            pltpu.VMEM(((deep + 2) // 2, 256, 256), jnp.bfloat16),
            pltpu.VMEM((8, 128), F32),
            pltpu.VMEM((nx, 8, 128), F32),
            pltpu.VMEM((ny, 8, 128), F32),
            pltpu.SemaphoreType.DMA((4,)),
            pltpu.SemaphoreType.DMA((14 + nx + ny,)),
            pltpu.SemaphoreType.DMA((14 + nx + ny,)),
        ],
        compiler_params=pltpu.CompilerParams(
            collective_id=0, has_side_effects=True, vmem_limit_bytes=GRANT
        ),
    )(*inputs)

    def second(*refs):
        combine_kernel(members, rows, *refs)

    return pl.pallas_call(
        second,
        out_shape=(jax.ShapeDtypeStruct(right_side.shape, F32),) * 2,
        in_specs=[vmem] * (ITERS + 3),
        out_specs=(hbm, hbm),
        compiler_params=pltpu.CompilerParams(vmem_limit_bytes=GRANT),
        scratch_shapes=[
            pltpu.VMEM((2, members, rows + 8, columns), F32),
            pltpu.SemaphoreType.DMA((2, 2, groups)),
        ],
    )(*basis, scale, sums)


def solution(mesh):
    in_specs = (P(None, "gy", "gx"), P(None, "gy", "gx"), P("gy", "gx"), P("gy", "gx"))
    out_specs = (P(None, "gy", "gx"), P(None, "gy", "gx"))
    return jax.shard_map(
        on_device, mesh=mesh, in_specs=in_specs, out_specs=out_specs, check_vma=False
    )
```

```python
import jax
import jax.numpy as jnp
from jax import lax
from jax.experimental import pallas as pl
from jax.experimental.pallas import tpu as pltpu
from jax.sharding import PartitionSpec as P

ITERS = 6
ROOT = 0.18
PAD = 16
VMEM = 67043328
GRANT = 24 * 1024 * 1024
SKEW = [(i, j) for i in range(ITERS) for j in range(i + 1, ITERS)]
SEAM = 16 + ITERS
F32 = jnp.float32


def iota(dim):
    return lax.broadcasted_iota(jnp.int32, (8, 128), dim)


def along(x, idx, axis):
    return jnp.take_along_axis(x, idx, axis=axis, mode="promise_in_bounds")


def prepare(members, rows, top, planes, shifted, inv, links, square, lhs, pick):
    first, chunk, tiles = PAD - 8, 48, 18
    lanes = lax.broadcasted_iota(jnp.int32, (chunk, 128), 1)
    seam = lanes == rows + 8
    folded = jnp.logical_and(top, lanes >= rows + 8)
    span = rows + 16
    factor = 1.0 / ROOT

    def before(v):
        return pltpu.roll(v, 1, 1)

    def after(v):
        return pltpu.roll(v, 127, 1)

    for t in range(0, 8 * tiles, chunk):
        at, nxt = slice(first + t, first + t + chunk), slice(first + t + 1, first + t + 1 + chunk)
        for n, p in enumerate((1, 2)):
            shifted[n, at, :] = jnp.where(folded, planes[p, nxt, :], planes[p, at, :])

    for t in range(0, 8 * tiles, chunk):
        at = slice(first + t, first + t + chunk)
        prv = slice(first + t - 1, first + t - 1 + chunk)
        cn, ce, cne = planes[0, at, :], shifted[0, at, :], shifted[1, at, :]
        cew, cnw = shifted[0, prv, :], shifted[1, prv, :]
        diag = planes[3, at, :] + cn + ce + cew + cne + cnw + before(cn + cne + cnw)
        ocean = planes[4, at, :] > 0.0
        root = jnp.sqrt(diag)
        recip = jnp.where(ocean, 1.0 / root, 0.0)
        root = jnp.where(ocean, root, 0.0)
        inv[at, :] = jnp.where(seam, after(recip), recip)
        square[at, :] = root

    for t in range(0, 8 * tiles, chunk):
        at = slice(first + t, first + t + chunk)
        nxt = slice(first + t + 1, first + t + 1 + chunk)
        here, east = inv[at, :], inv[nxt, :]
        up, up_east = after(here), after(east)
        here_up = jnp.where(seam, before(here), here)
        east_up = jnp.where(seam, before(east), east)
        cn, ce, cne = planes[0, at, :] * factor, shifted[0, at, :] * factor, shifted[1, at, :] * factor
        values = (cn * here_up * up, ce * here * east, cne * here_up * up_east, cne * east_up * up, here)
        for n, v in enumerate(values):
            top_part = v.astype(jnp.bfloat16).astype(F32)
            v = v - top_part
            mid_part = v.astype(jnp.bfloat16).astype(F32)
            moved = pltpu.roll(mid_part, span, 1)
            low_part = pltpu.roll(v - mid_part, 2 * span - 128, 1)
            left = jnp.where(lanes < span, top_part, moved)
            right = jnp.where(lanes < 2 * span - 128, moved, low_part)
            right = jnp.where(lanes < 3 * span - 128, right, 0.0)
            to = slice(8 * tiles * n + t, 8 * tiles * n + t + chunk)
            lhs[to, 0:128] = left.astype(jnp.bfloat16)
            lhs[to, 128:256] = right.astype(jnp.bfloat16)

    def spread(p, planes_from, halves):
        found = jnp.dot(lhs[8 * tiles * planes_from :, :], pick[p], preferred_element_type=F32)
        for n in range(planes_from, 5):
            for h in range(halves):
                at = 8 * tiles * (n - planes_from)
                links[n, 2 * p + h, first : first + 8 * tiles, :] = found[
                    at : at + 8 * tiles, 128 * h : 128 * h + 128
                ]

    pairs = pick.shape[0] - 1
    together = 2 - pairs % 2

    @pl.loop(0, pairs // together)
    def _(part):
        for within in range(together):
            spread(together * part + within, 0, 2)

    spread(pairs, 4, 1)


def choose(members, rows, pick):
    groups = 128 // members
    sub_rows = rows // groups
    span = rows + 16
    source = lax.broadcasted_iota(jnp.int32, (256, 256), 0)
    lane = lax.broadcasted_iota(jnp.int32, (256, 256), 1)
    source = source - span * ((source >= span).astype(jnp.int32) + (source >= 2 * span).astype(jnp.int32))
    group = lax.shift_right_logical(lane & 127, members.bit_length() - 1)
    half = lax.shift_right_logical(lane, 7)
    last = (group == groups - 1).astype(jnp.int32)
    base = source - sub_rows * group - half - 8 + ITERS

    @pl.loop(0, pick.shape[0])
    def _(p):
        later = (2 * p + half >= sub_rows + ITERS).astype(jnp.int32)
        hit = base == 2 * p + later * (last - 1)
        pick[p] = jnp.where(hit, 1.0, 0.0).astype(jnp.bfloat16)


def apply(k, links, basis, parts, low, count):
    depth = ITERS - 1 - k
    here, out = basis[k], basis[k + 1]
    old = basis[k - 1] if k else None

    def column(t):
        x0 = PAD - depth + 8 * t
        mid, east, west = pl.ds(x0, 8), pl.ds(x0 + 1, 8), pl.ds(x0 - 1, 8)

        def three(r):
            return here[r, west, :], here[r, mid, :], here[r, east, :]

        for start, stop in parts:
            dn, cur = three(start - 1), three(start)
            north = links[0, start - 1 + (1 if start > SEAM else 0), mid, :]
            for r in range(start, stop):
                nxt = three(r + 1)
                c = r + (1 if r >= SEAM else 0)
                if r == SEAM:
                    north = links[0, c - 1, mid, :]
                south, north = north, links[0, c, mid, :]
                total = (north * nxt[1] + south * dn[1]) + (
                    links[1, c, mid, :] * cur[2] + links[1, c, west, :] * cur[0]
                )
                total = total + (links[2, c, mid, :] * nxt[2] + links[2, c - 1, west, :] * dn[0])
                total = total + (links[3, c, west, :] * nxt[0] + links[3, c - 1, mid, :] * dn[2])
                total = total - (cur[1] if old is None else cur[1] + old[r, mid, :])
                out[r, mid, :] = total
                dn, cur = cur, nxt

    if count > 3:

        @pl.loop(0, count // 2)
        def _(t):
            column(low + 2 * t)
            column(low + 2 * t + 1)

    for t in range(count - count % 2 if count > 3 else 0, count):
        column(low + t)


def begin(raw, links, basis):
    @pl.loop(ITERS, SEAM)
    def _(r):
        for t in range(16):
            at = slice(PAD + 8 * t, PAD + 8 * t + 8)
            basis[0][r, at, :] = raw[r, at, :] * links[4, r, at, :]

    apply(0, links, basis, [(ITERS + 1, SEAM - 1)], 1, 15)
    apply(1, links, basis, [(ITERS + 2, SEAM - 2)], 1, 14)


def iterate(members, rows, top, raw, links, basis, gram_ref):
    subs = iota(0)
    group = lax.shift_right_logical(iota(1), members.bit_length() - 1)
    for r in range(ITERS, SEAM):
        for t in (0, 17):
            at = slice(PAD - 8 + 8 * t, PAD + 8 * t)
            basis[0][r, at, :] = raw[r, at, :] * links[4, r, at, :]

    apply(0, links, basis, [(1, ITERS + 1), (SEAM - 1, SEAM + ITERS - 1)], 0, 18)
    apply(0, links, basis, [(ITERS + 1, SEAM - 1)], 0, 1)
    apply(0, links, basis, [(ITERS + 1, SEAM - 1)], 16, 2)
    apply(1, links, basis, [(2, ITERS + 2), (SEAM - 2, SEAM + ITERS - 2)], 0, 17)
    apply(1, links, basis, [(ITERS + 2, SEAM - 2)], 0, 1)
    apply(1, links, basis, [(ITERS + 2, SEAM - 2)], 15, 2)
    for k in range(2, ITERS - 1):
        depth = ITERS - 1 - k
        count = (128 + 2 * depth + 7) // 8
        apply(k, links, basis, [(ITERS - depth, SEAM + depth)], 0, count)

    zero = jnp.zeros((8, 128), F32)
    fold = jnp.logical_and(group == 128 // members - 1, top)
    newest = basis[ITERS - 1]

    def body(r, sums):
        sums = list(sums)
        r = r + ITERS
        share = jnp.where(jnp.logical_and(fold, r == SEAM - 1), 0.5, 1.0)
        for t in range(16):
            at = slice(PAD + 8 * t, PAD + 8 * t + 8)
            east, west = (slice(PAD + 8 * t + d, PAD + 8 * t + d + 8) for d in (1, -1))
            vs = [basis[k][r, at, :] for k in range(ITERS)]
            for i in range(ITERS):
                sums[2 * i] = sums[2 * i] + vs[i] * vs[i]
                if i + 1 < ITERS:
                    sums[2 * i + 1] = sums[2 * i + 1] + vs[i] * vs[i + 1]
            ahead = links[0, r, at, :] * newest[r + 1, at, :]
            ahead = ahead + links[2, r, at, :] * newest[r + 1, east, :]
            ahead = ahead + links[3, r, west, :] * newest[r + 1, west, :]
            ahead = ahead * share + links[1, r, at, :] * newest[r, east, :]
            sums[-1] = sums[-1] + vs[-1] * ahead
        return tuple(sums)

    sums = lax.fori_loop(0, SEAM - ITERS, body, (zero,) * (2 * ITERS))
    sums = sums[:-1] + (sums[-1] + sums[-1],)

    def across(t, sums):
        sums = list(sums)
        for u in range(4):
            x0 = PAD + 32 * t + 8 * u
            mid, east, west = pl.ds(x0, 8), pl.ds(x0 + 1, 8), pl.ds(x0 - 1, 8)
            north, right, left = links[0, SEAM - 1, mid, :], links[2, SEAM - 1, mid, :], links[3, SEAM - 1, west, :]
            here, over = [], []
            for k in range(ITERS):
                w = basis[k]
                v = north * w[SEAM, mid, :] + right * w[SEAM, east, :] + left * w[SEAM, west, :]
                over.append(jnp.where(fold, v, 0.0))
                here.append(w[SEAM - 1, mid, :])
            for n, (i, j) in enumerate(SKEW):
                sums[n] = sums[n] + (here[i] * over[j] - here[j] * over[i])
        return tuple(sums)

    sums = sums + lax.fori_loop(0, 4, across, (zero,) * len(SKEW))
    pack = [zero] * 4
    for n, s in enumerate(sums):
        for step in (1, 2, 4):
            s = s + pltpu.roll(s, step, 0)
        pack[n // 8] = jnp.where(subs == n % 8, s, pack[n // 8])
    total = zero
    for j, v in enumerate(pack):
        width = members
        while width < 128:
            v = v + pltpu.roll(v, width, 1)
            width *= 2
        total = jnp.where(group == j, v, total)
    gram_ref[...] = total


def solve_kernel(members, rows, ny, nx, rhs_hbm, coup_hbm, center_hbm, mask_hbm, *refs):
    basis, (scale_ref, sum_ref) = refs[: ITERS + 1], refs[ITERS + 1 : ITERS + 3]
    (
        field, links, planes, rhs, coup, center, mask, coef_out, coef_in, rows_out, rows_in, strip_out, corner_out, corner_in, ext,
        shifted, inv, square, lhs, pick, gram, along_x, along_y, load, send, recv,
    ) = refs[ITERS + 3 :]
    groups = 128 // members
    sub_rows = rows // groups
    tall = rhs.shape[1]
    y, x = lax.axis_index("gy"), lax.axis_index("gx")
    top = (y + 1) // ny
    mirror = nx - 1 - x
    east, west = lax.rem(x + 1, nx), lax.rem(x + nx - 1, nx)
    up = (y + 1 - top, x + top * (mirror - x))
    down = (jnp.maximum(y - 1, 0), x)
    loads = [
        pltpu.make_async_copy(coup_hbm, coup, load.at[0]),
        pltpu.make_async_copy(center_hbm, center, load.at[1]),
        pltpu.make_async_copy(mask_hbm, mask, load.at[2]),
        pltpu.make_async_copy(rhs_hbm, rhs.at[:, 0:rows, :], load.at[3]),
    ]
    for c in loads:
        c.start()
    barrier = pltpu.get_barrier_semaphore()

    def greet(there):
        pl.semaphore_signal(barrier, inc=1, device_id=there, device_id_type=pl.DeviceIdType.MESH)

    for step in range(1, nx):
        greet((y, lax.rem(x + step, nx)))
    for step in range(1, ny):
        greet((lax.rem(y + step, ny), x))

    @pl.when(y > 0)
    def _():
        greet((y - 1, east))
        greet((y - 1, west))

    @pl.when(top == 0)
    def _():
        greet((y + 1, east))
        greet((y + 1, west))

    def copy(src, dst, n, m, there):
        return pltpu.make_async_remote_copy(
            src_ref=src,
            dst_ref=dst,
            send_sem=send.at[n],
            recv_sem=recv.at[m],
            device_id=there,
            device_id_type=pl.DeviceIdType.MESH,
        )

    def corner(base, parts):
        found = []
        for e in range(2):
            plain, folded = x + 2 * e - 1, mirror + 1 - 2 * e
            to = lax.rem(plain + top * (folded - plain) + nx, nx)
            k = 1 - e + top * (1 + 2 * e)
            c = copy(
                corner_out.at[e, parts], corner_in.at[k, parts], base + e, base + k, (y + 1 - top, to)
            )
            found.append((jnp.logical_or(top == 0, to != x), c, e, k))
        for e in range(2):
            k = 3 - e
            there = (jnp.maximum(y - 1, 0), east if e else west)
            c = copy(
                corner_out.at[2 + e, parts], corner_in.at[k, parts], base + 2 + e, base + k, there
            )
            found.append((y > 0, c, 2 + e, k))
        return found

    def start_corners(found, parts):
        for n, (remote, c, e, k) in enumerate(found):
            pl.when(remote)(c.start)
            if n < 2:

                @pl.when(jnp.logical_not(remote))
                def _():
                    corner_in[k, parts] = corner_out[e, parts]

    def corner_arrivals(found, base, parts):
        for k in range(4):
            c = copy(corner_out.at[0, parts], corner_in.at[k, parts], base, base + k, (y, east))
            pl.when(y > 0 if k < 2 else found[k - 2][0])(c.wait_recv)

    lanes, subs = iota(1), iota(0)
    flip_lane = jnp.where(top == 1, 127 - lanes, lanes)
    flip_sub = jnp.where(top == 1, 7 - subs, subs)
    tiles = (slice(PAD, PAD + 8), slice(PAD + 120, PAD + 128))
    beyond_tiles = (slice(PAD - 8, PAD), slice(PAD + 128, PAD + 136))
    for c in loads[:3]:
        c.wait()

    def own(p, at):
        if p < 3:
            return coup[p, at, :]
        return center[at, :] if p == 3 else mask[at, :].astype(F32)

    packs = [jnp.zeros((8, 128), F32)] * 4
    plane = lax.shift_right_logical(lanes, 3)
    high_lanes = jnp.where(top == 1, rows + 7 - (lanes & 7), rows + (lanes & 7))
    low_lanes = 8 + (lanes & 7)
    ext[0:8, :] = jnp.zeros((8, 128), F32)
    ext[rows + 8 : 128, :] = jnp.zeros((120 - rows, 128), F32)
    for p in range(5):
        coef_out[0, p] = along(along(own(p, slice(rows - 8, rows)), flip_lane, 1), flip_sub, 0)
        coef_out[1, p] = own(p, slice(0, 8))
        ext[8 : rows + 8, :] = own(p, slice(0, rows))
        turned = ext[...].T
        for e, edge in enumerate((turned[0:8], turned[120:128])):
            strip_out[e, p] = edge
            packs[e] = jnp.where(plane == p, along(edge, high_lanes, 1), packs[e])
            packs[2 + e] = jnp.where(plane == p, along(edge, low_lanes, 1), packs[2 + e])
    for e in range(4):
        corner_out[e, 0] = along(packs[e], flip_sub, 0) if e < 2 else packs[e]
    pl.semaphore_wait(barrier, nx + ny - 2 + 2 * (1 - top) + 2 * jnp.minimum(y, 1))
    coef_up = copy(coef_out.at[0], coef_in.at[top], 0, top, up)
    coef_down = copy(coef_out.at[1], coef_in.at[1], 1, 1, down)
    rows_up = copy(rows_out.at[0], rows_in.at[top], 2, 2 + top, up)
    rows_down = copy(rows_out.at[1], rows_in.at[1], 3, 3, down)
    first = slice(0, 1)
    later = slice(1, 3)
    coef_corners, rows_corners = corner(8, first), corner(12, later)
    sides = [
        copy(strip_out.at[0], planes.at[:, PAD + 128 : PAD + 136, :], 4, 4, (y, west)),
        copy(strip_out.at[1], planes.at[:, PAD - 8 : PAD, :], 5, 5, (y, east)),
    ]
    start_corners(coef_corners, first)
    coef_up.start()
    pl.when(y > 0)(coef_down.start)
    for c in sides:
        c.start()
    flat = rhs.reshape(members * tall, 128)

    def column(row, block):
        return flat[pl.ds(8 * block * tall + row, 8, stride=tall), :]

    blocks = members // 8
    loads[3].wait()
    for q in range(ITERS):
        high = rows - ITERS + q + top * (ITERS - 1 - 2 * q)
        for b in range(blocks):
            at = slice(q * members + 8 * b, q * members + 8 * b + 8)
            rows_out[0, at, :] = along(column(high, b), flip_lane, 1)
            rows_out[1, at, :] = column(q, b)

    @pl.loop(0, sub_rows // 4)
    def _(part):
        for within in range(4):
            r = 4 * part + within
            stack = [column(sub_rows * g + r, b) for g in range(groups) for b in range(blocks)]
            field[r + ITERS, PAD : PAD + 128, :] = jnp.concatenate(stack, axis=0).T

    member = lanes & (members - 1)
    group = lax.shift_right_logical(lanes, members.bit_length() - 1)
    for e in range(2):
        packs = [[jnp.zeros((8, 128), F32)] * 2 for _ in range(2)]
        for q in range(ITERS):
            here = group == q % groups
            v = field[sub_rows + q + top * (ITERS - 1 - 2 * q), tiles[e], :]
            v = along(v, member + (128 - members), 1)
            packs[0][q // groups] = jnp.where(here, v, packs[0][q // groups])
            v = along(field[ITERS + q, tiles[e], :], member, 1)
            packs[1][q // groups] = jnp.where(here, v, packs[1][q // groups])
        for n in range(2):
            corner_out[e, 1 + n] = along(packs[0][n], flip_sub, 0)
            corner_out[2 + e, 1 + n] = packs[1][n]
    inner = slice(ITERS, ITERS + sub_rows)
    more = [
        copy(field.at[inner, tiles[0], :], field.at[inner, beyond_tiles[1], :], 6, 6, (y, west)),
        copy(field.at[inner, tiles[1], :], field.at[inner, beyond_tiles[0], :], 7, 7, (y, east)),
    ]
    start_corners(rows_corners, later)
    for c in more:
        c.start()
    choose(members, rows, pick)
    coef_north = copy(coef_out.at[1], coef_in.at[1], 1, 1, down)
    coef_south = copy(coef_out.at[0], coef_in.at[0], 0, 0, up)
    coef_north.wait_recv()
    pl.when(y > 0)(coef_south.wait_recv)
    rows_up.start()
    pl.when(y > 0)(rows_down.start)
    for p in range(5):
        beyond = coef_in[1, p]
        moved = pltpu.roll(beyond, 1, 0)
        if p in (0, 2):
            last = jnp.broadcast_to(own(p, slice(rows - 1, rows)), (8, 128))
            beyond = jnp.where(top == 1, beyond, jnp.where(subs == 0, last, moved))
        else:
            beyond = jnp.where(subs == 0, beyond, moved)
        ext[0:8, :] = jnp.where(y == 0, 0.0, coef_in[0, p])
        ext[8 : rows + 8, :] = own(p, slice(0, rows))
        ext[rows + 8 : rows + 16, :] = beyond
        planes[p, PAD : PAD + 128, :] = ext[...].T
    for c in sides:
        c.wait_recv()
    corner_arrivals(coef_corners, 8, first)
    for e in range(2):
        low, high = corner_in[e, 0], corner_in[2 + e, 0]
        for p in range(5):
            strip = planes[p, beyond_tiles[e], :]
            shift = 1 - top if p in (0, 2) else 1
            idx = jnp.clip(lanes - (rows + 8) - shift, 0, 7) + 8 * p
            north = along(high, idx, 1)
            if p in (0, 2):
                joint = jnp.logical_and(lanes == rows + 8, top == 0)
                north = jnp.where(joint, pltpu.roll(strip, 1, 1), north)
            south = jnp.where(y == 0, 0.0, along(low, (lanes & 7) + 8 * p, 1))
            outside = jnp.logical_and(lanes >= rows + 8, lanes < rows + 16)
            strip = jnp.where(lanes < 8, south, jnp.where(outside, north, strip))
            planes[p, beyond_tiles[e], :] = strip
    prepare(members, rows, y == ny - 1, planes, shifted, inv, links, square, lhs, pick)
    begin(field, links, basis)
    copy(rows_out.at[1], rows_in.at[1], 3, 3, down).wait_recv()
    pl.when(y > 0)(copy(rows_out.at[0], rows_in.at[0], 2, 2, up).wait_recv)

    def arrived(side, q, b):
        return rows_in[side, q * members + 8 * b : q * members + 8 * b + 8, :]

    for _ in range(1):
        for q in range(ITERS):
            low = [jnp.where(y == 0, 0.0, arrived(0, q, b)) for b in range(blocks)]
            low += [column(sub_rows * g - ITERS + q, b) for g in range(1, groups) for b in range(blocks)]
            basis[0][q, PAD : PAD + 128, :] = (
                jnp.concatenate(low, axis=0).T * links[4, q, PAD : PAD + 128, :]
            )
            high = [column(sub_rows * g + q, b) for g in range(1, groups) for b in range(blocks)]
            high += [arrived(1, q, b) for b in range(blocks)]
            r = q + ITERS + sub_rows
            basis[0][r, PAD : PAD + 128, :] = (
                jnp.concatenate(high, axis=0).T * links[4, r + 1, PAD : PAD + 128, :]
            )

    for c in more:
        c.wait_recv()
    corner_arrivals(rows_corners, 12, later)
    for e in range(2):
        for q in range(ITERS):
            idx = member + members * (q % groups)
            south = along(corner_in[e, 1 + q // groups], idx, 1)
            south = jnp.where(y == 0, 0.0, south)
            v = pltpu.roll(field[sub_rows + q, beyond_tiles[e], :], members, 1)
            v = jnp.where(group == 0, south, v)
            basis[0][q, beyond_tiles[e], :] = v * links[4, q, beyond_tiles[e], :]
            north = along(corner_in[2 + e, 1 + q // groups], idx, 1)
            v = pltpu.roll(field[ITERS + q, beyond_tiles[e], :], 128 - members, 1)
            v, r = jnp.where(group == groups - 1, north, v), ITERS + sub_rows + q
            basis[0][r, beyond_tiles[e], :] = v * links[4, r + 1, beyond_tiles[e], :]
    coef_up.wait_send()
    rows_up.wait_send()

    @pl.when(y > 0)
    def _():
        coef_down.wait_send()
        rows_down.wait_send()

    for c in sides + more:
        c.wait_send()
    for remote, c, _, _ in coef_corners + rows_corners:
        pl.when(remote)(c.wait_send)
    iterate(members, rows, y == ny - 1, field, links, basis, gram)

    def sent(source, dst, n, there):
        c = copy(source, dst, n, n, there)
        c.start()
        return c

    across = [sent(gram, along_x.at[s], 15 + s, (y, lax.rem(x + s, nx))) for s in range(1, nx)]
    apply(ITERS - 1, links, basis, [(ITERS, SEAM)], 0, 16)
    scale_ref[0] = inv[PAD : PAD + 128, :].T
    scale_ref[1] = square[PAD : PAD + 128, :].T
    for c in across:
        c.wait()
    along_x[0] = sum((along_x[s] for s in range(1, nx)), gram[...])
    across = [
        sent(along_x.at[0], along_y.at[s], 14 + nx + s, (lax.rem(y + s, ny), x)) for s in range(1, ny)
    ]
    for c in across:
        c.wait()
    sum_ref[...] = sum((along_y[s] for s in range(1, ny)), along_x[0])


def coefficients(gram):
    def g(i, j):
        return gram[min(i, j)][max(i, j)]

    def applied(p):
        q = []
        for k in range(ITERS + 1):
            terms = []
            if k < len(p):
                terms.append((1.0 - ROOT) * p[k])
            if 0 < k <= len(p):
                terms.append(-ROOT * p[k - 1])
            if k + 1 < len(p):
                terms.append(-ROOT * p[k + 1])
            if terms:
                q.append(sum(terms[1:], terms[0]))
        return q

    def inner(p, q):
        total = None
        for i, a in enumerate(p):
            row = None
            for j, b in enumerate(q):
                t = g(i, j) * b
                row = t if row is None else row + t
            t = a * row
            total = t if total is None else total + t
        return total

    one = jnp.ones_like(gram[0][0])
    z, p, x = [one], [one], []
    rz = g(0, 0)
    for iteration in range(ITERS):
        q = applied(p)
        step = rz / inner(p, q)
        x = [(x[k] if k < len(x) else 0.0) + step * p[k] for k in range(len(p))]
        z = [(z[k] if k < len(z) else 0.0) - step * q[k] for k in range(len(q))]
        if iteration + 1 < ITERS:
            rz_new = inner(z, z)
            beta = rz_new / rz
            p = [z[k] + (beta * p[k] if k < len(p) else 0.0) for k in range(len(z))]
            rz = rz_new
    return x, z


def combine_kernel(members, rows, *refs):
    basis, (scale_ref, sum_ref, x_out, r_out, stage, sems) = refs[: ITERS + 1], refs[ITERS + 1 :]
    groups = 128 // members
    sub_rows = rows // groups
    tall = stage.shape[2]
    lanes = iota(1)
    sums = sum_ref[...]
    tiles = [along(sums, (lanes & (members - 1)) + members * j, 1) for j in range(4)]
    found = [
        jnp.broadcast_to(tiles[n // 8][n % 8 : n % 8 + 1, :], (8, 128))
        for n in range(2 * ITERS + len(SKEW))
    ]
    gram = [[None] * (ITERS + 1) for _ in range(ITERS + 1)]
    for i in range(ITERS):
        gram[i][i], gram[i][i + 1] = found[2 * i], found[2 * i + 1]
    last = ITERS - 1
    gram[last][ITERS] = gram[last][ITERS] - gram[last][last] - gram[last - 1][last]
    skew = dict(zip(SKEW, found[2 * ITERS :]))
    for gap in range(2, ITERS + 1):
        for i in range(ITERS + 1 - gap):
            j = i + gap - 1
            v = gram[i + 1][j] - gram[i][j - 1] + skew[i, j]
            gram[i][j + 1] = v + gram[i - 1][j] if i else v
    xs, zs = coefficients(gram)
    flat = stage.reshape(2 * members * tall, 128)
    blocks = members // 8
    half = sub_rows // 2
    outs = (x_out, r_out)

    def drain(h, o):
        copies = []
        for g in range(groups):
            at = slice(sub_rows * g + half * h, sub_rows * g + half * (h + 1))
            copies.append(
                pltpu.make_async_copy(stage.at[o, :, at, :], outs[o].at[:, at, :], sems.at[h, o, g])
            )
        return copies

    started = []
    for h in range(2):
        for o, weights in enumerate((xs, zs)):

            def row(r):
                found = []
                for t in range(16):
                    at = slice(PAD + 8 * t, PAD + 8 * t + 8)
                    terms = [w * basis[k][r + ITERS, at, :] for k, w in enumerate(weights)]
                    found.append(sum(terms[1:], terms[0]))
                turned = jnp.concatenate(found, axis=0).T
                for g in range(groups):
                    row = sub_rows * g + r
                    scale = jnp.broadcast_to(scale_ref[o, pl.ds(row + 8, 1), :], (8, 128))
                    for b in range(blocks):
                        n = 8 * (g * blocks + b)
                        at = pl.ds((o * members + 8 * b) * tall + row, 8, stride=tall)
                        flat[at, :] = turned[n : n + 8, :] * scale

            for within in range(half):
                row(half * h + within)

            for c in drain(h, o):
                c.start()
                started.append(c)
    for c in started:
        c.wait()


def on_device(right_side, couplings, center, ocean_mask):
    members, rows, columns = right_side.shape
    groups = 128 // members
    sub_rows = rows // groups
    assert lax.axis_size("gx") > 2 and ITERS <= 2 * groups
    assert columns == 128 and members % 8 == 0 and groups * members == 128
    assert 3 * (rows + 16) <= 256 < 4 * (rows + 16) and 2 * (rows + 16) >= 128 and sub_rows == SEAM - ITERS
    ny, nx = lax.axis_size("gy"), lax.axis_size("gx")
    vmem = pl.BlockSpec(memory_space=pltpu.VMEM)
    hbm = pl.BlockSpec(memory_space=pltpu.HBM)
    deep, wide = sub_rows + 2 * ITERS, columns + 2 * PAD + 8

    inputs = [
        pltpu.with_memory_space_constraint(v, pltpu.HBM)
        for v in (right_side, couplings, center, ocean_mask)
    ]

    def first(*refs):
        solve_kernel(members, rows, ny, nx, *refs)

    *basis, scale, sums = pl.pallas_call(
        first,
        out_shape=(pltpu.VMEM((deep, wide, 128), F32),) * (ITERS + 1)
        + (pltpu.VMEM((2, 128, 128), F32), pltpu.VMEM((8, 128), F32)),
        in_specs=[hbm] * 4,
        out_specs=(vmem,) * (ITERS + 3),
        scratch_shapes=[
            pltpu.VMEM((deep, wide, 128), F32),
            pltpu.VMEM((5, deep + 3, wide, 128), F32),
            pltpu.VMEM((5, wide, 128), F32),
            pltpu.VMEM((members, rows + 8, columns), F32),
            pltpu.VMEM((3, rows, columns), F32),
            pltpu.VMEM((rows, columns), F32),
            pltpu.VMEM((rows, columns), jnp.int32),
            pltpu.VMEM((2, 5, 8, columns), F32),
            pltpu.VMEM((2, 5, 8, columns), F32),
            pltpu.VMEM((2, ITERS * members, columns), F32),
            pltpu.VMEM((2, ITERS * members, columns), F32),
            pltpu.VMEM((2, 5, 8, 128), F32),
            pltpu.VMEM((4, 3, 8, 128), F32),
            pltpu.VMEM((4, 3, 8, 128), F32),
            pltpu.VMEM((128, 128), F32),
            pltpu.VMEM((2, wide, 128), F32),
            pltpu.VMEM((wide, 128), F32),
            pltpu.VMEM((wide, 128), F32),
            pltpu.VMEM((5 * 144, 256), jnp.bfloat16),
            pltpu.VMEM(((deep + 2) // 2, 256, 256), jnp.bfloat16),
            pltpu.VMEM((8, 128), F32),
            pltpu.VMEM((nx, 8, 128), F32),
            pltpu.VMEM((ny, 8, 128), F32),
            pltpu.SemaphoreType.DMA((4,)),
            pltpu.SemaphoreType.DMA((14 + nx + ny,)),
            pltpu.SemaphoreType.DMA((14 + nx + ny,)),
        ],
        compiler_params=pltpu.CompilerParams(
            collective_id=0, has_side_effects=True, vmem_limit_bytes=GRANT
        ),
    )(*inputs)

    def second(*refs):
        combine_kernel(members, rows, *refs)

    return pl.pallas_call(
        second,
        out_shape=(jax.ShapeDtypeStruct(right_side.shape, F32),) * 2,
        in_specs=[vmem] * (ITERS + 3),
        out_specs=(hbm, hbm),
        compiler_params=pltpu.CompilerParams(vmem_limit_bytes=GRANT),
        scratch_shapes=[
            pltpu.VMEM((2, members, rows + 8, columns), F32),
            pltpu.SemaphoreType.DMA((2, 2, groups)),
        ],
    )(*basis, scale, sums)


def solution(mesh):
    in_specs = (P(None, "gy", "gx"), P(None, "gy", "gx"), P("gy", "gx"), P("gy", "gx"))
    out_specs = (P(None, "gy", "gx"), P(None, "gy", "gx"))
    return jax.shard_map(
        on_device, mesh=mesh, in_specs=in_specs, out_specs=out_specs, check_vma=False
    )
```

```python
import jax
import jax.numpy as jnp
from jax import lax
from jax.experimental import pallas as pl
from jax.experimental.pallas import tpu as pltpu
from jax.sharding import PartitionSpec as P

ITERS = 6
ROOT = 0.18
PAD = 16
VMEM = 67043328
GRANT = 24 * 1024 * 1024
SKEW = [(i, j) for i in range(ITERS) for j in range(i + 1, ITERS)]
SEAM = 16 + ITERS
F32 = jnp.float32


def iota(dim):
    return lax.broadcasted_iota(jnp.int32, (8, 128), dim)


def along(x, idx, axis):
    return jnp.take_along_axis(x, idx, axis=axis, mode="promise_in_bounds")


def prepare(members, rows, top, planes, shifted, inv, links, square, lhs, pick):
    first, chunk, tiles = PAD - 8, 48, 18
    lanes = lax.broadcasted_iota(jnp.int32, (chunk, 128), 1)
    seam = lanes == rows + 8
    folded = jnp.logical_and(top, lanes >= rows + 8)
    span = rows + 16
    factor = 1.0 / ROOT

    def before(v):
        return pltpu.roll(v, 1, 1)

    def after(v):
        return pltpu.roll(v, 127, 1)

    for t in range(0, 8 * tiles, chunk):
        at, nxt = slice(first + t, first + t + chunk), slice(first + t + 1, first + t + 1 + chunk)
        for n, p in enumerate((1, 2)):
            shifted[n, at, :] = jnp.where(folded, planes[p, nxt, :], planes[p, at, :])

    for t in range(0, 8 * tiles, chunk):
        at = slice(first + t, first + t + chunk)
        prv = slice(first + t - 1, first + t - 1 + chunk)
        cn, ce, cne = planes[0, at, :], shifted[0, at, :], shifted[1, at, :]
        cew, cnw = shifted[0, prv, :], shifted[1, prv, :]
        diag = planes[3, at, :] + cn + ce + cew + cne + cnw + before(cn + cne + cnw)
        ocean = planes[4, at, :] > 0.0
        root = jnp.sqrt(diag)
        recip = jnp.where(ocean, 1.0 / root, 0.0)
        root = jnp.where(ocean, root, 0.0)
        inv[at, :] = jnp.where(seam, after(recip), recip)
        square[at, :] = root

    for t in range(0, 8 * tiles, chunk):
        at = slice(first + t, first + t + chunk)
        nxt = slice(first + t + 1, first + t + 1 + chunk)
        here, east = inv[at, :], inv[nxt, :]
        up, up_east = after(here), after(east)
        here_up = jnp.where(seam, before(here), here)
        east_up = jnp.where(seam, before(east), east)
        cn, ce, cne = planes[0, at, :] * factor, shifted[0, at, :] * factor, shifted[1, at, :] * factor
        values = (cn * here_up * up, ce * here * east, cne * here_up * up_east, cne * east_up * up, here)
        for n, v in enumerate(values):
            top_part = v.astype(jnp.bfloat16).astype(F32)
            v = v - top_part
            mid_part = v.astype(jnp.bfloat16).astype(F32)
            moved = pltpu.roll(mid_part, span, 1)
            low_part = pltpu.roll(v - mid_part, 2 * span - 128, 1)
            left = jnp.where(lanes < span, top_part, moved)
            right = jnp.where(lanes < 2 * span - 128, moved, low_part)
            right = jnp.where(lanes < 3 * span - 128, right, 0.0)
            to = slice(8 * tiles * n + t, 8 * tiles * n + t + chunk)
            lhs[to, 0:128] = left.astype(jnp.bfloat16)
            lhs[to, 128:256] = right.astype(jnp.bfloat16)

    def spread(p, planes_from, halves):
        found = jnp.dot(lhs[8 * tiles * planes_from :, :], pick[p], preferred_element_type=F32)
        for n in range(planes_from, 5):
            for h in range(halves):
                at = 8 * tiles * (n - planes_from)
                links[n, 2 * p + h, first : first + 8 * tiles, :] = found[
                    at : at + 8 * tiles, 128 * h : 128 * h + 128
                ]

    pairs = pick.shape[0] - 1
    together = 2 - pairs % 2

    @pl.loop(0, pairs // together)
    def _(part):
        for within in range(together):
            spread(together * part + within, 0, 2)

    spread(pairs, 4, 1)


def choose(members, rows, pick):
    groups = 128 // members
    sub_rows = rows // groups
    span = rows + 16
    source = lax.broadcasted_iota(jnp.int32, (256, 256), 0)
    lane = lax.broadcasted_iota(jnp.int32, (256, 256), 1)
    source = source - span * ((source >= span).astype(jnp.int32) + (source >= 2 * span).astype(jnp.int32))
    group = lax.shift_right_logical(lane & 127, members.bit_length() - 1)
    half = lax.shift_right_logical(lane, 7)
    last = (group == groups - 1).astype(jnp.int32)
    base = source - sub_rows * group - half - 8 + ITERS

    @pl.loop(0, pick.shape[0])
    def _(p):
        later = (2 * p + half >= sub_rows + ITERS).astype(jnp.int32)
        hit = base == 2 * p + later * (last - 1)
        pick[p] = jnp.where(hit, 1.0, 0.0).astype(jnp.bfloat16)


def apply(k, links, basis, parts, low, count):
    depth = ITERS - 1 - k
    here, out = basis[k], basis[k + 1]
    old = basis[k - 1] if k else None

    def column(t):
        x0 = PAD - depth + 8 * t
        mid, east, west = pl.ds(x0, 8), pl.ds(x0 + 1, 8), pl.ds(x0 - 1, 8)

        def three(r):
            return here[r, west, :], here[r, mid, :], here[r, east, :]

        for start, stop in parts:
            dn, cur = three(start - 1), three(start)
            north = links[0, start - 1 + (1 if start > SEAM else 0), mid, :]
            for r in range(start, stop):
                nxt = three(r + 1)
                c = r + (1 if r >= SEAM else 0)
                if r == SEAM:
                    north = links[0, c - 1, mid, :]
                south, north = north, links[0, c, mid, :]
                total = (north * nxt[1] + south * dn[1]) + (
                    links[1, c, mid, :] * cur[2] + links[1, c, west, :] * cur[0]
                )
                total = total + (links[2, c, mid, :] * nxt[2] + links[2, c - 1, west, :] * dn[0])
                total = total + (links[3, c, west, :] * nxt[0] + links[3, c - 1, mid, :] * dn[2])
                total = total - (cur[1] if old is None else cur[1] + old[r, mid, :])
                out[r, mid, :] = total
                dn, cur = cur, nxt

    if count > 3:

        @pl.loop(0, count // 2)
        def _(t):
            column(low + 2 * t)
            column(low + 2 * t + 1)

    for t in range(count - count % 2 if count > 3 else 0, count):
        column(low + t)


def begin(raw, links, basis):
    @pl.loop(ITERS, SEAM)
    def _(r):
        for t in range(16):
            at = slice(PAD + 8 * t, PAD + 8 * t + 8)
            basis[0][r, at, :] = raw[r, at, :] * links[4, r, at, :]

    apply(0, links, basis, [(ITERS + 1, SEAM - 1)], 1, 15)
    apply(1, links, basis, [(ITERS + 2, SEAM - 2)], 1, 14)


def iterate(members, rows, top, raw, links, basis, gram_ref):
    subs = iota(0)
    group = lax.shift_right_logical(iota(1), members.bit_length() - 1)
    for r in range(ITERS, SEAM):
        for t in (0, 17):
            at = slice(PAD - 8 + 8 * t, PAD + 8 * t)
            basis[0][r, at, :] = raw[r, at, :] * links[4, r, at, :]

    apply(0, links, basis, [(1, ITERS + 1), (SEAM - 1, SEAM + ITERS - 1)], 0, 18)
    apply(0, links, basis, [(ITERS + 1, SEAM - 1)], 0, 1)
    apply(0, links, basis, [(ITERS + 1, SEAM - 1)], 16, 2)
    apply(1, links, basis, [(2, ITERS + 2), (SEAM - 2, SEAM + ITERS - 2)], 0, 17)
    apply(1, links, basis, [(ITERS + 2, SEAM - 2)], 0, 1)
    apply(1, links, basis, [(ITERS + 2, SEAM - 2)], 15, 2)
    for k in range(2, ITERS - 1):
        depth = ITERS - 1 - k
        count = (128 + 2 * depth + 7) // 8
        apply(k, links, basis, [(ITERS - depth, SEAM + depth)], 0, count)

    zero = jnp.zeros((8, 128), F32)
    fold = jnp.logical_and(group == 128 // members - 1, top)
    newest = basis[ITERS - 1]

    def body(r, sums):
        sums = list(sums)
        r = r + ITERS
        share = jnp.where(jnp.logical_and(fold, r == SEAM - 1), 0.5, 1.0)
        for t in range(16):
            at = slice(PAD + 8 * t, PAD + 8 * t + 8)
            east, west = (slice(PAD + 8 * t + d, PAD + 8 * t + d + 8) for d in (1, -1))
            vs = [basis[k][r, at, :] for k in range(ITERS)]
            for i in range(ITERS):
                sums[2 * i] = sums[2 * i] + vs[i] * vs[i]
                if i + 1 < ITERS:
                    sums[2 * i + 1] = sums[2 * i + 1] + vs[i] * vs[i + 1]
            ahead = links[0, r, at, :] * newest[r + 1, at, :]
            ahead = ahead + links[2, r, at, :] * newest[r + 1, east, :]
            ahead = ahead + links[3, r, west, :] * newest[r + 1, west, :]
            ahead = ahead * share + links[1, r, at, :] * newest[r, east, :]
            sums[-1] = sums[-1] + vs[-1] * ahead
        return tuple(sums)

    sums = lax.fori_loop(0, SEAM - ITERS, body, (zero,) * (2 * ITERS))
    sums = sums[:-1] + (sums[-1] + sums[-1],)

    def across(t, sums):
        sums = list(sums)
        for u in range(8):
            x0 = PAD + 64 * t + 8 * u
            mid, east, west = pl.ds(x0, 8), pl.ds(x0 + 1, 8), pl.ds(x0 - 1, 8)
            north, right, left = links[0, SEAM - 1, mid, :], links[2, SEAM - 1, mid, :], links[3, SEAM - 1, west, :]
            here, over = [], []
            for k in range(ITERS):
                w = basis[k]
                v = north * w[SEAM, mid, :] + right * w[SEAM, east, :] + left * w[SEAM, west, :]
                over.append(jnp.where(fold, v, 0.0))
                here.append(w[SEAM - 1, mid, :])
            for n, (i, j) in enumerate(SKEW):
                sums[n] = sums[n] + (here[i] * over[j] - here[j] * over[i])
        return tuple(sums)

    sums = sums + lax.fori_loop(0, 2, across, (zero,) * len(SKEW))
    pack = [zero] * 4
    for n, s in enumerate(sums):
        for step in (1, 2, 4):
            s = s + pltpu.roll(s, step, 0)
        pack[n // 8] = jnp.where(subs == n % 8, s, pack[n // 8])
    total = zero
    for j, v in enumerate(pack):
        width = members
        while width < 128:
            v = v + pltpu.roll(v, width, 1)
            width *= 2
        total = jnp.where(group == j, v, total)
    gram_ref[...] = total


def solve_kernel(members, rows, ny, nx, rhs_hbm, coup_hbm, center_hbm, mask_hbm, *refs):
    basis, (scale_ref, sum_ref) = refs[: ITERS + 1], refs[ITERS + 1 : ITERS + 3]
    (
        field, links, planes, rhs, coup, center, mask, coef_out, coef_in, rows_out, rows_in, strip_out, corner_out, corner_in, ext,
        shifted, inv, square, lhs, pick, gram, along_x, along_y, load, send, recv,
    ) = refs[ITERS + 3 :]
    groups = 128 // members
    sub_rows = rows // groups
    tall = rhs.shape[1]
    y, x = lax.axis_index("gy"), lax.axis_index("gx")
    top = (y + 1) // ny
    mirror = nx - 1 - x
    east, west = lax.rem(x + 1, nx), lax.rem(x + nx - 1, nx)
    up = (y + 1 - top, x + top * (mirror - x))
    down = (jnp.maximum(y - 1, 0), x)
    loads = [
        pltpu.make_async_copy(coup_hbm, coup, load.at[0]),
        pltpu.make_async_copy(center_hbm, center, load.at[1]),
        pltpu.make_async_copy(mask_hbm, mask, load.at[2]),
        pltpu.make_async_copy(rhs_hbm, rhs.at[:, 0:rows, :], load.at[3]),
    ]
    for c in loads:
        c.start()
    barrier = pltpu.get_barrier_semaphore()

    def greet(there):
        pl.semaphore_signal(barrier, inc=1, device_id=there, device_id_type=pl.DeviceIdType.MESH)

    for step in range(1, nx):
        greet((y, lax.rem(x + step, nx)))
    for step in range(1, ny):
        greet((lax.rem(y + step, ny), x))

    @pl.when(y > 0)
    def _():
        greet((y - 1, east))
        greet((y - 1, west))

    @pl.when(top == 0)
    def _():
        greet((y + 1, east))
        greet((y + 1, west))

    def copy(src, dst, n, m, there):
        return pltpu.make_async_remote_copy(
            src_ref=src,
            dst_ref=dst,
            send_sem=send.at[n],
            recv_sem=recv.at[m],
            device_id=there,
            device_id_type=pl.DeviceIdType.MESH,
        )

    def corner(base, parts):
        found = []
        for e in range(2):
            plain, folded = x + 2 * e - 1, mirror + 1 - 2 * e
            to = lax.rem(plain + top * (folded - plain) + nx, nx)
            k = 1 - e + top * (1 + 2 * e)
            c = copy(
                corner_out.at[e, parts], corner_in.at[k, parts], base + e, base + k, (y + 1 - top, to)
            )
            found.append((jnp.logical_or(top == 0, to != x), c, e, k))
        for e in range(2):
            k = 3 - e
            there = (jnp.maximum(y - 1, 0), east if e else west)
            c = copy(
                corner_out.at[2 + e, parts], corner_in.at[k, parts], base + 2 + e, base + k, there
            )
            found.append((y > 0, c, 2 + e, k))
        return found

    def start_corners(found, parts):
        for n, (remote, c, e, k) in enumerate(found):
            pl.when(remote)(c.start)
            if n < 2:

                @pl.when(jnp.logical_not(remote))
                def _():
                    corner_in[k, parts] = corner_out[e, parts]

    def corner_arrivals(found, base, parts):
        for k in range(4):
            c = copy(corner_out.at[0, parts], corner_in.at[k, parts], base, base + k, (y, east))
            pl.when(y > 0 if k < 2 else found[k - 2][0])(c.wait_recv)

    lanes, subs = iota(1), iota(0)
    flip_lane = jnp.where(top == 1, 127 - lanes, lanes)
    flip_sub = jnp.where(top == 1, 7 - subs, subs)
    tiles = (slice(PAD, PAD + 8), slice(PAD + 120, PAD + 128))
    beyond_tiles = (slice(PAD - 8, PAD), slice(PAD + 128, PAD + 136))
    for c in loads[:3]:
        c.wait()

    def own(p, at):
        if p < 3:
            return coup[p, at, :]
        return center[at, :] if p == 3 else mask[at, :].astype(F32)

    packs = [jnp.zeros((8, 128), F32)] * 4
    plane = lax.shift_right_logical(lanes, 3)
    high_lanes = jnp.where(top == 1, rows + 7 - (lanes & 7), rows + (lanes & 7))
    low_lanes = 8 + (lanes & 7)
    ext[0:8, :] = jnp.zeros((8, 128), F32)
    ext[rows + 8 : 128, :] = jnp.zeros((120 - rows, 128), F32)
    for p in range(5):
        coef_out[0, p] = along(along(own(p, slice(rows - 8, rows)), flip_lane, 1), flip_sub, 0)
        coef_out[1, p] = own(p, slice(0, 8))
        ext[8 : rows + 8, :] = own(p, slice(0, rows))
        turned = ext[...].T
        for e, edge in enumerate((turned[0:8], turned[120:128])):
            strip_out[e, p] = edge
            packs[e] = jnp.where(plane == p, along(edge, high_lanes, 1), packs[e])
            packs[2 + e] = jnp.where(plane == p, along(edge, low_lanes, 1), packs[2 + e])
    for e in range(4):
        corner_out[e, 0] = along(packs[e], flip_sub, 0) if e < 2 else packs[e]
    pl.semaphore_wait(barrier, nx + ny - 2 + 2 * (1 - top) + 2 * jnp.minimum(y, 1))
    coef_up = copy(coef_out.at[0], coef_in.at[top], 0, top, up)
    coef_down = copy(coef_out.at[1], coef_in.at[1], 1, 1, down)
    rows_up = copy(rows_out.at[0], rows_in.at[top], 2, 2 + top, up)
    rows_down = copy(rows_out.at[1], rows_in.at[1], 3, 3, down)
    first = slice(0, 1)
    later = slice(1, 3)
    coef_corners, rows_corners = corner(8, first), corner(12, later)
    sides = [
        copy(strip_out.at[0], planes.at[:, PAD + 128 : PAD + 136, :], 4, 4, (y, west)),
        copy(strip_out.at[1], planes.at[:, PAD - 8 : PAD, :], 5, 5, (y, east)),
    ]
    start_corners(coef_corners, first)
    coef_up.start()
    pl.when(y > 0)(coef_down.start)
    for c in sides:
        c.start()
    flat = rhs.reshape(members * tall, 128)

    def column(row, block):
        return flat[pl.ds(8 * block * tall + row, 8, stride=tall), :]

    blocks = members // 8
    loads[3].wait()
    for q in range(ITERS):
        high = rows - ITERS + q + top * (ITERS - 1 - 2 * q)
        for b in range(blocks):
            at = slice(q * members + 8 * b, q * members + 8 * b + 8)
            rows_out[0, at, :] = along(column(high, b), flip_lane, 1)
            rows_out[1, at, :] = column(q, b)

    @pl.loop(0, sub_rows // 4)
    def _(part):
        for within in range(4):
            r = 4 * part + within
            stack = [column(sub_rows * g + r, b) for g in range(groups) for b in range(blocks)]
            field[r + ITERS, PAD : PAD + 128, :] = jnp.concatenate(stack, axis=0).T

    member = lanes & (members - 1)
    group = lax.shift_right_logical(lanes, members.bit_length() - 1)
    for e in range(2):
        packs = [[jnp.zeros((8, 128), F32)] * 2 for _ in range(2)]
        for q in range(ITERS):
            here = group == q % groups
            v = field[sub_rows + q + top * (ITERS - 1 - 2 * q), tiles[e], :]
            v = along(v, member + (128 - members), 1)
            packs[0][q // groups] = jnp.where(here, v, packs[0][q // groups])
            v = along(field[ITERS + q, tiles[e], :], member, 1)
            packs[1][q // groups] = jnp.where(here, v, packs[1][q // groups])
        for n in range(2):
            corner_out[e, 1 + n] = along(packs[0][n], flip_sub, 0)
            corner_out[2 + e, 1 + n] = packs[1][n]
    inner = slice(ITERS, ITERS + sub_rows)
    more = [
        copy(field.at[inner, tiles[0], :], field.at[inner, beyond_tiles[1], :], 6, 6, (y, west)),
        copy(field.at[inner, tiles[1], :], field.at[inner, beyond_tiles[0], :], 7, 7, (y, east)),
    ]
    start_corners(rows_corners, later)
    for c in more:
        c.start()
    choose(members, rows, pick)
    coef_north = copy(coef_out.at[1], coef_in.at[1], 1, 1, down)
    coef_south = copy(coef_out.at[0], coef_in.at[0], 0, 0, up)
    coef_north.wait_recv()
    pl.when(y > 0)(coef_south.wait_recv)
    rows_up.start()
    pl.when(y > 0)(rows_down.start)
    for p in range(5):
        beyond = coef_in[1, p]
        moved = pltpu.roll(beyond, 1, 0)
        if p in (0, 2):
            last = jnp.broadcast_to(own(p, slice(rows - 1, rows)), (8, 128))
            beyond = jnp.where(top == 1, beyond, jnp.where(subs == 0, last, moved))
        else:
            beyond = jnp.where(subs == 0, beyond, moved)
        ext[0:8, :] = jnp.where(y == 0, 0.0, coef_in[0, p])
        ext[8 : rows + 8, :] = own(p, slice(0, rows))
        ext[rows + 8 : rows + 16, :] = beyond
        planes[p, PAD : PAD + 128, :] = ext[...].T
    for c in sides:
        c.wait_recv()
    corner_arrivals(coef_corners, 8, first)
    for e in range(2):
        low, high = corner_in[e, 0], corner_in[2 + e, 0]
        for p in range(5):
            strip = planes[p, beyond_tiles[e], :]
            shift = 1 - top if p in (0, 2) else 1
            idx = jnp.clip(lanes - (rows + 8) - shift, 0, 7) + 8 * p
            north = along(high, idx, 1)
            if p in (0, 2):
                joint = jnp.logical_and(lanes == rows + 8, top == 0)
                north = jnp.where(joint, pltpu.roll(strip, 1, 1), north)
            south = jnp.where(y == 0, 0.0, along(low, (lanes & 7) + 8 * p, 1))
            outside = jnp.logical_and(lanes >= rows + 8, lanes < rows + 16)
            strip = jnp.where(lanes < 8, south, jnp.where(outside, north, strip))
            planes[p, beyond_tiles[e], :] = strip
    prepare(members, rows, y == ny - 1, planes, shifted, inv, links, square, lhs, pick)
    begin(field, links, basis)
    copy(rows_out.at[1], rows_in.at[1], 3, 3, down).wait_recv()
    pl.when(y > 0)(copy(rows_out.at[0], rows_in.at[0], 2, 2, up).wait_recv)

    def arrived(side, q, b):
        return rows_in[side, q * members + 8 * b : q * members + 8 * b + 8, :]

    for _ in range(1):
        for q in range(ITERS):
            low = [jnp.where(y == 0, 0.0, arrived(0, q, b)) for b in range(blocks)]
            low += [column(sub_rows * g - ITERS + q, b) for g in range(1, groups) for b in range(blocks)]
            basis[0][q, PAD : PAD + 128, :] = (
                jnp.concatenate(low, axis=0).T * links[4, q, PAD : PAD + 128, :]
            )
            high = [column(sub_rows * g + q, b) for g in range(1, groups) for b in range(blocks)]
            high += [arrived(1, q, b) for b in range(blocks)]
            r = q + ITERS + sub_rows
            basis[0][r, PAD : PAD + 128, :] = (
                jnp.concatenate(high, axis=0).T * links[4, r + 1, PAD : PAD + 128, :]
            )

    for c in more:
        c.wait_recv()
    corner_arrivals(rows_corners, 12, later)
    for e in range(2):
        for q in range(ITERS):
            idx = member + members * (q % groups)
            south = along(corner_in[e, 1 + q // groups], idx, 1)
            south = jnp.where(y == 0, 0.0, south)
            v = pltpu.roll(field[sub_rows + q, beyond_tiles[e], :], members, 1)
            v = jnp.where(group == 0, south, v)
            basis[0][q, beyond_tiles[e], :] = v * links[4, q, beyond_tiles[e], :]
            north = along(corner_in[2 + e, 1 + q // groups], idx, 1)
            v = pltpu.roll(field[ITERS + q, beyond_tiles[e], :], 128 - members, 1)
            v, r = jnp.where(group == groups - 1, north, v), ITERS + sub_rows + q
            basis[0][r, beyond_tiles[e], :] = v * links[4, r + 1, beyond_tiles[e], :]
    coef_up.wait_send()
    rows_up.wait_send()

    @pl.when(y > 0)
    def _():
        coef_down.wait_send()
        rows_down.wait_send()

    for c in sides + more:
        c.wait_send()
    for remote, c, _, _ in coef_corners + rows_corners:
        pl.when(remote)(c.wait_send)
    iterate(members, rows, y == ny - 1, field, links, basis, gram)

    def sent(source, dst, n, there):
        c = copy(source, dst, n, n, there)
        c.start()
        return c

    across = [sent(gram, along_x.at[s], 15 + s, (y, lax.rem(x + s, nx))) for s in range(1, nx)]
    apply(ITERS - 1, links, basis, [(ITERS, SEAM)], 0, 16)
    scale_ref[0] = inv[PAD : PAD + 128, :].T
    scale_ref[1] = square[PAD : PAD + 128, :].T
    for c in across:
        c.wait()
    along_x[0] = sum((along_x[s] for s in range(1, nx)), gram[...])
    across = [
        sent(along_x.at[0], along_y.at[s], 14 + nx + s, (lax.rem(y + s, ny), x)) for s in range(1, ny)
    ]
    for c in across:
        c.wait()
    sum_ref[...] = sum((along_y[s] for s in range(1, ny)), along_x[0])


def coefficients(gram):
    def g(i, j):
        return gram[min(i, j)][max(i, j)]

    def applied(p):
        q = []
        for k in range(ITERS + 1):
            terms = []
            if k < len(p):
                terms.append((1.0 - ROOT) * p[k])
            if 0 < k <= len(p):
                terms.append(-ROOT * p[k - 1])
            if k + 1 < len(p):
                terms.append(-ROOT * p[k + 1])
            if terms:
                q.append(sum(terms[1:], terms[0]))
        return q

    def inner(p, q):
        total = None
        for i, a in enumerate(p):
            row = None
            for j, b in enumerate(q):
                t = g(i, j) * b
                row = t if row is None else row + t
            t = a * row
            total = t if total is None else total + t
        return total

    one = jnp.ones_like(gram[0][0])
    z, p, x = [one], [one], []
    rz = g(0, 0)
    for iteration in range(ITERS):
        q = applied(p)
        step = rz / inner(p, q)
        x = [(x[k] if k < len(x) else 0.0) + step * p[k] for k in range(len(p))]
        z = [(z[k] if k < len(z) else 0.0) - step * q[k] for k in range(len(q))]
        if iteration + 1 < ITERS:
            rz_new = inner(z, z)
            beta = rz_new / rz
            p = [z[k] + (beta * p[k] if k < len(p) else 0.0) for k in range(len(z))]
            rz = rz_new
    return x, z


def combine_kernel(members, rows, *refs):
    basis, (scale_ref, sum_ref, x_out, r_out, stage, sems) = refs[: ITERS + 1], refs[ITERS + 1 :]
    groups = 128 // members
    sub_rows = rows // groups
    tall = stage.shape[2]
    lanes = iota(1)
    sums = sum_ref[...]
    tiles = [along(sums, (lanes & (members - 1)) + members * j, 1) for j in range(4)]
    found = [
        jnp.broadcast_to(tiles[n // 8][n % 8 : n % 8 + 1, :], (8, 128))
        for n in range(2 * ITERS + len(SKEW))
    ]
    gram = [[None] * (ITERS + 1) for _ in range(ITERS + 1)]
    for i in range(ITERS):
        gram[i][i], gram[i][i + 1] = found[2 * i], found[2 * i + 1]
    last = ITERS - 1
    gram[last][ITERS] = gram[last][ITERS] - gram[last][last] - gram[last - 1][last]
    skew = dict(zip(SKEW, found[2 * ITERS :]))
    for gap in range(2, ITERS + 1):
        for i in range(ITERS + 1 - gap):
            j = i + gap - 1
            v = gram[i + 1][j] - gram[i][j - 1] + skew[i, j]
            gram[i][j + 1] = v + gram[i - 1][j] if i else v
    xs, zs = coefficients(gram)
    flat = stage.reshape(2 * members * tall, 128)
    blocks = members // 8
    half = sub_rows // 2
    outs = (x_out, r_out)

    def drain(h, o):
        copies = []
        for g in range(groups):
            at = slice(sub_rows * g + half * h, sub_rows * g + half * (h + 1))
            copies.append(
                pltpu.make_async_copy(stage.at[o, :, at, :], outs[o].at[:, at, :], sems.at[h, o, g])
            )
        return copies

    started = []
    for h in range(2):
        for o, weights in enumerate((xs, zs)):

            def row(r):
                found = []
                for t in range(16):
                    at = slice(PAD + 8 * t, PAD + 8 * t + 8)
                    terms = [w * basis[k][r + ITERS, at, :] for k, w in enumerate(weights)]
                    found.append(sum(terms[1:], terms[0]))
                turned = jnp.concatenate(found, axis=0).T
                for g in range(groups):
                    row = sub_rows * g + r
                    scale = jnp.broadcast_to(scale_ref[o, pl.ds(row + 8, 1), :], (8, 128))
                    for b in range(blocks):
                        n = 8 * (g * blocks + b)
                        at = pl.ds((o * members + 8 * b) * tall + row, 8, stride=tall)
                        flat[at, :] = turned[n : n + 8, :] * scale

            for within in range(half):
                row(half * h + within)

            for c in drain(h, o):
                c.start()
                started.append(c)
    for c in started:
        c.wait()


def on_device(right_side, couplings, center, ocean_mask):
    members, rows, columns = right_side.shape
    groups = 128 // members
    sub_rows = rows // groups
    assert lax.axis_size("gx") > 2 and ITERS <= 2 * groups
    assert columns == 128 and members % 8 == 0 and groups * members == 128
    assert 3 * (rows + 16) <= 256 < 4 * (rows + 16) and 2 * (rows + 16) >= 128 and sub_rows == SEAM - ITERS
    ny, nx = lax.axis_size("gy"), lax.axis_size("gx")
    vmem = pl.BlockSpec(memory_space=pltpu.VMEM)
    hbm = pl.BlockSpec(memory_space=pltpu.HBM)
    deep, wide = sub_rows + 2 * ITERS, columns + 2 * PAD + 8

    inputs = [
        pltpu.with_memory_space_constraint(v, pltpu.HBM)
        for v in (right_side, couplings, center, ocean_mask)
    ]

    def first(*refs):
        solve_kernel(members, rows, ny, nx, *refs)

    *basis, scale, sums = pl.pallas_call(
        first,
        out_shape=(pltpu.VMEM((deep, wide, 128), F32),) * (ITERS + 1)
        + (pltpu.VMEM((2, 128, 128), F32), pltpu.VMEM((8, 128), F32)),
        in_specs=[hbm] * 4,
        out_specs=(vmem,) * (ITERS + 3),
        scratch_shapes=[
            pltpu.VMEM((deep, wide, 128), F32),
            pltpu.VMEM((5, deep + 3, wide, 128), F32),
            pltpu.VMEM((5, wide, 128), F32),
            pltpu.VMEM((members, rows + 8, columns), F32),
            pltpu.VMEM((3, rows, columns), F32),
            pltpu.VMEM((rows, columns), F32),
            pltpu.VMEM((rows, columns), jnp.int32),
            pltpu.VMEM((2, 5, 8, columns), F32),
            pltpu.VMEM((2, 5, 8, columns), F32),
            pltpu.VMEM((2, ITERS * members, columns), F32),
            pltpu.VMEM((2, ITERS * members, columns), F32),
            pltpu.VMEM((2, 5, 8, 128), F32),
            pltpu.VMEM((4, 3, 8, 128), F32),
            pltpu.VMEM((4, 3, 8, 128), F32),
            pltpu.VMEM((128, 128), F32),
            pltpu.VMEM((2, wide, 128), F32),
            pltpu.VMEM((wide, 128), F32),
            pltpu.VMEM((wide, 128), F32),
            pltpu.VMEM((5 * 144, 256), jnp.bfloat16),
            pltpu.VMEM(((deep + 2) // 2, 256, 256), jnp.bfloat16),
            pltpu.VMEM((8, 128), F32),
            pltpu.VMEM((nx, 8, 128), F32),
            pltpu.VMEM((ny, 8, 128), F32),
            pltpu.SemaphoreType.DMA((4,)),
            pltpu.SemaphoreType.DMA((14 + nx + ny,)),
            pltpu.SemaphoreType.DMA((14 + nx + ny,)),
        ],
        compiler_params=pltpu.CompilerParams(
            collective_id=0, has_side_effects=True, vmem_limit_bytes=GRANT
        ),
    )(*inputs)

    def second(*refs):
        combine_kernel(members, rows, *refs)

    return pl.pallas_call(
        second,
        out_shape=(jax.ShapeDtypeStruct(right_side.shape, F32),) * 2,
        in_specs=[vmem] * (ITERS + 3),
        out_specs=(hbm, hbm),
        compiler_params=pltpu.CompilerParams(vmem_limit_bytes=GRANT),
        scratch_shapes=[
            pltpu.VMEM((2, members, rows + 8, columns), F32),
            pltpu.SemaphoreType.DMA((2, 2, groups)),
        ],
    )(*basis, scale, sums)


def solution(mesh):
    in_specs = (P(None, "gy", "gx"), P(None, "gy", "gx"), P("gy", "gx"), P("gy", "gx"))
    out_specs = (P(None, "gy", "gx"), P(None, "gy", "gx"))
    return jax.shard_map(
        on_device, mesh=mesh, in_specs=in_specs, out_specs=out_specs, check_vma=False
    )
```
